128 devices in a mesh: ka: 16 (over z_lo, y, core), ga: 8 (over x, z_hi).
Axes of the slice: x: 4, y: 4, z: 4 (z_hi: 2, z_lo: 2; z = z_hi * 2 + z_lo), core: 2. Of those that a mesh axis runs over, the one named last changes fastest.
Arguments:
- coeffs: bfloat16 [16, 2, 15360, 256], P('ka', None, 'ga'), may hold values from -1 to 1
- projectors: bfloat16 [2, 15360, 1024], P(None, 'ga'), may hold values from -1.5 to 1.5
- proj_deriv: bfloat16 [2, 15360, 1024], P(None, 'ga'), may hold values from -1.5 to 1.5
- shift_map: int32 [15360], P('ga'), may hold values from 0 to 15359, as said below
- atom_of: int32 [1024], replicated, may hold values from 0 to 127, as said below
Outputs:
- transport: float32 [16, 2, 256, 256], P('ka')
- forces: float32 [128], replicated
The draws below stay inside these ranges and needn't reach their ends.
Inputs may be any that keep to these rules, and one draw needn't show every extreme that they name: `shift_map`: a permutation that maps each aligned block of 1920 plane waves onto itself. `atom_of`: each atom owns exactly 8 projectors.
All inputs are finite; a program needn't handle non-finite values.
Results may differ from the reference program's by a relative error of at most 0.0003.
Values may be sent and summed in bfloat16 or wider, within the bound.
A program may use at most 128 MiB of HBM per device.

```python
import math
import jax
import jax.numpy as jnp
from jax import lax

NB = 256
GD = 1920
NP = 1024
NA = 128
NEWTON = 2
NK = 16
NG = 15360


def block_shift(key):
    start_key = jax.random.fold_in(key, 11)
    block_keys = jax.random.split(start_key, NG // GD)
    shuffled = jax.vmap(lambda single: jax.random.permutation(single, GD))(block_keys)
    offsets = jnp.arange(NG // GD, dtype=jnp.int32) * GD
    return (shuffled.astype(jnp.int32) + offsets[:, None]).reshape(NG)


def draw_shift_map(key, part):
    return block_shift(key)


def draw_coeffs(key, part):
    mapping = block_shift(key)
    common_key = jax.random.fold_in(key, 21)
    spread_key = jax.random.fold_in(key, 22)
    common = jax.random.normal(common_key, (2, NG, NB), jnp.float32)
    spread_part = 0.3 * jax.random.normal(spread_key, (NK, 2, NG, NB), jnp.float32)
    norming = (2.0 * NG) ** (-0.5)
    common = common * norming
    spread_part = spread_part * norming
    angles = math.pi / 2 * jnp.arange(NK, dtype=jnp.float32) / NK
    moved = common[:, mapping, :]
    values = jnp.cos(angles)[:, None, None, None] * common[None] + jnp.sin(angles)[:, None, None, None] * moved[None] + spread_part
    return jnp.clip(values, -1.0, 1.0).astype(jnp.bfloat16)


def draw_atom_of(key, part):
    order = jax.random.permutation(jax.random.fold_in(key, 31), NP)
    return (order // (NP // NA)).astype(jnp.int32)


def level_of(stream_key, extent, pieces, smallest, top_value):
    def one(dim, parts):
        heights = jax.random.uniform(jax.random.fold_in(jax.random.fold_in(stream_key, 6), dim), (parts,), jnp.float32, smallest / len(pieces), top_value / len(pieces))
        return jnp.repeat(jnp.exp(heights), extent[dim] // parts).reshape((-1,) + (1,) * (len(extent) - dim - 1))

    factor_of = one(*pieces[0])
    for cut in pieces[1:]:
        factor_of = factor_of * one(*cut)
    return factor_of


def gaussian(stream_key, extent, scale, bound, pieces=(), kind=jnp.bfloat16):
    drawn = jax.random.normal(stream_key, extent, jnp.float32) * scale
    if len(pieces) > 0:
        drawn = level_of(stream_key, extent, pieces, -0.22, 0.18) * drawn
    return jnp.clip(drawn, min=-bound, max=bound).astype(kind)


def setup_inputs(seed: int = 0) -> dict:
    arg_keys = jax.random.split(jax.random.key(seed), 6)
    return {
        "coeffs": draw_coeffs(jax.random.fold_in(arg_keys[5], 71), 0),
        "projectors": gaussian(arg_keys[1], (2, NG, NP), 0.25, 1.5, ((1, 8),)),
        "proj_deriv": gaussian(arg_keys[2], (2, NG, NP), 0.25, 1.5, ((1, 8),)),
        "shift_map": draw_shift_map(jax.random.fold_in(arg_keys[5], 71), 0),
        "atom_of": draw_atom_of(jax.random.fold_in(arg_keys[5], 71), 0),
    }


def cmul(left, right):
    highest = lax.Precision.HIGHEST
    left_re, left_im = left[..., 0, :, :], left[..., 1, :, :]
    right_re, right_im = right[..., 0, :, :], right[..., 1, :, :]
    real_part = jnp.matmul(left_re, right_re, precision=highest) - jnp.matmul(left_im, right_im, precision=highest)
    imag_part = jnp.matmul(left_re, right_im, precision=highest) + jnp.matmul(left_im, right_re, precision=highest)
    return jnp.stack([real_part, imag_part], axis=-3)


def invert(intersection, eye_c):
    estimate = eye_c
    for newton_step in range(NEWTON):
        estimate = cmul(estimate, 2.0 * eye_c - cmul(intersection, estimate))
    return estimate


def project(proj_table, columns, swapped):
    real_part = jnp.dot(proj_table.T, columns, preferred_element_type=jnp.float32)
    imag_part = jnp.dot(proj_table.T, swapped, preferred_element_type=jnp.float32)
    return jnp.stack([real_part, imag_part])


def reference(coeffs, projectors, proj_deriv, shift_map, atom_of):
    proj_table = projectors.reshape(2 * NG, NP)
    deriv_table = proj_deriv.reshape(2 * NG, NP)
    eye_c = jnp.stack([jnp.eye(NB, dtype=jnp.float32), jnp.zeros((NB, NB), jnp.float32)])

    def k_point(state_pair, k_index):
        running, accumulated = state_pair
        own_point = lax.dynamic_index_in_dim(coeffs, k_index, 0, keepdims=False)
        following = lax.dynamic_index_in_dim(coeffs, (k_index + 1) % NK, 0, keepdims=False)
        following = jnp.where(k_index == NK - 1, following[:, shift_map, :], following)
        columns = own_point.reshape(2 * NG, NB)
        own_swap = jnp.concatenate([own_point[1], -own_point[0]], axis=0)
        next_cols = following.reshape(2 * NG, NB)
        next_swap = jnp.concatenate([following[1], -following[0]], axis=0)
        intersections = jnp.stack([
            jnp.dot(columns.T, next_cols, preferred_element_type=jnp.float32),
            jnp.dot(columns.T, next_swap, preferred_element_type=jnp.float32)])
        inverse = invert(intersections, eye_c)
        running = cmul(running, inverse)
        proj_vals = project(proj_table, columns, own_swap)
        deriv_vals = project(deriv_table, columns, own_swap)
        weighted = cmul(proj_vals, running)
        accumulated = accumulated + jnp.sum(deriv_vals[0] * weighted[1] - deriv_vals[1] * weighted[0], axis=1)
        return (running, accumulated), running

    (running, accumulated), transport = lax.scan(
        k_point, (eye_c, jnp.zeros((NP,), jnp.float32)), jnp.arange(NK, dtype=jnp.int32))
    onehot = (atom_of[None, :] == jnp.arange(NA, dtype=jnp.int32)[:, None]).astype(jnp.float32)
    forces = jnp.dot(onehot, accumulated / NK, precision=lax.Precision.HIGHEST)
    return transport, forces
```

```python
import functools

import jax
import jax.numpy as jnp
from jax import lax
from jax.experimental import pallas as pl
from jax.experimental.pallas import tpu as pltpu
from jax.sharding import PartitionSpec as P

MESH = pl.DeviceIdType.MESH
F32 = jnp.float32
BF16 = jnp.bfloat16


def split(value):
    high = value.astype(BF16)
    low = (value - high.astype(F32)).astype(BF16)
    return high, low


def dot(left, right):
    return jnp.dot(left, right, preferred_element_type=F32)


def dot3(left, right_high, right_low):
    left_high, left_low = split(left)
    return dot(left_high, right_high) + (dot(left_high, right_low) + dot(left_low, right_high))


def cmul(left, right_re, right_im):
    rows = left.shape[0] // 2
    by_re = dot3(left, *split(right_re))
    by_im = dot3(left, *split(right_im))
    return by_re[:rows] - by_im[rows:], by_im[:rows] + by_re[rows:]


def kernel(
    ka, ga, coeffs, proj, deriv, shift, atoms, transport, forces,
    own, following, moved, lhs, rhs, part, arrived, mpart, mrows, erow, efull,
    xfull, tin, trow, tfull, fka, fga,
    load_sem, rhs_sem, nb_send, nb_recv, rs_send, rs_recv, m_send, m_recv, e_send, e_recv,
    t_send, t_recv, g_send, g_recv, f_send, f_recv, h_send, h_recv, out_sem,
):
    nb = own.shape[1]
    half = own.shape[0] // 2
    cols = part.shape[2] // 2
    rows = nb // ga
    k = lax.axis_index("ka")
    g = lax.axis_index("ga")

    def ga_at(offset):
        return lax.rem(g + offset, ga)

    def ka_at(offset):
        return lax.rem(k + offset, ka)

    own_load = pltpu.make_async_copy(coeffs, own, load_sem.at[0])
    own_load.start()

    def rhs_loads(i):
        target = ga_at(1 + i)
        slot = lax.rem(i, 3)
        at = pl.ds(pl.multiple_of(target * cols, cols), cols)
        return (
            pltpu.make_async_copy(proj.at[:, :, at], rhs.at[slot, :, :, pl.ds(0, cols)], rhs_sem.at[slot, 0]),
            pltpu.make_async_copy(deriv.at[:, :, at], rhs.at[slot, :, :, pl.ds(cols, cols)], rhs_sem.at[slot, 1]),
        )

    for i in range(2):
        for copy in rhs_loads(i):
            copy.start()

    barrier = pltpu.get_barrier_semaphore()
    for offset in range(1, ga):
        pl.semaphore_signal(barrier, inc=1, device_id={"ka": k, "ga": ga_at(offset)}, device_id_type=MESH)
    for offset in range(1, ka):
        pl.semaphore_signal(barrier, inc=1, device_id={"ka": ka_at(offset), "ga": g}, device_id_type=MESH)
    pl.semaphore_wait(barrier, ga + ka - 2)

    own_load.wait()
    neighbour = pltpu.make_async_remote_copy(
        src_ref=own, dst_ref=following, send_sem=nb_send, recv_sem=nb_recv,
        device_id={"ka": ka_at(ka - 1), "ga": g}, device_id_type=MESH)
    neighbour.start()

    for at in range(0, half, 384):
        width = min(384, half - at)
        re = own[at:at + width, :].T
        im = own[half + at:half + at + width, :].T
        lhs[0:nb, at:at + width] = re
        lhs[0:nb, half + at:half + at + width] = im
        lhs[nb:2 * nb, at:at + width] = im
        lhs[nb:2 * nb, half + at:half + at + width] = -re

    def rs_copy(i):
        return pltpu.make_async_remote_copy(
            src_ref=part.at[i], dst_ref=arrived.at[i], send_sem=rs_send.at[i], recv_sem=rs_recv.at[i],
            device_id={"ka": k, "ga": ga_at(1 + i)}, device_id_type=MESH)

    def project(i, carry):
        for copy in rhs_loads(i):
            copy.wait()

        @pl.when(i + 2 < ga)
        def _():
            for copy in rhs_loads(i + 2):
                copy.start()

        part[i] = dot(lhs[...], rhs[lax.rem(i, 3)].reshape(2 * half, 2 * cols))

        @pl.when(i < ga - 1)
        def _():
            rs_copy(i).start()

        return carry

    lax.fori_loop(0, ga, project, 0)

    neighbour.wait_recv()

    @pl.when(k == ka - 1)
    def _():
        lanes = lax.broadcasted_iota(jnp.int32, (128, 128), 1).astype(F32)
        base = (g * half).astype(F32)

        def permute(b, carry):
            blocks = []
            for s in range(3):
                line = shift[pl.ds(b * 3 + s, 1), :].astype(F32) - base
                column = jnp.broadcast_to(line, (128, 128)).T
                blocks.append(jnp.concatenate(
                    [jnp.where(column == lanes + 128.0 * h, 1.0, 0.0).astype(BF16) for h in range(half // 128)], axis=1))
            chosen = jnp.concatenate(blocks, axis=0)
            at = pl.multiple_of(b * 384, 384)
            moved[pl.ds(at, 384), :] = dot(chosen, following[0:half, :]).astype(BF16)
            moved[pl.ds(half + at, 384), :] = dot(chosen, following[half:2 * half, :]).astype(BF16)
            return carry

        lax.fori_loop(0, half // 384, permute, 0)
        following[...] = moved[...]

    mpart[...] = dot(lhs[...], following[...]).reshape(2, nb, nb)

    def m_copy(i):
        at = pl.ds(pl.multiple_of(ga_at(1 + i) * rows, rows), rows)
        return pltpu.make_async_remote_copy(
            src_ref=mpart.at[:, at, :], dst_ref=mrows.at[i], send_sem=m_send.at[i], recv_sem=m_recv.at[i],
            device_id={"ka": k, "ga": ga_at(1 + i)}, device_id_type=MESH)

    for i in range(ga - 1):
        m_copy(i).start()
    mine = pl.ds(pl.multiple_of(g * rows, rows), rows)
    total = mpart[:, mine, :]
    for i in range(ga - 1):
        m_copy(i).wait_recv()
        total = total + mrows[i]
    row_at = lax.broadcasted_iota(jnp.int32, (rows, nb), 0) + g * rows
    col_at = lax.broadcasted_iota(jnp.int32, (rows, nb), 1)
    erow[0] = jnp.where(row_at == col_at, 1.0, 0.0) - total[0]
    erow[1] = total[1]

    def spread(i, source, target, send, recv):
        return pltpu.make_async_remote_copy(
            src_ref=source, dst_ref=target.at[:, mine, :], send_sem=send.at[i], recv_sem=recv.at[i],
            device_id={"ka": k, "ga": ga_at(1 + i)}, device_id_type=MESH)

    for i in range(ga - 1):
        spread(i, erow, efull, e_send, e_recv).start()
    efull[:, mine, :] = erow[...]
    for i in range(ga - 1):
        spread(i, erow, efull, e_send, e_recv).wait_recv()

    e_re, e_im = efull[0], efull[1]
    both = efull[...].reshape(2 * nb, nb)
    sq_re, sq_im = cmul(both, e_re, e_im)
    eye = jnp.where(
        lax.broadcasted_iota(jnp.int32, (nb, nb), 0) == lax.broadcasted_iota(jnp.int32, (nb, nb), 1), 1.0, 0.0)
    cu_re, cu_im = cmul(both, sq_re, sq_im)
    xfull[0] = eye + (e_re + (sq_re + cu_re))
    xfull[1] = e_im + (sq_im + cu_im)

    onward = pltpu.make_async_remote_copy(
        src_ref=trow, dst_ref=tin, send_sem=t_send, recv_sem=t_recv,
        device_id={"ka": ka_at(1), "ga": g}, device_id_type=MESH)

    @pl.when(k == 0)
    def _():
        trow[...] = xfull[:, mine, :]

    @pl.when(k > 0)
    def _():
        onward.wait_recv()
        re, im = cmul(tin[...].reshape(2 * rows, nb), xfull[0], xfull[1])
        trow[0] = re
        trow[1] = im

    @pl.when(k < ka - 1)
    def _():
        onward.start()

    for i in range(ga - 1):
        spread(i, trow, tfull, g_send, g_recv).start()
    tfull[:, mine, :] = trow[...]

    whole = part[ga - 1]
    for i in range(ga - 1):
        rs_copy(i).wait_recv()
        whole = whole + arrived[i]
    b_both = jnp.concatenate([whole[0:nb, 0:cols].T, whole[nb:2 * nb, 0:cols].T], axis=0)
    d_re = whole[0:nb, cols:2 * cols].T
    d_im = whole[nb:2 * nb, cols:2 * cols].T
    atom_column = jnp.broadcast_to(atoms[pl.ds(g, 1), :].astype(F32), (cols, 128)).T

    for i in range(ga - 1):
        spread(i, trow, tfull, g_send, g_recv).wait_recv()
    out_copy = pltpu.make_async_copy(tfull, transport, out_sem)
    out_copy.start()
    w_re, w_im = cmul(b_both, tfull[0], tfull[1])
    per_proj = jnp.sum(d_re * w_im - d_im * w_re, axis=1, keepdims=True) * (1.0 / ka)
    atom_ids = lax.broadcasted_iota(jnp.int32, (cols, 128), 1).astype(F32)
    force = jnp.sum(jnp.where(atom_column == atom_ids, per_proj, 0.0), axis=0, keepdims=True)
    fka[k] = jnp.broadcast_to(force, (8, 128))

    def along_ka(i):
        return pltpu.make_async_remote_copy(
            src_ref=fka.at[k], dst_ref=fka.at[k], send_sem=f_send.at[i], recv_sem=f_recv.at[i],
            device_id={"ka": ka_at(1 + i), "ga": g}, device_id_type=MESH)

    def along_ga(i):
        return pltpu.make_async_remote_copy(
            src_ref=fga.at[g], dst_ref=fga.at[g], send_sem=h_send.at[i], recv_sem=h_recv.at[i],
            device_id={"ka": k, "ga": ga_at(1 + i)}, device_id_type=MESH)

    for i in range(ka - 1):
        along_ka(i).start()
    for i in range(ka - 1):
        along_ka(i).wait_recv()
    fga[g] = jnp.sum(fka[...], axis=0)
    for i in range(ga - 1):
        along_ga(i).start()
    for i in range(ga - 1):
        along_ga(i).wait_recv()
    forces[...] = jnp.sum(fga[...], axis=0)[0:1]

    neighbour.wait_send()
    for i in range(ga - 1):
        rs_copy(i).wait_send()
        m_copy(i).wait_send()
        spread(i, erow, efull, e_send, e_recv).wait_send()
        spread(i, trow, tfull, g_send, g_recv).wait_send()
        along_ga(i).wait_send()
    for i in range(ka - 1):
        along_ka(i).wait_send()

    @pl.when(k < ka - 1)
    def _():
        onward.wait_send()

    out_copy.wait()


def local(ka, ga, coeffs, projectors, proj_deriv, shift_map, atom_of):
    _, _, half, nb = coeffs.shape
    np_ = projectors.shape[2]
    cols = np_ // ga
    rows = nb // ga
    anywhere = pl.BlockSpec(memory_space=pl.ANY)
    vmem = pl.BlockSpec(memory_space=pltpu.VMEM)
    dma = pltpu.SemaphoreType.DMA
    transport, forces = pl.pallas_call(
        functools.partial(kernel, ka, ga),
        out_shape=(jax.ShapeDtypeStruct((2, nb, nb), F32), jax.ShapeDtypeStruct((1, 128), F32)),
        in_specs=[anywhere, anywhere, anywhere, vmem, vmem],
        out_specs=(anywhere, vmem),
        scratch_shapes=[
            pltpu.VMEM((2 * half, nb), BF16),
            pltpu.VMEM((2 * half, nb), BF16),
            pltpu.VMEM((2 * half, nb), BF16),
            pltpu.VMEM((2 * nb, 2 * half), BF16),
            pltpu.VMEM((3, 2, half, 2 * cols), BF16),
            pltpu.VMEM((ga, 2 * nb, 2 * cols), F32),
            pltpu.VMEM((ga - 1, 2 * nb, 2 * cols), F32),
            pltpu.VMEM((2, nb, nb), F32),
            pltpu.VMEM((ga - 1, 2, rows, nb), F32),
            pltpu.VMEM((2, rows, nb), F32),
            pltpu.VMEM((2, nb, nb), F32),
            pltpu.VMEM((2, nb, nb), F32),
            pltpu.VMEM((2, rows, nb), F32),
            pltpu.VMEM((2, rows, nb), F32),
            pltpu.VMEM((2, nb, nb), F32),
            pltpu.VMEM((ka, 8, 128), F32),
            pltpu.VMEM((ga, 8, 128), F32),
            dma((1,)), dma((3, 2)), dma, dma, dma((ga - 1,)), dma((ga - 1,)), dma((ga - 1,)), dma((ga - 1,)),
            dma((ga - 1,)), dma((ga - 1,)), dma, dma, dma((ga - 1,)), dma((ga - 1,)),
            dma((ka - 1,)), dma((ka - 1,)), dma((ga - 1,)), dma((ga - 1,)), dma,
        ],
        compiler_params=pltpu.CompilerParams(
            collective_id=0, has_side_effects=True, vmem_limit_bytes=60 * 1024 * 1024),
        name="string",
    )(
        coeffs.reshape(2 * half, nb), projectors, proj_deriv,
        shift_map.reshape(half // 128, 128), atom_of.reshape(ga, cols),
    )
    return transport[None], forces.reshape(128)


def solution(mesh):
    in_specs = (P("ka", None, "ga", None), P(None, "ga", None), P(None, "ga", None), P("ga"), P())
    out_specs = (P("ka", None, None, None), P())
    body = functools.partial(local, mesh.shape["ka"], mesh.shape["ga"])
    return jax.shard_map(body, mesh=mesh, in_specs=in_specs, out_specs=out_specs, check_vma=False)
```

```python
import functools

import jax
import jax.numpy as jnp
from jax import lax
from jax.experimental import pallas as pl
from jax.experimental.pallas import tpu as pltpu
from jax.sharding import PartitionSpec as P

MESH = pl.DeviceIdType.MESH
F32 = jnp.float32
BF16 = jnp.bfloat16
I16 = jnp.int16
BANDS = 64
EARLY = 2


def split(value):
    high = value.astype(BF16)
    low = (value - high.astype(F32)).astype(BF16)
    return high, low


def dot(left, right):
    return jnp.dot(left, right, preferred_element_type=F32)


def dot3(left, right_high, right_low):
    left_high, left_low = split(left)
    return dot(left_high, right_high) + (dot(left_high, right_low) + dot(left_low, right_high))


def join(by_re, by_im):
    rows = by_re.shape[0] // 2
    return by_re[:rows] - by_im[rows:], by_im[:rows] + by_re[rows:]


def cmul(left, right_re, right_im):
    return join(dot3(left, *split(right_re)), dot3(left, *split(right_im)))


def kernel(
    ka, ga, coeffs, proj, deriv, shift, atoms, transport, forces,
    own, moved, lhs, nbt, rhs, part, pieces, scales, in_pieces, in_scales, mpart, mrows, erow, efull,
    xfull, xmate, qhigh, qlow, tin, trow, tfull, fka, fga,
    load_sem, rhs_sem, nb_send, nb_recv, p_send, p_recv, m_send, m_recv, e_send, e_recv,
    x_send, x_recv, t_send, t_recv, g_send, g_recv, h_send, f_send, f_recv, l_send, l_recv, out_sem, ready_sem,
):
    phases = []

    def phase(name):
        if phases:
            phases.pop().__exit__(None, None, None)
        if name:
            phases.append(jax.named_scope(name))
            phases[-1].__enter__()

    phase("start")
    nb = own.shape[1]
    half = own.shape[0] // 2
    cols = part.shape[1] // 2
    rows = nb // ga
    blocks = nb // BANDS
    brows = BANDS // ga
    k = lax.axis_index("ka")
    g = lax.axis_index("ga")
    odd = lax.rem(k, 2)
    mate = k + 1 - 2 * odd

    def ga_at(offset):
        return lax.rem(g + offset, ga)

    def ka_at(offset):
        return lax.rem(k + offset, ka)

    def remote(source, target, send, recv, to_k, to_g):
        return pltpu.make_async_remote_copy(
            src_ref=source, dst_ref=target, send_sem=send, recv_sem=recv,
            device_id={"ka": to_k, "ga": to_g}, device_id_type=MESH)

    own_load = pltpu.make_async_copy(coeffs, own, load_sem)
    own_load.start()

    def rhs_loads(i):
        target = ga_at(1 + i)
        slot = lax.rem(i, 3)
        at = pl.ds(pl.multiple_of(target * cols, cols), cols)
        return (
            pltpu.make_async_copy(proj.at[:, :, at], rhs.at[slot, :, :, pl.ds(0, cols)], rhs_sem.at[slot, 0]),
            pltpu.make_async_copy(deriv.at[:, :, at], rhs.at[slot, :, :, pl.ds(cols, cols)], rhs_sem.at[slot, 1]),
        )

    for i in range(2):
        for copy in rhs_loads(i):
            copy.start()

    phase("barrier")
    barrier = pltpu.get_barrier_semaphore()
    for offset in range(1, ga):
        pl.semaphore_signal(barrier, inc=1, device_id={"ka": k, "ga": ga_at(offset)}, device_id_type=MESH)
    for offset in range(ga):
        pl.semaphore_signal(barrier, inc=1, device_id={"ka": mate, "ga": ga_at(offset)}, device_id_type=MESH)
    for offset in range(1, ka - 1):
        other = lax.rem(lax.max(k, mate) + offset, ka)
        pl.semaphore_signal(barrier, inc=1, device_id={"ka": other, "ga": g}, device_id_type=MESH)
    pl.semaphore_wait(barrier, 2 * ga + ka - 3)

    phase("load")
    own_load.wait()

    phase("lhs")
    for at in range(0, half, 384):
        width = min(384, half - at)
        re = own[at:at + width, :].T
        im = own[half + at:half + at + width, :].T
        lhs[0:nb, at:at + width] = re
        lhs[0:nb, half + at:half + at + width] = im
        lhs[nb:2 * nb, at:at + width] = im
        lhs[nb:2 * nb, half + at:half + at + width] = -re

    def nb_copy(b):
        return remote(lhs.at[pl.ds(b * BANDS, BANDS)], nbt.at[b], nb_send.at[b], nb_recv.at[b], ka_at(ka - 1), g)

    for b in range(blocks):
        nb_copy(b).start()

    def piece_copies(i):
        return (
            remote(pieces.at[i], in_pieces.at[i], p_send.at[i, 0], p_recv.at[i, 0], k, ga_at(1 + i)),
            remote(scales.at[i], in_scales.at[i], p_send.at[i, 1], p_recv.at[i, 1], k, ga_at(1 + i)),
        )

    def project(i, carry):
        for copy in rhs_loads(i):
            copy.wait()

        @pl.when(i + 2 < ga)
        def _():
            for copy in rhs_loads(i + 2):
                copy.start()

        part[...] = dot(lhs[...], rhs[lax.rem(i, 3)].reshape(2 * half, 2 * cols))

        @pl.when(i < ga - 1)
        def _():
            values = part[...]
            top = jnp.maximum(jnp.max(jnp.abs(values), axis=0, keepdims=True), 1e-30)
            pieces[i] = jnp.round(values * (32767.0 / top)).astype(jnp.int32).astype(I16)
            scales[i] = jnp.broadcast_to(top * (1.0 / 32767.0), (8, 2 * cols))

        @pl.when(i < EARLY)
        def _():
            for copy in piece_copies(i):
                copy.start()

        return carry

    def m_copy(b, i):
        target = ga_at(1 + i)
        at = pl.ds(pl.multiple_of(target * brows, brows), brows)
        return remote(mpart.at[b, :, at, :], mrows.at[b, i], m_send.at[b, i], m_recv.at[b, i], k, target)

    def intersect(b):
        phase(f"nb_wait{b}")
        nb_copy(b).wait_recv()
        phase(f"m_dot{b}")
        block = nbt[b]
        swapped = jnp.concatenate([block[:, half:], -block[:, :half]], axis=1)
        mpart[b] = dot(jnp.concatenate([block, swapped], axis=0), own[...]).reshape(2, BANDS, nb)
        for i in range(ga - 1):
            m_copy(b, i).start()

    def e_copy(b, i):
        at = pl.ds(pl.multiple_of(b * BANDS + g * brows, brows), brows)
        return remote(erow.at[b], efull.at[:, at, :], e_send.at[b, i], e_recv.at[b, i], k, ga_at(1 + i))

    def settle(b):
        phase(f"m_rs{b}")
        total = mpart[b, :, pl.ds(pl.multiple_of(g * brows, brows), brows), :]
        for i in range(ga - 1):
            m_copy(b, i).wait_recv()
            total = total + mrows[b, i]
        first = b * BANDS + g * brows
        row_at = lax.broadcasted_iota(jnp.int32, (brows, nb), 0) + first
        col_at = lax.broadcasted_iota(jnp.int32, (brows, nb), 1)
        erow[b, 0] = jnp.where(row_at == col_at, 1.0, 0.0) - total[0]
        erow[b, 1] = -total[1]
        for i in range(ga - 1):
            e_copy(b, i).start()
        efull[:, pl.ds(pl.multiple_of(first, brows), brows), :] = erow[b]

    phase("project0")
    lax.fori_loop(0, 4, project, 0)

    phase("permute")

    @pl.when(k == ka - 1)
    def _():
        wanted = shift[...] - g * half

        def permute(b, carry):
            at = pl.multiple_of(b * 384, 384)
            index = lax.broadcasted_iota(jnp.int32, (384, half), 0) + at
            chosen = jnp.where(wanted == index, 1.0, 0.0).astype(BF16)
            moved[pl.ds(at, 384), :] = dot(chosen, own[0:half, :]).astype(BF16)
            moved[pl.ds(half + at, 384), :] = dot(chosen, own[half:2 * half, :]).astype(BF16)
            return carry

        lax.fori_loop(0, half // 384, permute, 0)
        own[...] = moved[...]

    intersect(0)
    phase("project1")
    lax.fori_loop(4, 6, project, 0)
    intersect(1)
    settle(0)
    phase("project2")
    lax.fori_loop(6, ga, project, 0)
    intersect(2)
    settle(1)
    intersect(3)
    settle(2)
    settle(3)

    phase("token")

    @pl.when(odd == 1)
    def _():
        pl.semaphore_signal(ready_sem, inc=1, device_id={"ka": mate, "ga": g}, device_id_type=MESH)

    @pl.when(odd == 0)
    def _():
        pl.semaphore_wait(ready_sem, 1)

    for i in range(EARLY, ga - 1):
        for copy in piece_copies(i):
            copy.start()

    phase("e_ag")
    for b in range(blocks):
        for i in range(ga - 1):
            e_copy(b, i).wait_recv()

    phase("newton")
    e_re, e_im = efull[0], efull[1]
    both = efull[...].reshape(2 * nb, nb)
    sq_re, sq_im = cmul(both, e_re, e_im)
    eye = jnp.where(
        lax.broadcasted_iota(jnp.int32, (nb, nb), 0) == lax.broadcasted_iota(jnp.int32, (nb, nb), 1), 1.0, 0.0)
    cu_re, cu_im = cmul(both, sq_re, sq_im)
    xfull[0] = (eye + (e_re + (sq_re + cu_re))).T
    xfull[1] = (e_im + (sq_im + cu_im)).T

    phase("chain")
    mine = pl.ds(pl.multiple_of(g * rows, rows), rows)
    x_copy = remote(xfull, xmate, x_send, x_recv, mate, g)
    onward = remote(trow.at[1], tin, t_send, t_recv, ka_at(2), g)

    def same_copy(i):
        return remote(trow.at[1], tfull.at[:, mine, :], g_send.at[i], g_recv.at[i], k, ga_at(i))

    def mate_copy(i):
        return remote(trow.at[0], tfull.at[:, mine, :], h_send.at[i], g_recv.at[i], mate, ga_at(i))

    @pl.when(odd == 0)
    def _():
        x_copy.start()

    @pl.when(odd == 1)
    def _():
        phase("x_wait")
        x_copy.wait_recv()

        def keep(re, im):
            high, low = split(re)
            qhigh[:, 0:nb] = high
            qlow[:, 0:nb] = low
            high, low = split(im)
            qhigh[:, nb:2 * nb] = high
            qlow[:, nb:2 * nb] = low

        def step(left, high, low):
            out = dot3(left, high, low)
            return join(out[:, 0:nb], out[:, nb:2 * nb])

        phase("q")

        @pl.when(k == 1)
        def _():
            keep(xfull[0], xfull[1])
            tin[...] = xmate[:, mine, :]

        @pl.when(k > 1)
        def _():
            keep(*cmul(xmate[...].reshape(2 * nb, nb), xfull[0], xfull[1]))
            phase("t_in")
            onward.wait_recv()

        phase("t_step")
        left = tin[...].reshape(2 * rows, nb)
        re, im = step(left, qhigh[...], qlow[...])
        trow[1, 0] = re
        trow[1, 1] = im

        @pl.when(k < ka - 1)
        def _():
            onward.start()

        for i in range(1, ga):
            same_copy(i).start()
        tfull[:, mine, :] = trow[1]

        phase("t_mate")

        @pl.when(k == 1)
        def _():
            trow[0] = tin[...]

        @pl.when(k > 1)
        def _():
            re, im = cmul(left, xmate[0], xmate[1])
            trow[0, 0] = re
            trow[0, 1] = im

        for i in range(ga):
            mate_copy(i).start()

    phase("p_wait")
    for i in range(ga - 1):
        for copy in piece_copies(i):
            copy.wait_recv()
    phase("p_sum")
    whole = part[...]
    for i in range(ga - 1):
        whole = whole + in_pieces[i].astype(jnp.int32).astype(F32) * in_scales[i, 0:1, :]
    b_both = jnp.concatenate([whole[0:nb, 0:cols].T, whole[nb:2 * nb, 0:cols].T], axis=0)
    d_re = whole[0:nb, cols:2 * cols].T
    d_im = whole[nb:2 * nb, cols:2 * cols].T
    atom_column = jnp.broadcast_to(atoms[pl.ds(g, 1), :].astype(F32), (cols, 128)).T

    phase("t_ag")
    for i in range(1, ga):
        same_copy(i).wait_recv()

    @pl.when(odd == 0)
    def _():
        mate_copy(0).wait_recv()

    phase("w")
    out_copy = pltpu.make_async_copy(tfull, transport, out_sem)
    out_copy.start()
    w_re, w_im = cmul(b_both, tfull[0], tfull[1])
    per_proj = jnp.sum(d_re * w_im - d_im * w_re, axis=1, keepdims=True) * (1.0 / ka)
    atom_ids = lax.broadcasted_iota(jnp.int32, (cols, 128), 1).astype(F32)
    force = jnp.sum(jnp.where(atom_column == atom_ids, per_proj, 0.0), axis=0, keepdims=True)
    fka[k] = jnp.broadcast_to(force, (8, 128))

    def along_ka(i):
        return remote(fka.at[k], fka.at[k], f_send.at[i], f_recv.at[i], ka_at(1 + i), g)

    def along_ga(i):
        return remote(fga.at[g], fga.at[g], l_send.at[i], l_recv.at[i], k, ga_at(1 + i))

    phase("f_ka")
    for i in range(ka - 1):
        along_ka(i).start()
    for i in range(ka - 1):
        along_ka(i).wait_recv()
    phase("f_ga")
    fga[g] = jnp.sum(fka[...], axis=0)
    for i in range(ga - 1):
        along_ga(i).start()
    for i in range(ga - 1):
        along_ga(i).wait_recv()
    forces[...] = jnp.sum(fga[...], axis=0)[0:1]

    phase("drain")
    for b in range(blocks):
        nb_copy(b).wait_send()
        for i in range(ga - 1):
            m_copy(b, i).wait_send()
            e_copy(b, i).wait_send()
    for i in range(ga - 1):
        for copy in piece_copies(i):
            copy.wait_send()
        along_ga(i).wait_send()
    for i in range(ka - 1):
        along_ka(i).wait_send()

    @pl.when(odd == 0)
    def _():
        x_copy.wait_send()

    @pl.when(odd == 1)
    def _():
        for i in range(1, ga):
            same_copy(i).wait_send()
        for i in range(ga):
            mate_copy(i).wait_send()

        @pl.when(k < ka - 1)
        def _():
            onward.wait_send()

    out_copy.wait()
    phase(None)


def local(ka, ga, coeffs, projectors, proj_deriv, shift_map, atom_of):
    _, _, half, nb = coeffs.shape
    np_ = projectors.shape[2]
    cols = np_ // ga
    rows = nb // ga
    blocks = nb // BANDS
    brows = BANDS // ga
    anywhere = pl.BlockSpec(memory_space=pl.ANY)
    vmem = pl.BlockSpec(memory_space=pltpu.VMEM)
    dma = pltpu.SemaphoreType.DMA
    transport, forces = pl.pallas_call(
        functools.partial(kernel, ka, ga),
        out_shape=(jax.ShapeDtypeStruct((2, nb, nb), F32), jax.ShapeDtypeStruct((1, 128), F32)),
        in_specs=[anywhere, anywhere, anywhere, vmem, vmem],
        out_specs=(anywhere, vmem),
        scratch_shapes=[
            pltpu.VMEM((2 * half, nb), BF16),
            pltpu.VMEM((2 * half, nb), BF16),
            pltpu.VMEM((2 * nb, 2 * half), BF16),
            pltpu.VMEM((blocks, BANDS, 2 * half), BF16),
            pltpu.VMEM((3, 2, half, 2 * cols), BF16),
            pltpu.VMEM((2 * nb, 2 * cols), F32),
            pltpu.VMEM((ga - 1, 2 * nb, 2 * cols), I16),
            pltpu.VMEM((ga - 1, 8, 2 * cols), F32),
            pltpu.VMEM((ga - 1, 2 * nb, 2 * cols), I16),
            pltpu.VMEM((ga - 1, 8, 2 * cols), F32),
            pltpu.VMEM((blocks, 2, BANDS, nb), F32),
            pltpu.VMEM((blocks, ga - 1, 2, brows, nb), F32),
            pltpu.VMEM((blocks, 2, brows, nb), F32),
            pltpu.VMEM((2, nb, nb), F32),
            pltpu.VMEM((2, nb, nb), F32),
            pltpu.VMEM((2, nb, nb), F32),
            pltpu.VMEM((nb, 2 * nb), BF16),
            pltpu.VMEM((nb, 2 * nb), BF16),
            pltpu.VMEM((2, rows, nb), F32),
            pltpu.VMEM((2, 2, rows, nb), F32),
            pltpu.VMEM((2, nb, nb), F32),
            pltpu.VMEM((ka, 8, 128), F32),
            pltpu.VMEM((ga, 8, 128), F32),
            dma, dma((3, 2)), dma((blocks,)), dma((blocks,)), dma((ga - 1, 2)), dma((ga - 1, 2)),
            dma((blocks, ga - 1)), dma((blocks, ga - 1)), dma((blocks, ga - 1)), dma((blocks, ga - 1)),
            dma, dma, dma, dma, dma((ga,)), dma((ga,)), dma((ga,)),
            dma((ka - 1,)), dma((ka - 1,)), dma((ga - 1,)), dma((ga - 1,)), dma,
            pltpu.SemaphoreType.REGULAR,
        ],
        compiler_params=pltpu.CompilerParams(
            collective_id=0, has_side_effects=True, vmem_limit_bytes=60 * 1024 * 1024),
        name="string",
    )(
        coeffs.reshape(2 * half, nb), projectors, proj_deriv,
        shift_map.reshape(1, half), atom_of.reshape(ga, cols),
    )
    return transport[None], forces.reshape(128)


def solution(mesh):
    in_specs = (P("ka", None, "ga", None), P(None, "ga", None), P(None, "ga", None), P("ga"), P())
    out_specs = (P("ka", None, None, None), P())
    body = functools.partial(local, mesh.shape["ka"], mesh.shape["ga"])
    return jax.shard_map(body, mesh=mesh, in_specs=in_specs, out_specs=out_specs, check_vma=False)
```

```python
import functools

import jax
import jax.numpy as jnp
from jax import lax
from jax.experimental import pallas as pl
from jax.experimental.pallas import tpu as pltpu
from jax.sharding import PartitionSpec as P

MESH = pl.DeviceIdType.MESH
F32 = jnp.float32
BF16 = jnp.bfloat16
I16 = jnp.int16
BANDS = 64
SHARED = 640
EARLY = 2
LATE = 8


def split(value):
    high = value.astype(BF16)
    low = (value - high.astype(F32)).astype(BF16)
    return high, low


def dot(left, right):
    return jnp.dot(left, right, preferred_element_type=F32)


def dot3(left, right_high, right_low):
    left_high, left_low = split(left)
    return dot(left_high, right_high) + (dot(left_high, right_low) + dot(left_low, right_high))


def join(by_re, by_im):
    rows = by_re.shape[0] // 2
    return by_re[:rows] - by_im[rows:], by_im[:rows] + by_re[rows:]


def cmul(left, right_re, right_im):
    return join(dot3(left, *split(right_re)), dot3(left, *split(right_im)))


def kernel(
    ka, ga, coeffs, proj, deriv, shift, atoms, transport, forces,
    own, moved, lhs, nbt, cnat, taken, taken_rows, taken_sum, taken_in, rhs, part, pieces, scales, in_pieces, in_scales, z_piece, z_scale, z_in, z_in_scale, mpart, mrows, erow, efull,
    xfull, xmate, qhigh, qlow, tin, trow, tfull, fka, fga,
    load_sem, rhs_sem, nb_send, nb_recv, z_send, z_recv, c_send, c_recv, a_send, a_recv, s_send, s_recv, p_send, p_recv, m_send, m_recv, e_send, e_recv,
    x_send, x_recv, t_send, t_recv, g_send, g_recv, h_send, f_send, f_recv, l_send, l_recv, out_sem, ready_sem,
):
    phases = []

    def phase(name):
        if phases:
            phases.pop().__exit__(None, None, None)
        if name:
            phases.append(jax.named_scope(name))
            phases[-1].__enter__()

    phase("start")
    nb = own.shape[1]
    half = own.shape[0] // 2
    cols = part.shape[2] // 2
    rows = nb // ga
    blocks = nb // BANDS
    brows = BANDS // ga
    kept = half - SHARED
    k = lax.axis_index("ka")
    g = lax.axis_index("ga")
    odd = lax.rem(k, 2)
    mate = k + 1 - 2 * odd
    ring = ga // 2
    ring_at, place = g // 2, lax.rem(g, 2)

    def ga_at(offset):
        return lax.rem(g + offset, ga)

    def ka_at(offset):
        return lax.rem(k + offset, ka)

    def remote(source, target, send, recv, to_k, to_g):
        return pltpu.make_async_remote_copy(
            src_ref=source, dst_ref=target, send_sem=send, recv_sem=recv,
            device_id={"ka": to_k, "ga": to_g}, device_id_type=MESH)

    own_load = pltpu.make_async_copy(coeffs, own, load_sem)
    own_load.start()

    def along_ring(step):
        return lax.rem(ring_at + step, ring) * 2

    def block_of(i):
        last = i // 4
        step = (1 - last) * (1 + 2 * lax.rem(i, 2)) + last * (6 - 2 * (i // 2))
        other = (1 - last) * (1 - i // 2) + last * (1 - lax.rem(i, 2))
        return step, other

    def rhs_loads(i):
        step, other = block_of(i)
        target = along_ring(step) + place + other - 2 * place * other
        slot = lax.rem(i, 3)
        at = pl.ds(pl.multiple_of(target * cols, cols), cols)
        return (
            pltpu.make_async_copy(proj.at[:, :, at], rhs.at[slot, :, :, pl.ds(0, cols)], rhs_sem.at[slot, 0]),
            pltpu.make_async_copy(deriv.at[:, :, at], rhs.at[slot, :, :, pl.ds(cols, cols)], rhs_sem.at[slot, 1]),
        )

    for i in range(2):
        for copy in rhs_loads(i):
            copy.start()

    phase("barrier")
    barrier = pltpu.get_barrier_semaphore()
    for offset in range(1, ga):
        pl.semaphore_signal(barrier, inc=1, device_id={"ka": k, "ga": ga_at(offset)}, device_id_type=MESH)
    for offset in range(ga):
        pl.semaphore_signal(barrier, inc=1, device_id={"ka": mate, "ga": ga_at(offset)}, device_id_type=MESH)
    for offset in range(1, ka - 1):
        other = lax.rem(lax.max(k, mate) + offset, ka)
        pl.semaphore_signal(barrier, inc=1, device_id={"ka": other, "ga": g}, device_id_type=MESH)
    pl.semaphore_wait(barrier, 2 * ga + ka - 3)

    phase("load")
    own_load.wait()

    phase("lhs")
    for at in range(0, half, 384):
        width = min(384, half - at)
        re = own[at:at + width, :].T
        im = own[half + at:half + at + width, :].T
        lhs[0:nb, at:at + width] = re
        lhs[0:nb, half + at:half + at + width] = im
        lhs[nb:2 * nb, at:at + width] = im
        lhs[nb:2 * nb, half + at:half + at + width] = -re

    ranges = ((0, kept), (half, kept), (kept, SHARED), (half + kept, SHARED))

    def nb_copy(b, r):
        at = pl.ds(*ranges[r])
        return remote(lhs.at[pl.ds(b * BANDS, BANDS), at], nbt.at[b, :, at], nb_send.at[b, r], nb_recv.at[b, r],
                      ka_at(ka - 1), g)

    plane = ka // 2
    turn = lax.rem(k, plane) == 0

    def nb_start(b):
        for r in range(2):
            nb_copy(b, r).start()

    def nb_turn(b):
        @pl.when(turn)
        def _():
            nb_start(b)

    nb_start(0)
    nb_start(1)

    @pl.when(jnp.logical_not(turn))
    def _():
        nb_start(2)
        nb_start(3)

    @pl.when(odd == 1)
    def _():
        for b in range(blocks):
            for r in range(2, 4):
                nb_copy(b, r).start()

    phase("permute")

    @pl.when(k == ka - 1)
    def _():
        wanted = jnp.concatenate([shift[r:r + 1, :] for r in range(half // 128)], axis=1) - g * half

        def permute(b, carry):
            at = pl.multiple_of(b * 384, 384)
            index = lax.broadcasted_iota(jnp.int32, (384, half), 0) + at
            chosen = jnp.where(wanted == index, 1.0, 0.0).astype(BF16)
            moved[pl.ds(at, 384), :] = dot(chosen, own[0:half, :]).astype(BF16)
            moved[pl.ds(half + at, 384), :] = dot(chosen, own[half:2 * half, :]).astype(BF16)
            return carry

        lax.fori_loop(0, half // 384, permute, 0)
        own[...] = moved[...]

    def c_copy(r):
        return remote(own.at[pl.ds(kept + r * half, SHARED)], cnat.at[r], c_send.at[r], c_recv.at[r], ka_at(1), g)

    @pl.when(odd == 1)
    def _():
        for r in range(2):
            c_copy(r).start()

    def piece_copies(i):
        return (
            remote(pieces.at[i], in_pieces.at[i], p_send.at[i, 0], p_recv.at[i, 0], k, along_ring(block_of(i)[0]) + place),
            remote(scales.at[i], in_scales.at[i], p_send.at[i, 1], p_recv.at[i, 1], k, along_ring(block_of(i)[0]) + place),
        )

    def coded(values):
        top = jnp.maximum(jnp.max(jnp.abs(values), axis=0, keepdims=True), 1e-30)
        code = jnp.round(values * (32767.0 / top)).astype(jnp.int32).astype(I16)
        return code, jnp.broadcast_to(top * (1.0 / 32767.0), (8, 2 * cols))

    def decoded(code, scale):
        return code.astype(jnp.int32).astype(F32) * scale[0:1, :]

    def project(i, carry):
        for copy in rhs_loads(i):
            copy.wait()

        @pl.when(i + 2 < ga)
        def _():
            for copy in rhs_loads(i + 2):
                copy.start()

        part[i] = dot(lhs[...], rhs[lax.rem(i, 3)].reshape(2 * half, 2 * cols))

        @pl.when(i < ga - 2)
        def _():
            code, scale = coded(part[i])
            pieces[i] = code
            scales[i] = scale

        @pl.when(i < EARLY)
        def _():
            for copy in piece_copies(i):
                copy.start()

        return carry

    def m_copy(b, i):
        target = ga_at(1 + i)
        at = pl.ds(pl.multiple_of(target * brows, brows), brows)
        return remote(mpart.at[b, :, at, :], mrows.at[b, i], m_send.at[b, i], m_recv.at[b, i], k, target)

    def intersect(b):
        phase(f"nb_wait{b}")

        def over(count):
            re, im = nbt[b, :, 0:count], nbt[b, :, half:half + count]
            by_re = dot(jnp.concatenate([re, im], axis=0), own[0:count, :])
            by_im = dot(jnp.concatenate([im, -re], axis=0), own[half:half + count, :])
            mpart[b] = (by_re + by_im).reshape(2, BANDS, nb)

        for r in range(2):
            nb_copy(b, r).wait_recv()

        @pl.when(odd == 1)
        def _():
            over(kept)

        @pl.when(odd == 0)
        def _():
            for r in range(2, 4):
                nb_copy(b, r).wait_recv()
            over(half)

        phase(f"m_dot{b}")
        for i in range(ga - 1):
            m_copy(b, i).start()

    def a_copy(i):
        at = pl.ds(pl.multiple_of(ga_at(1 + i) * brows, brows), brows)
        return remote(taken.at[:, :, at, :], taken_rows.at[i], a_send.at[i], a_recv.at[i], k, ga_at(1 + i))

    s_copy = remote(taken_sum, taken_in, s_send, s_recv, ka_at(ka - 1), g)

    def take():
        for r in range(2):
            c_copy(r).wait_recv()
        out = dot(lhs[:, kept:half], cnat[0]) + dot(lhs[:, half + kept:2 * half], cnat[1])
        taken[...] = out.reshape(2, blocks, BANDS, nb)
        for i in range(ga - 1):
            a_copy(i).start()

    def give_back():
        out = taken[:, :, pl.ds(pl.multiple_of(g * brows, brows), brows), :]
        for i in range(ga - 1):
            a_copy(i).wait_recv()
            out = out + taken_rows[i]
        taken_sum[...] = out
        s_copy.start()

    even = jnp.logical_and(odd == 0, k > 0)

    def e_copy(b, i):
        at = pl.ds(pl.multiple_of(b * BANDS + g * brows, brows), brows)
        return remote(erow.at[b], efull.at[:, at, :], e_send.at[b, i], e_recv.at[b, i], k, ga_at(1 + i))

    def settle(b):
        phase(f"m_rs{b}")
        total = mpart[b, :, pl.ds(pl.multiple_of(g * brows, brows), brows), :]
        for i in range(ga - 1):
            m_copy(b, i).wait_recv()
            total = total + mrows[b, i]
        erow[b] = total

        @pl.when(odd == 1)
        def _():
            if b == 0:
                s_copy.wait_recv()
            erow[b] = total + taken_in[:, b]

        total = erow[b]
        first = b * BANDS + g * brows
        row_at = lax.broadcasted_iota(jnp.int32, (brows, nb), 0) + first
        col_at = lax.broadcasted_iota(jnp.int32, (brows, nb), 1)
        erow[b, 0] = jnp.where(row_at == col_at, 1.0, 0.0) - total[0]
        erow[b, 1] = -total[1]
        for i in range(ga - 1):
            e_copy(b, i).start()
        efull[:, pl.ds(pl.multiple_of(first, brows), brows), :] = erow[b]

    phase("project0")
    lax.fori_loop(0, 4, project, 0)

    intersect(0)
    phase("project1")
    lax.fori_loop(4, 6, project, 0)
    intersect(1)
    phase("take")

    @pl.when(even)
    def _():
        take()

    phase("project2")
    lax.fori_loop(6, ga, project, 0)
    nb_turn(2)
    intersect(2)
    intersect(3)
    phase("give_back")

    @pl.when(even)
    def _():
        give_back()

    settle(0)
    nb_turn(3)
    settle(1)
    settle(2)
    settle(3)
    phase("take_last")

    @pl.when(k == 0)
    def _():
        take()
        give_back()

    phase("e_ag")
    for b in range(blocks):
        for i in range(ga - 1):
            e_copy(b, i).wait_recv()

    pl.semaphore_signal(ready_sem, inc=1, device_id={"ka": mate, "ga": g}, device_id_type=MESH)

    phase("newton")
    e_re, e_im = efull[0], efull[1]
    both = efull[...].reshape(2 * nb, nb)
    sq_re, sq_im = cmul(both, e_re, e_im)
    eye = jnp.where(
        lax.broadcasted_iota(jnp.int32, (nb, nb), 0) == lax.broadcasted_iota(jnp.int32, (nb, nb), 1), 1.0, 0.0)
    cu_re, cu_im = cmul(both, sq_re, sq_im)
    xfull[0] = (eye + (e_re + (sq_re + cu_re))).T
    xfull[1] = (e_im + (sq_im + cu_im)).T

    phase("chain")
    mine = pl.ds(pl.multiple_of(g * rows, rows), rows)
    x_copy = remote(xfull, xmate, x_send, x_recv, mate, g)
    onward = remote(trow.at[1], tin, t_send, t_recv, ka_at(2), g)
    first = remote(xfull.at[:, mine, :], tin, t_send, t_recv, 1, g)

    def same_copy(i):
        return remote(trow.at[1], tfull.at[:, mine, :], g_send.at[i], g_recv.at[i], k, ga_at(i))

    def mate_copy(i):
        return remote(trow.at[0], tfull.at[:, mine, :], h_send.at[i], g_recv.at[i], mate, ga_at(i))

    @pl.when(k == 0)
    def _():
        first.start()

    @pl.when(jnp.logical_and(odd == 0, k > 0))
    def _():
        x_copy.start()

    phase("token")
    pl.semaphore_wait(ready_sem, 1)
    for i in range(EARLY, ga - 2):
        for copy in piece_copies(i):
            copy.start()

    z_copies = (
        remote(z_piece, z_in, z_send.at[0], z_recv.at[0], k, ring_at * 2 + 1 - place),
        remote(z_scale, z_in_scale, z_send.at[1], z_recv.at[1], k, ring_at * 2 + 1 - place),
    )

    def sum_ring():
        phase("p_wait")
        for i in range(ga - 2):
            for copy in piece_copies(i):
                copy.wait_recv()
        phase("p_sum")
        out = part[ga - 2]
        for i in (0, 1, 4):
            out = out + decoded(in_pieces[i], in_scales[i])
        code, scale = coded(out)
        z_piece[...] = code
        z_scale[...] = scale
        for copy in z_copies:
            copy.start()
        out = part[ga - 1]
        for i in (2, 3, 5):
            out = out + decoded(in_pieces[i], in_scales[i])
        part[ga - 1] = out

    late = jnp.logical_or(odd == 0, k > LATE)

    @pl.when(late)
    def _():
        sum_ring()

    phase("chain")

    @pl.when(odd == 1)
    def _():
        def keep(re, im):
            high, low = split(re)
            qhigh[:, 0:nb] = high
            qlow[:, 0:nb] = low
            high, low = split(im)
            qhigh[:, nb:2 * nb] = high
            qlow[:, nb:2 * nb] = low

        def step(left, high, low):
            out = dot3(left, high, low)
            return join(out[:, 0:nb], out[:, nb:2 * nb])

        phase("q")

        @pl.when(k == 1)
        def _():
            keep(xfull[0], xfull[1])

        @pl.when(k > 1)
        def _():
            x_copy.wait_recv()
            keep(*cmul(xmate[...].reshape(2 * nb, nb), xfull[0], xfull[1]))

        phase("t_in")
        onward.wait_recv()
        phase("t_step")
        left = tin[...].reshape(2 * rows, nb)
        re, im = step(left, qhigh[...], qlow[...])
        trow[1, 0] = re
        trow[1, 1] = im

        @pl.when(k < ka - 1)
        def _():
            onward.start()

        for i in range(1, ga):
            same_copy(i).start()
        tfull[:, mine, :] = trow[1]

        phase("t_mate")

        @pl.when(k == 1)
        def _():
            trow[0] = tin[...]

        @pl.when(k > 1)
        def _():
            re, im = cmul(left, xmate[0], xmate[1])
            trow[0, 0] = re
            trow[0, 1] = im

        for i in range(ga):
            mate_copy(i).start()

    @pl.when(jnp.logical_not(late))
    def _():
        sum_ring()

    phase("z_wait")
    for copy in z_copies:
        copy.wait_recv()
    phase("z_sum")
    whole = part[ga - 1] + decoded(z_in[...], z_in_scale[...])
    b_both = jnp.concatenate([whole[0:nb, 0:cols].T, whole[nb:2 * nb, 0:cols].T], axis=0)
    d_re = whole[0:nb, cols:2 * cols].T
    d_im = whole[nb:2 * nb, cols:2 * cols].T
    atom_column = jnp.broadcast_to(atoms[pl.ds(g, 1), :].astype(F32), (cols, 128)).T

    phase("t_ag")
    for i in range(1, ga):
        same_copy(i).wait_recv()

    @pl.when(odd == 0)
    def _():
        mate_copy(0).wait_recv()

    phase("w")
    out_copy = pltpu.make_async_copy(tfull, transport, out_sem)
    out_copy.start()
    w_re, w_im = cmul(b_both, tfull[0], tfull[1])
    per_proj = jnp.sum(d_re * w_im - d_im * w_re, axis=1, keepdims=True) * (1.0 / ka)
    atom_ids = lax.broadcasted_iota(jnp.int32, (cols, 128), 1).astype(F32)
    force = jnp.sum(jnp.where(atom_column == atom_ids, per_proj, 0.0), axis=0, keepdims=True)
    fka[k] = jnp.broadcast_to(force, (8, 128))

    def along_ka(i):
        return remote(fka.at[k], fka.at[k], f_send.at[i], f_recv.at[i], ka_at(1 + i), g)

    def along_ga(i):
        return remote(fga.at[g], fga.at[g], l_send.at[i], l_recv.at[i], k, ga_at(1 + i))

    phase("f_ka")
    for i in range(ka - 1):
        along_ka(i).start()
    for i in range(ka - 1):
        along_ka(i).wait_recv()
    phase("f_ga")
    fga[g] = jnp.sum(fka[...], axis=0)
    for i in range(ga - 1):
        along_ga(i).start()
    for i in range(ga - 1):
        along_ga(i).wait_recv()
    forces[...] = jnp.sum(fga[...], axis=0)[0:1]

    phase("drain")
    for b in range(blocks):
        for r in range(2):
            nb_copy(b, r).wait_send()

        @pl.when(odd == 1)
        def _():
            for r in range(2, 4):
                nb_copy(b, r).wait_send()

        for i in range(ga - 1):
            m_copy(b, i).wait_send()
            e_copy(b, i).wait_send()
    for i in range(ga - 2):
        for copy in piece_copies(i):
            copy.wait_send()
    for copy in z_copies:
        copy.wait_send()
    for i in range(ga - 1):
        along_ga(i).wait_send()
    for i in range(ka - 1):
        along_ka(i).wait_send()

    @pl.when(odd == 0)
    def _():
        for i in range(ga - 1):
            a_copy(i).wait_send()
        s_copy.wait_send()

    @pl.when(k == 0)
    def _():
        first.wait_send()

    @pl.when(jnp.logical_and(odd == 0, k > 0))
    def _():
        x_copy.wait_send()

    @pl.when(odd == 1)
    def _():
        for r in range(2):
            c_copy(r).wait_send()
        for i in range(1, ga):
            same_copy(i).wait_send()
        for i in range(ga):
            mate_copy(i).wait_send()

        @pl.when(k < ka - 1)
        def _():
            onward.wait_send()

    out_copy.wait()
    phase(None)


def local(ka, ga, coeffs, projectors, proj_deriv, shift_map, atom_of):
    _, _, half, nb = coeffs.shape
    np_ = projectors.shape[2]
    cols = np_ // ga
    rows = nb // ga
    blocks = nb // BANDS
    brows = BANDS // ga
    anywhere = pl.BlockSpec(memory_space=pl.ANY)
    vmem = pl.BlockSpec(memory_space=pltpu.VMEM)
    dma = pltpu.SemaphoreType.DMA
    transport, forces = pl.pallas_call(
        functools.partial(kernel, ka, ga),
        out_shape=(jax.ShapeDtypeStruct((2, nb, nb), F32), jax.ShapeDtypeStruct((1, 128), F32)),
        in_specs=[anywhere, anywhere, anywhere, vmem, vmem],
        out_specs=(anywhere, vmem),
        scratch_shapes=[
            pltpu.VMEM((2 * half, nb), BF16),
            pltpu.VMEM((2 * half, nb), BF16),
            pltpu.VMEM((2 * nb, 2 * half), BF16),
            pltpu.VMEM((blocks, BANDS, 2 * half), BF16),
            pltpu.VMEM((2, SHARED, nb), BF16),
            pltpu.VMEM((2, blocks, BANDS, nb), F32),
            pltpu.VMEM((ga - 1, 2, blocks, brows, nb), F32),
            pltpu.VMEM((2, blocks, brows, nb), F32),
            pltpu.VMEM((2, blocks, brows, nb), F32),
            pltpu.VMEM((3, 2, half, 2 * cols), BF16),
            pltpu.VMEM((ga, 2 * nb, 2 * cols), F32),
            pltpu.VMEM((ga - 2, 2 * nb, 2 * cols), I16),
            pltpu.VMEM((ga - 2, 8, 2 * cols), F32),
            pltpu.VMEM((ga - 2, 2 * nb, 2 * cols), I16),
            pltpu.VMEM((ga - 2, 8, 2 * cols), F32),
            pltpu.VMEM((2 * nb, 2 * cols), I16),
            pltpu.VMEM((8, 2 * cols), F32),
            pltpu.VMEM((2 * nb, 2 * cols), I16),
            pltpu.VMEM((8, 2 * cols), F32),
            pltpu.VMEM((blocks, 2, BANDS, nb), F32),
            pltpu.VMEM((blocks, ga - 1, 2, brows, nb), F32),
            pltpu.VMEM((blocks, 2, brows, nb), F32),
            pltpu.VMEM((2, nb, nb), F32),
            pltpu.VMEM((2, nb, nb), F32),
            pltpu.VMEM((2, nb, nb), F32),
            pltpu.VMEM((nb, 2 * nb), BF16),
            pltpu.VMEM((nb, 2 * nb), BF16),
            pltpu.VMEM((2, rows, nb), F32),
            pltpu.VMEM((2, 2, rows, nb), F32),
            pltpu.VMEM((2, nb, nb), F32),
            pltpu.VMEM((ka, 8, 128), F32),
            pltpu.VMEM((ga, 8, 128), F32),
            dma, dma((3, 2)), dma((blocks, 4)), dma((blocks, 4)), dma((2,)), dma((2,)),
            dma((2,)), dma((2,)), dma((ga - 1,)), dma((ga - 1,)), dma, dma,
            dma((ga - 2, 2)), dma((ga - 2, 2)),
            dma((blocks, ga - 1)), dma((blocks, ga - 1)), dma((blocks, ga - 1)), dma((blocks, ga - 1)),
            dma, dma, dma, dma, dma((ga,)), dma((ga,)), dma((ga,)),
            dma((ka - 1,)), dma((ka - 1,)), dma((ga - 1,)), dma((ga - 1,)), dma,
            pltpu.SemaphoreType.REGULAR,
        ],
        compiler_params=pltpu.CompilerParams(
            collective_id=0, has_side_effects=True, vmem_limit_bytes=60 * 1024 * 1024),
        name="string",
    )(
        coeffs.reshape(2 * half, nb), projectors, proj_deriv,
        shift_map.reshape(half // 128, 128), atom_of.reshape(ga, cols),
    )
    return transport[None], forces.reshape(128)


def solution(mesh):
    in_specs = (P("ka", None, "ga", None), P(None, "ga", None), P(None, "ga", None), P("ga"), P())
    out_specs = (P("ka", None, None, None), P())
    body = functools.partial(local, mesh.shape["ka"], mesh.shape["ga"])
    return jax.shard_map(body, mesh=mesh, in_specs=in_specs, out_specs=out_specs, check_vma=False)
```

```python
import functools

import jax
import jax.numpy as jnp
from jax import lax
from jax.experimental import pallas as pl
from jax.experimental.pallas import tpu as pltpu
from jax.sharding import PartitionSpec as P

MESH = pl.DeviceIdType.MESH
F32 = jnp.float32
BF16 = jnp.bfloat16
I16 = jnp.int16
BANDS = 64
SHARED = 640
EARLY = 2
MIDDLE = 4
HURRY = 12
LATE = 10


def split(value):
    high = value.astype(BF16)
    low = (value - high.astype(F32)).astype(BF16)
    return high, low


def dot(left, right):
    return jnp.dot(left, right, preferred_element_type=F32)


def dot3(left, right_high, right_low):
    left_high, left_low = split(left)
    return dot(left_high, right_high) + (dot(left_high, right_low) + dot(left_low, right_high))


def join(by_re, by_im):
    rows = by_re.shape[0] // 2
    return by_re[:rows] - by_im[rows:], by_im[:rows] + by_re[rows:]


def cmul(left, right_re, right_im):
    return join(dot3(left, *split(right_re)), dot3(left, *split(right_im)))


def kernel(
    ka, ga, coeffs, proj, deriv, shift, atoms, transport, forces,
    own, moved, lhs, nbt, cnat, taken, taken_rows, taken_sum, taken_in, rhs, part, pieces, scales, in_pieces, in_scales, z_piece, z_scale, z_in, z_in_scale, mpart, mrows, erow, efull,
    xfull, xmate, qhigh, qlow, tin, trow, tcode, tscale, tcodes, tscales, tfull, fka, fga,
    load_sem, rhs_sem, nb_send, nb_recv, z_send, z_recv, c_send, c_recv, a_send, a_recv, s_send, s_recv, p_send, p_recv, m_send, m_recv, e_send, e_recv,
    x_send, x_recv, t_send, t_recv, g_send, g_recv, h_send, f_send, f_recv, l_send, l_recv, out_sem, ready_sem,
):
    phases = []

    def phase(name):
        if phases:
            phases.pop().__exit__(None, None, None)
        if name:
            phases.append(jax.named_scope(name))
            phases[-1].__enter__()

    phase("start")
    nb = own.shape[1]
    half = own.shape[0] // 2
    cols = part.shape[2] // 2
    rows = nb // ga
    blocks = nb // BANDS
    brows = BANDS // ga
    kept = half - SHARED
    k = lax.axis_index("ka")
    g = lax.axis_index("ga")
    odd = lax.rem(k, 2)
    mate = k + 1 - 2 * odd
    ring = ga // 2
    ring_at, place = g // 2, lax.rem(g, 2)

    def ga_at(offset):
        return lax.rem(g + offset, ga)

    def ka_at(offset):
        return lax.rem(k + offset, ka)

    def remote(source, target, send, recv, to_k, to_g):
        return pltpu.make_async_remote_copy(
            src_ref=source, dst_ref=target, send_sem=send, recv_sem=recv,
            device_id={"ka": to_k, "ga": to_g}, device_id_type=MESH)

    own_load = pltpu.make_async_copy(coeffs, own, load_sem)
    own_load.start()

    def along_ring(step):
        return lax.rem(ring_at + step, ring) * 2

    def block_of(i):
        last = i // 4
        step = (1 - last) * (1 + 2 * lax.rem(i, 2)) + last * (6 - 2 * (i // 2))
        other = (1 - last) * (1 - i // 2) + last * (1 - lax.rem(i, 2))
        return step, other

    def rhs_loads(i):
        step, other = block_of(i)
        target = along_ring(step) + place + other - 2 * place * other
        slot = lax.rem(i, 3)
        at = pl.ds(pl.multiple_of(target * cols, cols), cols)
        return (
            pltpu.make_async_copy(proj.at[:, :, at], rhs.at[slot, :, :, pl.ds(0, cols)], rhs_sem.at[slot, 0]),
            pltpu.make_async_copy(deriv.at[:, :, at], rhs.at[slot, :, :, pl.ds(cols, cols)], rhs_sem.at[slot, 1]),
        )

    for i in range(2):
        for copy in rhs_loads(i):
            copy.start()

    phase("barrier")
    barrier = pltpu.get_barrier_semaphore()
    for offset in range(1, ga):
        pl.semaphore_signal(barrier, inc=1, device_id={"ka": k, "ga": ga_at(offset)}, device_id_type=MESH)
    for offset in range(ga):
        pl.semaphore_signal(barrier, inc=1, device_id={"ka": mate, "ga": ga_at(offset)}, device_id_type=MESH)
    for offset in range(1, ka - 1):
        other = lax.rem(lax.max(k, mate) + offset, ka)
        pl.semaphore_signal(barrier, inc=1, device_id={"ka": other, "ga": g}, device_id_type=MESH)
    pl.semaphore_wait(barrier, 2 * ga + ka - 3)

    phase("load")
    own_load.wait()

    phase("lhs")
    for at in range(0, half, 384):
        width = min(384, half - at)
        re = own[at:at + width, :].T
        im = own[half + at:half + at + width, :].T
        lhs[0:nb, at:at + width] = re
        lhs[0:nb, half + at:half + at + width] = im
        lhs[nb:2 * nb, at:at + width] = im
        lhs[nb:2 * nb, half + at:half + at + width] = -re

    ranges = ((0, kept), (half, kept), (kept, SHARED), (half + kept, SHARED))

    def nb_copy(b, r):
        at = pl.ds(*ranges[r])
        return remote(lhs.at[pl.ds(b * BANDS, BANDS), at], nbt.at[b, :, at], nb_send.at[b, r], nb_recv.at[b, r],
                      ka_at(ka - 1), g)

    plane = ka // 2
    turn = lax.rem(k, plane) == 0

    def nb_start(b):
        for r in range(2):
            nb_copy(b, r).start()

    def nb_turn(b):
        @pl.when(turn)
        def _():
            nb_start(b)

    nb_start(0)
    nb_start(1)

    @pl.when(jnp.logical_not(turn))
    def _():
        nb_start(2)
        nb_start(3)

    @pl.when(odd == 1)
    def _():
        for b in range(blocks):
            for r in range(2, 4):
                nb_copy(b, r).start()

    phase("permute")

    @pl.when(k == ka - 1)
    def _():
        wanted = jnp.concatenate([shift[r:r + 1, :] for r in range(half // 128)], axis=1) - g * half

        def permute(b, carry):
            at = pl.multiple_of(b * 384, 384)
            index = lax.broadcasted_iota(jnp.int32, (384, half), 0) + at
            chosen = jnp.where(wanted == index, 1.0, 0.0).astype(BF16)
            moved[pl.ds(at, 384), :] = dot(chosen, own[0:half, :]).astype(BF16)
            moved[pl.ds(half + at, 384), :] = dot(chosen, own[half:2 * half, :]).astype(BF16)
            return carry

        lax.fori_loop(0, half // 384, permute, 0)
        own[...] = moved[...]

    def c_copy(r):
        return remote(own.at[pl.ds(kept + r * half, SHARED)], cnat.at[r], c_send.at[r], c_recv.at[r], ka_at(1), g)

    @pl.when(odd == 1)
    def _():
        for r in range(2):
            c_copy(r).start()

    def piece_copies(i):
        return (
            remote(pieces.at[i], in_pieces.at[i], p_send.at[i, 0], p_recv.at[i, 0], k, along_ring(block_of(i)[0]) + place),
            remote(scales.at[i], in_scales.at[i], p_send.at[i, 1], p_recv.at[i, 1], k, along_ring(block_of(i)[0]) + place),
        )

    def coded(values):
        top = jnp.maximum(jnp.max(jnp.abs(values), axis=0, keepdims=True), 1e-30)
        code = jnp.round(values * (32767.0 / top)).astype(jnp.int32).astype(I16)
        return code, jnp.broadcast_to(top * (1.0 / 32767.0), (8, values.shape[1]))

    def decoded(code, scale):
        return code.astype(jnp.int32).astype(F32) * scale[0:1, :]

    hurry = k < HURRY

    def send(first, last):
        for i in range(first, last):
            for copy in piece_copies(i):
                copy.start()

    def project(i, carry):
        for copy in rhs_loads(i):
            copy.wait()

        @pl.when(i + 2 < ga)
        def _():
            for copy in rhs_loads(i + 2):
                copy.start()

        part[i] = dot(lhs[...], rhs[lax.rem(i, 3)].reshape(2 * half, 2 * cols))

        @pl.when(i < ga - 2)
        def _():
            code, scale = coded(part[i])
            pieces[i] = code
            scales[i] = scale

        @pl.when(i < EARLY)
        def _():
            for copy in piece_copies(i):
                copy.start()

        return carry

    def m_copy(b, i):
        target = ga_at(1 + i)
        at = pl.ds(pl.multiple_of(target * brows, brows), brows)
        return remote(mpart.at[b, :, at, :], mrows.at[b, i], m_send.at[b, i], m_recv.at[b, i], k, target)

    def intersect(b):
        phase(f"nb_wait{b}")

        def over(count):
            re, im = nbt[b, :, 0:count], nbt[b, :, half:half + count]
            by_re = dot(jnp.concatenate([re, im], axis=0), own[0:count, :])
            by_im = dot(jnp.concatenate([im, -re], axis=0), own[half:half + count, :])
            mpart[b] = (by_re + by_im).reshape(2, BANDS, nb)

        for r in range(2):
            nb_copy(b, r).wait_recv()

        @pl.when(odd == 1)
        def _():
            over(kept)

        @pl.when(odd == 0)
        def _():
            for r in range(2, 4):
                nb_copy(b, r).wait_recv()
            over(half)

        phase(f"m_dot{b}")
        for i in range(ga - 1):
            m_copy(b, i).start()

    def a_copy(i):
        at = pl.ds(pl.multiple_of(ga_at(1 + i) * brows, brows), brows)
        return remote(taken.at[:, :, at, :], taken_rows.at[i], a_send.at[i], a_recv.at[i], k, ga_at(1 + i))

    s_copy = remote(taken_sum, taken_in, s_send, s_recv, ka_at(ka - 1), g)

    def take():
        for r in range(2):
            c_copy(r).wait_recv()
        out = dot(lhs[:, kept:half], cnat[0]) + dot(lhs[:, half + kept:2 * half], cnat[1])
        taken[...] = out.reshape(2, blocks, BANDS, nb)
        for i in range(ga - 1):
            a_copy(i).start()

    def give_back():
        out = taken[:, :, pl.ds(pl.multiple_of(g * brows, brows), brows), :]
        for i in range(ga - 1):
            a_copy(i).wait_recv()
            out = out + taken_rows[i]
        taken_sum[...] = out
        s_copy.start()

    even = jnp.logical_and(odd == 0, k > 0)

    def e_copy(b, i):
        at = pl.ds(pl.multiple_of(b * BANDS + g * brows, brows), brows)
        return remote(erow.at[b], efull.at[:, at, :], e_send.at[b, i], e_recv.at[b, i], k, ga_at(1 + i))

    def settle(b):
        phase(f"m_rs{b}")
        total = mpart[b, :, pl.ds(pl.multiple_of(g * brows, brows), brows), :]
        for i in range(ga - 1):
            m_copy(b, i).wait_recv()
            total = total + mrows[b, i]
        erow[b] = total

        @pl.when(odd == 1)
        def _():
            if b == 0:
                s_copy.wait_recv()
            erow[b] = total + taken_in[:, b]

        total = erow[b]
        first = b * BANDS + g * brows
        row_at = lax.broadcasted_iota(jnp.int32, (brows, nb), 0) + first
        col_at = lax.broadcasted_iota(jnp.int32, (brows, nb), 1)
        erow[b, 0] = jnp.where(row_at == col_at, 1.0, 0.0) - total[0]
        erow[b, 1] = -total[1]
        for i in range(ga - 1):
            e_copy(b, i).start()
        efull[:, pl.ds(pl.multiple_of(first, brows), brows), :] = erow[b]

    phase("project0")
    lax.fori_loop(0, 4, project, 0)

    intersect(0)
    phase("project1")
    lax.fori_loop(4, 6, project, 0)
    intersect(1)
    phase("take")

    @pl.when(even)
    def _():
        take()

    send(EARLY, MIDDLE)
    phase("project2")
    lax.fori_loop(6, ga, project, 0)
    intersect(2)
    intersect(3)
    nb_turn(2)
    nb_turn(3)
    phase("give_back")

    @pl.when(even)
    def _():
        give_back()

    @pl.when(jnp.logical_not(hurry))
    def _():
        send(MIDDLE, ga - 2)

    settle(0)
    settle(1)
    settle(2)
    settle(3)
    phase("take_last")

    @pl.when(k == 0)
    def _():
        take()

    phase("e_ag")
    for b in range(blocks):
        for i in range(ga - 1):
            e_copy(b, i).wait_recv()

    @pl.when(hurry)
    def _():
        pl.semaphore_signal(ready_sem, inc=1, device_id={"ka": mate, "ga": g}, device_id_type=MESH)

    phase("newton")
    e_re, e_im = efull[0], efull[1]
    both = efull[...].reshape(2 * nb, nb)
    sq_re, sq_im = cmul(both, e_re, e_im)
    eye = jnp.where(
        lax.broadcasted_iota(jnp.int32, (nb, nb), 0) == lax.broadcasted_iota(jnp.int32, (nb, nb), 1), 1.0, 0.0)
    cu_re, cu_im = cmul(both, sq_re, sq_im)
    xfull[0] = (eye + (e_re + (sq_re + cu_re))).T
    xfull[1] = (e_im + (sq_im + cu_im)).T

    phase("chain")
    mine = pl.ds(pl.multiple_of(g * rows, rows), rows)
    x_copy = remote(xfull, xmate, x_send, x_recv, mate, g)
    onward = remote(trow.at[1], tin, t_send, t_recv, ka_at(2), g)
    first = remote(xfull.at[:, mine, :], tin, t_send, t_recv, 1, g)

    def same_copy(i):
        return (
            remote(tcode.at[1], tcodes.at[g], g_send.at[i, 0], g_recv.at[i, 0], k, ga_at(i)),
            remote(tscale.at[1], tscales.at[g], g_send.at[i, 1], g_recv.at[i, 1], k, ga_at(i)),
        )

    def mate_copy(i):
        return (
            remote(tcode.at[0], tcodes.at[g], h_send.at[i, 0], g_recv.at[i, 0], mate, ga_at(i)),
            remote(tscale.at[0], tscales.at[g], h_send.at[i, 1], g_recv.at[i, 1], mate, ga_at(i)),
        )

    def encode(which):
        code, scale = coded(trow[which].reshape(2 * rows, nb))
        tcode[which] = code
        tscale[which] = scale

    @pl.when(k == 0)
    def _():
        first.start()
        give_back()

    @pl.when(jnp.logical_and(odd == 0, k > 0))
    def _():
        x_copy.start()

    phase("token")
    @pl.when(hurry)
    def _():
        pl.semaphore_wait(ready_sem, 1)
        send(MIDDLE, ga - 2)

    z_copies = (
        remote(z_piece, z_in, z_send.at[0], z_recv.at[0], k, ring_at * 2 + 1 - place),
        remote(z_scale, z_in_scale, z_send.at[1], z_recv.at[1], k, ring_at * 2 + 1 - place),
    )

    def sum_ring():
        phase("p_wait")
        for i in range(ga - 2):
            for copy in piece_copies(i):
                copy.wait_recv()
        phase("p_sum")
        out = part[ga - 2]
        for i in (0, 1, 4):
            out = out + decoded(in_pieces[i], in_scales[i])
        code, scale = coded(out)
        z_piece[...] = code
        z_scale[...] = scale
        for copy in z_copies:
            copy.start()
        out = part[ga - 1]
        for i in (2, 3, 5):
            out = out + decoded(in_pieces[i], in_scales[i])
        part[ga - 1] = out

    late = jnp.logical_or(odd == 0, k > LATE)

    @pl.when(late)
    def _():
        sum_ring()

    phase("chain")

    @pl.when(odd == 1)
    def _():
        def keep(re, im):
            high, low = split(re)
            qhigh[:, 0:nb] = high
            qlow[:, 0:nb] = low
            high, low = split(im)
            qhigh[:, nb:2 * nb] = high
            qlow[:, nb:2 * nb] = low

        def step(left, high, low):
            out = dot3(left, high, low)
            return join(out[:, 0:nb], out[:, nb:2 * nb])

        phase("q")

        @pl.when(k == 1)
        def _():
            keep(xfull[0], xfull[1])

        @pl.when(k > 1)
        def _():
            x_copy.wait_recv()
            keep(*cmul(xmate[...].reshape(2 * nb, nb), xfull[0], xfull[1]))

        phase("t_in")
        onward.wait_recv()
        phase("t_step")
        left = tin[...].reshape(2 * rows, nb)
        re, im = step(left, qhigh[...], qlow[...])
        trow[1, 0] = re
        trow[1, 1] = im

        @pl.when(k < ka - 1)
        def _():
            onward.start()

        encode(1)
        for i in range(1, ga):
            for copy in same_copy(i):
                copy.start()
        tcodes[g] = tcode[1]
        tscales[g] = tscale[1]

        phase("t_mate")

        @pl.when(k == 1)
        def _():
            trow[0] = tin[...]

        @pl.when(k > 1)
        def _():
            re, im = cmul(left, xmate[0], xmate[1])
            trow[0, 0] = re
            trow[0, 1] = im

        encode(0)
        for i in range(ga):
            for copy in mate_copy(i):
                copy.start()

    @pl.when(jnp.logical_not(late))
    def _():
        sum_ring()

    phase("z_wait")
    for copy in z_copies:
        copy.wait_recv()
    phase("z_sum")
    whole = part[ga - 1] + decoded(z_in[...], z_in_scale[...])
    b_both = jnp.concatenate([whole[0:nb, 0:cols].T, whole[nb:2 * nb, 0:cols].T], axis=0)
    d_re = whole[0:nb, cols:2 * cols].T
    d_im = whole[nb:2 * nb, cols:2 * cols].T
    atom_column = jnp.broadcast_to(atoms[pl.ds(g, 1), :].astype(F32), (cols, 128)).T

    phase("t_ag")
    for i in range(1, ga):
        for copy in same_copy(i):
            copy.wait_recv()

    @pl.when(odd == 0)
    def _():
        for copy in mate_copy(0):
            copy.wait_recv()

    for i in range(ga):
        tfull[:, i * rows:(i + 1) * rows, :] = decoded(tcodes[i], tscales[i]).reshape(2, rows, nb)

    phase("w")
    out_copy = pltpu.make_async_copy(tfull, transport, out_sem)
    out_copy.start()
    w_re, w_im = cmul(b_both, tfull[0], tfull[1])
    per_proj = jnp.sum(d_re * w_im - d_im * w_re, axis=1, keepdims=True) * (1.0 / ka)
    atom_ids = lax.broadcasted_iota(jnp.int32, (cols, 128), 1).astype(F32)
    force = jnp.sum(jnp.where(atom_column == atom_ids, per_proj, 0.0), axis=0, keepdims=True)
    fka[k] = force

    def along_ka(i):
        return remote(fka.at[k], fka.at[k], f_send.at[i], f_recv.at[i], ka_at(1 + i), g)

    def along_ga(i):
        return remote(fga.at[g], fga.at[g], l_send.at[i], l_recv.at[i], k, ga_at(1 + i))

    phase("f_ka")
    for i in range(ka - 1):
        along_ka(i).start()
    for i in range(ka - 1):
        along_ka(i).wait_recv()
    phase("f_ga")
    fga[g] = jnp.sum(fka[...], axis=0)
    for i in range(ga - 1):
        along_ga(i).start()
    for i in range(ga - 1):
        along_ga(i).wait_recv()
    forces[...] = jnp.sum(fga[...], axis=0)

    phase("drain")
    for b in range(blocks):
        for r in range(2):
            nb_copy(b, r).wait_send()

        @pl.when(odd == 1)
        def _():
            for r in range(2, 4):
                nb_copy(b, r).wait_send()

        for i in range(ga - 1):
            m_copy(b, i).wait_send()
            e_copy(b, i).wait_send()
    for i in range(ga - 2):
        for copy in piece_copies(i):
            copy.wait_send()
    for copy in z_copies:
        copy.wait_send()
    for i in range(ga - 1):
        along_ga(i).wait_send()
    for i in range(ka - 1):
        along_ka(i).wait_send()

    @pl.when(odd == 0)
    def _():
        for i in range(ga - 1):
            a_copy(i).wait_send()
        s_copy.wait_send()

    @pl.when(k == 0)
    def _():
        first.wait_send()

    @pl.when(jnp.logical_and(odd == 0, k > 0))
    def _():
        x_copy.wait_send()

    @pl.when(odd == 1)
    def _():
        for r in range(2):
            c_copy(r).wait_send()
        for i in range(1, ga):
            for copy in same_copy(i):
                copy.wait_send()
        for i in range(ga):
            for copy in mate_copy(i):
                copy.wait_send()

        @pl.when(k < ka - 1)
        def _():
            onward.wait_send()

    out_copy.wait()
    phase(None)


def local(ka, ga, coeffs, projectors, proj_deriv, shift_map, atom_of):
    _, _, half, nb = coeffs.shape
    np_ = projectors.shape[2]
    cols = np_ // ga
    rows = nb // ga
    blocks = nb // BANDS
    brows = BANDS // ga
    anywhere = pl.BlockSpec(memory_space=pl.ANY)
    vmem = pl.BlockSpec(memory_space=pltpu.VMEM)
    dma = pltpu.SemaphoreType.DMA
    transport, forces = pl.pallas_call(
        functools.partial(kernel, ka, ga),
        out_shape=(jax.ShapeDtypeStruct((2, nb, nb), F32), jax.ShapeDtypeStruct((1, 128), F32)),
        in_specs=[anywhere, anywhere, anywhere, vmem, vmem],
        out_specs=(anywhere, vmem),
        scratch_shapes=[
            pltpu.VMEM((2 * half, nb), BF16),
            pltpu.VMEM((2 * half, nb), BF16),
            pltpu.VMEM((2 * nb, 2 * half), BF16),
            pltpu.VMEM((blocks, BANDS, 2 * half), BF16),
            pltpu.VMEM((2, SHARED, nb), BF16),
            pltpu.VMEM((2, blocks, BANDS, nb), F32),
            pltpu.VMEM((ga - 1, 2, blocks, brows, nb), F32),
            pltpu.VMEM((2, blocks, brows, nb), F32),
            pltpu.VMEM((2, blocks, brows, nb), F32),
            pltpu.VMEM((3, 2, half, 2 * cols), BF16),
            pltpu.VMEM((ga, 2 * nb, 2 * cols), F32),
            pltpu.VMEM((ga - 2, 2 * nb, 2 * cols), I16),
            pltpu.VMEM((ga - 2, 8, 2 * cols), F32),
            pltpu.VMEM((ga - 2, 2 * nb, 2 * cols), I16),
            pltpu.VMEM((ga - 2, 8, 2 * cols), F32),
            pltpu.VMEM((2 * nb, 2 * cols), I16),
            pltpu.VMEM((8, 2 * cols), F32),
            pltpu.VMEM((2 * nb, 2 * cols), I16),
            pltpu.VMEM((8, 2 * cols), F32),
            pltpu.VMEM((blocks, 2, BANDS, nb), F32),
            pltpu.VMEM((blocks, ga - 1, 2, brows, nb), F32),
            pltpu.VMEM((blocks, 2, brows, nb), F32),
            pltpu.VMEM((2, nb, nb), F32),
            pltpu.VMEM((2, nb, nb), F32),
            pltpu.VMEM((2, nb, nb), F32),
            pltpu.VMEM((nb, 2 * nb), BF16),
            pltpu.VMEM((nb, 2 * nb), BF16),
            pltpu.VMEM((2, rows, nb), F32),
            pltpu.VMEM((2, 2, rows, nb), F32),
            pltpu.VMEM((2, 2 * rows, nb), I16),
            pltpu.VMEM((2, 8, nb), F32),
            pltpu.VMEM((ga, 2 * rows, nb), I16),
            pltpu.VMEM((ga, 8, nb), F32),
            pltpu.VMEM((2, nb, nb), F32),
            pltpu.VMEM((ka, 1, 128), F32),
            pltpu.VMEM((ga, 1, 128), F32),
            dma, dma((3, 2)), dma((blocks, 4)), dma((blocks, 4)), dma((2,)), dma((2,)),
            dma((2,)), dma((2,)), dma((ga - 1,)), dma((ga - 1,)), dma, dma,
            dma((ga - 2, 2)), dma((ga - 2, 2)),
            dma((blocks, ga - 1)), dma((blocks, ga - 1)), dma((blocks, ga - 1)), dma((blocks, ga - 1)),
            dma, dma, dma, dma, dma((ga, 2)), dma((ga, 2)), dma((ga, 2)),
            dma((ka - 1,)), dma((ka - 1,)), dma((ga - 1,)), dma((ga - 1,)), dma,
            pltpu.SemaphoreType.REGULAR,
        ],
        compiler_params=pltpu.CompilerParams(
            collective_id=0, has_side_effects=True, vmem_limit_bytes=60 * 1024 * 1024),
        name="string",
    )(
        coeffs.reshape(2 * half, nb), projectors, proj_deriv,
        shift_map.reshape(half // 128, 128), atom_of.reshape(ga, cols),
    )
    return transport[None], forces.reshape(128)


def solution(mesh):
    in_specs = (P("ka", None, "ga", None), P(None, "ga", None), P(None, "ga", None), P("ga"), P())
    out_specs = (P("ka", None, None, None), P())
    body = functools.partial(local, mesh.shape["ka"], mesh.shape["ga"])
    return jax.shard_map(body, mesh=mesh, in_specs=in_specs, out_specs=out_specs, check_vma=False)
```

```python
import functools

import jax
import jax.numpy as jnp
from jax import lax
from jax.experimental import pallas as pl
from jax.experimental.pallas import tpu as pltpu
from jax.sharding import PartitionSpec as P

MESH = pl.DeviceIdType.MESH
F32 = jnp.float32
BF16 = jnp.bfloat16
I16 = jnp.int16
BANDS = 64
SHARED = 640
TURNED = 1024
EARLY = 2
FIRST = 4
HURRY = 12
LATE = 10


def split(value):
    high = value.astype(BF16)
    low = (value - high.astype(F32)).astype(BF16)
    return high, low


def dot(left, right):
    return jnp.dot(left, right, preferred_element_type=F32)


def dot3(left, right_high, right_low):
    left_high, left_low = split(left)
    return dot(left_high, right_high) + (dot(left_high, right_low) + dot(left_low, right_high))


def join(by_re, by_im):
    rows = by_re.shape[0] // 2
    return by_re[:rows] - by_im[rows:], by_im[:rows] + by_re[rows:]


def cmul(left, right_re, right_im):
    return join(dot3(left, *split(right_re)), dot3(left, *split(right_im)))


def kernel(
    ka, ga, coeffs, proj, deriv, shift, atoms, transport, forces,
    own, moved, lhs, nbt, cnat, taken, taken_rows, taken_sum, taken_in, rhs, part, pieces, scales, in_pieces, in_scales, z_piece, z_scale, z_in, z_in_scale, mpart, mrows, erow, ecode, escale, ecodes, escales, efull,
    xfull, xmate, qhigh, qlow, tin, trow, tcode, tscale, tcodes, tscales, tfull, fka, fga,
    load_sem, rhs_sem, nb_send, nb_recv, z_send, z_recv, c_send, c_recv, a_send, a_recv, s_send, s_recv, p_send, p_recv, m_send, m_recv, e_send, e_recv,
    x_send, x_recv, t_send, t_recv, g_send, g_recv, h_send, f_send, f_recv, l_send, l_recv, out_sem, ready_sem,
):
    phases = []

    def phase(name):
        if phases:
            phases.pop().__exit__(None, None, None)
        if name:
            phases.append(jax.named_scope(name))
            phases[-1].__enter__()

    phase("start")
    nb = own.shape[1]
    half = own.shape[0] // 2
    cols = part.shape[2] // 2
    rows = nb // ga
    blocks = nb // BANDS
    brows = BANDS // ga
    kept = half - SHARED
    least = half - TURNED
    k = lax.axis_index("ka")
    g = lax.axis_index("ga")
    odd = lax.rem(k, 2)
    mate = k + 1 - 2 * odd
    ring = ga // 2
    ring_at, place = g // 2, lax.rem(g, 2)

    def ga_at(offset):
        return lax.rem(g + offset, ga)

    def ka_at(offset):
        return lax.rem(k + offset, ka)

    def remote(source, target, send, recv, to_k, to_g):
        return pltpu.make_async_remote_copy(
            src_ref=source, dst_ref=target, send_sem=send, recv_sem=recv,
            device_id={"ka": to_k, "ga": to_g}, device_id_type=MESH)

    own_load = pltpu.make_async_copy(coeffs, own, load_sem)
    own_load.start()

    def along_ring(step):
        return lax.rem(ring_at + step, ring) * 2

    def block_of(i):
        last = i // 4
        step = (1 - last) * (1 + 2 * lax.rem(i, 2)) + last * (6 - 2 * (i // 2))
        other = (1 - last) * (1 - i // 2) + last * (1 - lax.rem(i, 2))
        return step, other

    def rhs_loads(i):
        step, other = block_of(i)
        target = along_ring(step) + place + other - 2 * place * other
        slot = lax.rem(i, 3)
        at = pl.ds(pl.multiple_of(target * cols, cols), cols)
        return (
            pltpu.make_async_copy(proj.at[:, :, at], rhs.at[slot, :, :, pl.ds(0, cols)], rhs_sem.at[slot, 0]),
            pltpu.make_async_copy(deriv.at[:, :, at], rhs.at[slot, :, :, pl.ds(cols, cols)], rhs_sem.at[slot, 1]),
        )

    for i in range(2):
        for copy in rhs_loads(i):
            copy.start()

    phase("barrier")
    barrier = pltpu.get_barrier_semaphore()
    for offset in range(1, ga):
        pl.semaphore_signal(barrier, inc=1, device_id={"ka": k, "ga": ga_at(offset)}, device_id_type=MESH)
    for offset in range(ga):
        pl.semaphore_signal(barrier, inc=1, device_id={"ka": mate, "ga": ga_at(offset)}, device_id_type=MESH)
    for offset in range(1, ka - 1):
        other = lax.rem(lax.max(k, mate) + offset, ka)
        pl.semaphore_signal(barrier, inc=1, device_id={"ka": other, "ga": g}, device_id_type=MESH)
    pl.semaphore_wait(barrier, 2 * ga + ka - 3)

    phase("load")
    own_load.wait()

    phase("lhs")
    for at in range(0, half, 384):
        width = min(384, half - at)
        re = own[at:at + width, :].T
        im = own[half + at:half + at + width, :].T
        lhs[0:nb, at:at + width] = re
        lhs[0:nb, half + at:half + at + width] = im
        lhs[nb:2 * nb, at:at + width] = im
        lhs[nb:2 * nb, half + at:half + at + width] = -re

    plane = ka // 2
    turn_back = lax.rem(k, plane) == 0
    turn_on = lax.rem(k, plane) == plane - 1
    ranges = tuple(
        (part_at + first, last - first) for first, last in ((0, least), (least, kept), (kept, half)) for part_at in (0, half))

    def nb_copy(b, r):
        at = pl.ds(*ranges[r])
        return remote(lhs.at[pl.ds(b * BANDS, BANDS), at], nbt.at[b, :, at], nb_send.at[b, r], nb_recv.at[b, r],
                      ka_at(ka - 1), g)

    def nb_each(act, b, sent):
        short = turn_back if sent else turn_on
        whole = odd == 1 if sent else odd == 0
        for r in (0, 1):
            act(nb_copy(b, r))

        @pl.when(jnp.logical_not(short))
        def _():
            for r in (2, 3):
                act(nb_copy(b, r))

        @pl.when(whole)
        def _():
            for r in (4, 5):
                act(nb_copy(b, r))

    for b in range(blocks):
        nb_each(lambda copy: copy.start(), b, True)

    phase("permute")

    @pl.when(k == ka - 1)
    def _():
        wanted = jnp.concatenate([shift[r:r + 1, :] for r in range(half // 128)], axis=1) - g * half

        def permute(b, carry):
            at = pl.multiple_of(b * 384, 384)
            index = lax.broadcasted_iota(jnp.int32, (384, half), 0) + at
            chosen = jnp.where(wanted == index, 1.0, 0.0).astype(BF16)
            moved[pl.ds(at, 384), :] = dot(chosen, own[0:half, :]).astype(BF16)
            moved[pl.ds(half + at, 384), :] = dot(chosen, own[half:2 * half, :]).astype(BF16)
            return carry

        lax.fori_loop(0, half // 384, permute, 0)
        own[...] = moved[...]

    def c_copy(r):
        first, count = ranges[2 + r]
        part_at = half * (r % 2)
        return remote(own.at[pl.ds(first, count)], cnat.at[r % 2, pl.ds(first - part_at - least, count)],
                      c_send.at[r], c_recv.at[r], ka_at(1), g)

    def c_each(act, short):
        for r in (2, 3):
            act(c_copy(r))

        @pl.when(short)
        def _():
            for r in (0, 1):
                act(c_copy(r))

    @pl.when(odd == 1)
    def _():
        c_each(lambda copy: copy.start(), turn_on)

    def piece_to(i):
        across = (i // 4) * (1 - lax.rem(i, 2))
        return along_ring((1 - across) * block_of(i)[0]) + place + across * (1 - 2 * place)

    def piece_copies(i):
        return (
            remote(pieces.at[i], in_pieces.at[i], p_send.at[i, 0], p_recv.at[i, 0], k, piece_to(i)),
            remote(scales.at[i], in_scales.at[i], p_send.at[i, 1], p_recv.at[i, 1], k, piece_to(i)),
        )

    def coded(values):
        top = jnp.maximum(jnp.max(jnp.abs(values), axis=0, keepdims=True), 1e-30)
        code = jnp.round(values * (32767.0 / top)).astype(jnp.int32).astype(I16)
        return code, top * (1.0 / 32767.0)

    def decoded(code, scale):
        return code.astype(jnp.int32).astype(F32) * scale

    hurry = k < HURRY

    def combine():
        for copy in piece_copies(4):
            copy.wait_recv()
        code, scale = coded(part[5] + decoded(in_pieces[4], in_scales[4]))
        pieces[5] = code
        scales[5] = scale

    def send(first, last):
        for i in range(first, last):
            for copy in piece_copies(i):
                copy.start()

    def project(i, carry):
        for copy in rhs_loads(i):
            copy.wait()

        @pl.when(i + 2 < ga)
        def _():
            for copy in rhs_loads(i + 2):
                copy.start()

        part[i] = dot(lhs[...], rhs[lax.rem(i, 3)].reshape(2 * half, 2 * cols))

        @pl.when(i < ga - 3)
        def _():
            code, scale = coded(part[i])
            pieces[i] = code
            scales[i] = scale

        @pl.when(i < EARLY)
        def _():
            for copy in piece_copies(i):
                copy.start()

        return carry

    def m_copy(b, i):
        target = ga_at(1 + i)
        at = pl.ds(pl.multiple_of(target * brows, brows), brows)
        return remote(mpart.at[b, :, at, :], mrows.at[b, i], m_send.at[b, i], m_recv.at[b, i], k, target)

    def intersect(b):
        phase(f"nb_wait{b}")

        def over(count):
            re, im = nbt[b, :, 0:count], nbt[b, :, half:half + count]
            by_re = dot(jnp.concatenate([re, im], axis=0), own[0:count, :])
            by_im = dot(jnp.concatenate([im, -re], axis=0), own[half:half + count, :])
            mpart[b] = (by_re + by_im).reshape(2, BANDS, nb)

        nb_each(lambda copy: copy.wait_recv(), b, False)

        @pl.when(turn_on)
        def _():
            over(least)

        @pl.when(jnp.logical_and(odd == 1, jnp.logical_not(turn_on)))
        def _():
            over(kept)

        @pl.when(odd == 0)
        def _():
            over(half)

        phase(f"m_dot{b}")
        for i in range(ga - 1):
            m_copy(b, i).start()

    def a_copy(i):
        at = pl.ds(pl.multiple_of(ga_at(1 + i) * brows, brows), brows)
        return remote(taken.at[:, :, at, :], taken_rows.at[i], a_send.at[i], a_recv.at[i], k, ga_at(1 + i))

    s_copy = remote(taken_sum, taken_in, s_send, s_recv, ka_at(ka - 1), g)

    def take():
        c_each(lambda copy: copy.wait_recv(), turn_back)

        def from_wave(first):
            out = dot(lhs[:, first:half], cnat[0, first - least:])
            out = out + dot(lhs[:, half + first:2 * half], cnat[1, first - least:])
            taken[...] = out.reshape(2, blocks, BANDS, nb)

        @pl.when(turn_back)
        def _():
            from_wave(least)

        @pl.when(jnp.logical_not(turn_back))
        def _():
            from_wave(kept)

        for i in range(ga - 1):
            a_copy(i).start()

    def give_back():
        out = taken[:, :, pl.ds(pl.multiple_of(g * brows, brows), brows), :]
        for i in range(ga - 1):
            a_copy(i).wait_recv()
            out = out + taken_rows[i]
        taken_sum[...] = out
        s_copy.start()

    even = jnp.logical_and(odd == 0, k > 0)

    spans = ((0, blocks - 1), (blocks - 1, blocks))

    def span_rows(span):
        return pl.ds(2 * brows * spans[span][0], 2 * brows * (spans[span][1] - spans[span][0]))

    def e_copies(span, i):
        to = ga_at(1 + i)
        return (
            remote(ecode.at[span_rows(span)], ecodes.at[g, span_rows(span)], e_send.at[span, i, 0], e_recv.at[span, i, 0], k, to),
            remote(escale.at[span], escales.at[span, g], e_send.at[span, i, 1], e_recv.at[span, i, 1], k, to),
        )

    def spread(span):
        first, last = spans[span]
        code, scale = coded(erow[first:last].reshape(2 * brows * (last - first), nb))
        ecode[span_rows(span), :] = code
        escale[span] = scale
        for i in range(ga - 1):
            for copy in e_copies(span, i):
                copy.start()
        ecodes[g, span_rows(span), :] = code
        escales[span, g] = scale

    def settle(b):
        phase(f"m_rs{b}")
        total = mpart[b, :, pl.ds(pl.multiple_of(g * brows, brows), brows), :]
        for i in range(ga - 1):
            m_copy(b, i).wait_recv()
            total = total + mrows[b, i]
        erow[b] = total

        @pl.when(odd == 1)
        def _():
            if b == 0:
                s_copy.wait_recv()
            erow[b] = total + taken_in[:, b]

        total = erow[b]
        first = b * BANDS + g * brows
        row_at = lax.broadcasted_iota(jnp.int32, (brows, nb), 0) + first
        col_at = lax.broadcasted_iota(jnp.int32, (brows, nb), 1)
        erow[b, 0] = jnp.where(row_at == col_at, 1.0, 0.0) - total[0]
        erow[b, 1] = -total[1]

    phase("project0")
    lax.fori_loop(0, 4, project, 0)

    intersect(0)
    phase("project1")
    lax.fori_loop(4, 6, project, 0)
    intersect(1)
    phase("take")

    @pl.when(even)
    def _():
        take()


    @pl.when(k >= FIRST)
    def _():
        send(EARLY, 4)

    phase("project2")
    lax.fori_loop(6, ga, project, 0)
    intersect(2)
    intersect(3)
    phase("give_back")

    @pl.when(even)
    def _():
        give_back()

    @pl.when(k >= FIRST)
    def _():
        send(4, 5)

    settle(0)
    settle(1)
    settle(2)
    spread(0)
    settle(3)
    spread(1)
    phase("combine")

    @pl.when(k >= FIRST)
    def _():
        combine()

    @pl.when(jnp.logical_not(hurry))
    def _():
        send(5, 6)

    phase("take_last")

    @pl.when(k == 0)
    def _():
        take()

    phase("e_ag")
    for span in range(2):
        for i in range(ga - 1):
            for copy in e_copies(span, i):
                copy.wait_recv()
    for i in range(ga):
        for b in range(blocks):
            span = b // (blocks - 1)
            code = ecodes[i, 2 * brows * b:2 * brows * (b + 1), :]
            efull[:, b * BANDS + i * brows:b * BANDS + (i + 1) * brows, :] = decoded(code, escales[span, i]).reshape(
                2, brows, nb)

    @pl.when(hurry)
    def _():
        pl.semaphore_signal(ready_sem, inc=1, device_id={"ka": mate, "ga": g}, device_id_type=MESH)

    phase("newton")
    e_re, e_im = efull[0], efull[1]
    both = efull[...].reshape(2 * nb, nb)
    sq_re, sq_im = cmul(both, e_re, e_im)
    eye = jnp.where(
        lax.broadcasted_iota(jnp.int32, (nb, nb), 0) == lax.broadcasted_iota(jnp.int32, (nb, nb), 1), 1.0, 0.0)
    cu_re, cu_im = cmul(both, sq_re, sq_im)
    xfull[0] = (eye + (e_re + (sq_re + cu_re))).T
    xfull[1] = (e_im + (sq_im + cu_im)).T

    phase("chain")
    mine = pl.ds(pl.multiple_of(g * rows, rows), rows)
    x_copy = remote(xfull, xmate, x_send, x_recv, mate, g)
    few = rows // 2

    def onward(h):
        return remote(trow.at[1, h], tin.at[h], t_send.at[h], t_recv.at[h], ka_at(2), g)

    def first(h):
        at = pl.ds(pl.multiple_of(g * rows + h * few, few), few)
        return remote(xfull.at[:, at, :], tin.at[h], t_send.at[h], t_recv.at[h], 1, g)

    def same_copy(i):
        return (
            remote(tcode.at[1], tcodes.at[g], g_send.at[i, 0], g_recv.at[i, 0], k, ga_at(i)),
            remote(tscale.at[1], tscales.at[g], g_send.at[i, 1], g_recv.at[i, 1], k, ga_at(i)),
        )

    def mate_copy(i):
        return (
            remote(tcode.at[0], tcodes.at[g], h_send.at[i, 0], g_recv.at[i, 0], mate, ga_at(i)),
            remote(tscale.at[0], tscales.at[g], h_send.at[i, 1], g_recv.at[i, 1], mate, ga_at(i)),
        )

    def encode(which):
        code, scale = coded(trow[which].reshape(2 * rows, nb))
        tcode[which] = code
        tscale[which] = scale

    @pl.when(k == 0)
    def _():
        first(0).start()
        first(1).start()
        give_back()

    @pl.when(jnp.logical_and(odd == 0, k > 0))
    def _():
        x_copy.start()

    phase("token")
    @pl.when(hurry)
    def _():
        pl.semaphore_wait(ready_sem, 1)

        @pl.when(k < FIRST)
        def _():
            send(EARLY, 5)

        @pl.when(k >= FIRST)
        def _():
            send(5, 6)

    z_copies = (
        remote(z_piece, z_in, z_send.at[0], z_recv.at[0], k, ring_at * 2 + 1 - place),
        remote(z_scale, z_in_scale, z_send.at[1], z_recv.at[1], k, ring_at * 2 + 1 - place),
    )

    def sum_ring():
        phase("p_combine")

        @pl.when(k < FIRST)
        def _():
            combine()
            send(5, 6)

        phase("p_wait")
        for i in (0, 1, 2, 3, 5):
            for copy in piece_copies(i):
                copy.wait_recv()
        phase("p_sum")
        out = part[ga - 2]
        for i in (0, 1):
            out = out + decoded(in_pieces[i], in_scales[i])
        code, scale = coded(out)
        z_piece[...] = code
        z_scale[...] = scale
        for copy in z_copies:
            copy.start()
        out = part[ga - 1]
        for i in (2, 3, 5):
            out = out + decoded(in_pieces[i], in_scales[i])
        part[ga - 1] = out

    late = jnp.logical_or(odd == 0, k > LATE)

    @pl.when(late)
    def _():
        sum_ring()

    phase("chain")

    @pl.when(odd == 1)
    def _():
        def keep(re, im):
            high, low = split(re)
            qhigh[:, 0:nb] = high
            qlow[:, 0:nb] = low
            high, low = split(im)
            qhigh[:, nb:2 * nb] = high
            qlow[:, nb:2 * nb] = low

        def step(left, high, low):
            out = dot3(left, high, low)
            return join(out[:, 0:nb], out[:, nb:2 * nb])

        phase("q")

        @pl.when(k == 1)
        def _():
            keep(xfull[0], xfull[1])

        @pl.when(k > 1)
        def _():
            x_copy.wait_recv()
            keep(*cmul(xmate[...].reshape(2 * nb, nb), xfull[0], xfull[1]))

        for h in range(2):
            phase("t_in")
            onward(h).wait_recv()
            phase("t_step")
            re, im = step(tin[h].reshape(rows, nb), qhigh[...], qlow[...])
            trow[1, h, 0] = re
            trow[1, h, 1] = im

            @pl.when(k < ka - 1)
            def _():
                onward(h).start()

        encode(1)
        for i in range(1, ga):
            for copy in same_copy(i):
                copy.start()
        tcodes[g] = tcode[1]
        tscales[g] = tscale[1]

        phase("t_mate")

        @pl.when(k == 1)
        def _():
            trow[0] = tin[...]

        @pl.when(k > 1)
        def _():
            left = jnp.concatenate([tin[0, 0], tin[1, 0], tin[0, 1], tin[1, 1]], axis=0)
            re, im = cmul(left, xmate[0], xmate[1])
            for h in range(2):
                trow[0, h, 0] = re[h * few:(h + 1) * few]
                trow[0, h, 1] = im[h * few:(h + 1) * few]

        encode(0)
        for i in range(ga):
            for copy in mate_copy(i):
                copy.start()

    @pl.when(jnp.logical_not(late))
    def _():
        sum_ring()

    phase("z_wait")
    for copy in z_copies:
        copy.wait_recv()
    phase("z_sum")
    whole = part[ga - 1] + decoded(z_in[...], z_in_scale[...])
    b_both = jnp.concatenate([whole[0:nb, 0:cols].T, whole[nb:2 * nb, 0:cols].T], axis=0)
    d_re = whole[0:nb, cols:2 * cols].T
    d_im = whole[nb:2 * nb, cols:2 * cols].T
    atom_column = jnp.broadcast_to(atoms[pl.ds(g, 1), :].astype(F32), (cols, 128)).T

    phase("t_ag")
    for i in range(1, ga):
        for copy in same_copy(i):
            copy.wait_recv()

    @pl.when(odd == 0)
    def _():
        for copy in mate_copy(0):
            copy.wait_recv()

    for i in range(ga):
        lines = decoded(tcodes[i], tscales[i]).reshape(2, 2, few, nb)
        for h in range(2):
            tfull[:, i * rows + h * few:i * rows + (h + 1) * few, :] = lines[h]

    phase("w")
    out_copy = pltpu.make_async_copy(tfull, transport, out_sem)
    out_copy.start()
    w_re, w_im = cmul(b_both, tfull[0], tfull[1])
    per_proj = jnp.sum(d_re * w_im - d_im * w_re, axis=1, keepdims=True) * (1.0 / ka)
    atom_ids = lax.broadcasted_iota(jnp.int32, (cols, 128), 1).astype(F32)
    force = jnp.sum(jnp.where(atom_column == atom_ids, per_proj, 0.0), axis=0, keepdims=True)
    fka[k] = force

    def along_ka(i):
        return remote(fka.at[k], fka.at[k], f_send.at[i], f_recv.at[i], ka_at(1 + i), g)

    def along_ga(i):
        return remote(fga.at[g], fga.at[g], l_send.at[i], l_recv.at[i], k, ga_at(1 + i))

    phase("f_ka")
    for i in range(ka - 1):
        along_ka(i).start()
    for i in range(ka - 1):
        along_ka(i).wait_recv()
    phase("f_ga")
    fga[g] = jnp.sum(fka[...], axis=0)
    for i in range(ga - 1):
        along_ga(i).start()
    for i in range(ga - 1):
        along_ga(i).wait_recv()
    forces[...] = jnp.sum(fga[...], axis=0)

    phase("drain")
    for b in range(blocks):
        nb_each(lambda copy: copy.wait_send(), b, True)
        for i in range(ga - 1):
            m_copy(b, i).wait_send()
    for span in range(2):
        for i in range(ga - 1):
            for copy in e_copies(span, i):
                copy.wait_send()
    for i in range(ga - 2):
        for copy in piece_copies(i):
            copy.wait_send()
    for copy in z_copies:
        copy.wait_send()
    for i in range(ga - 1):
        along_ga(i).wait_send()
    for i in range(ka - 1):
        along_ka(i).wait_send()

    @pl.when(odd == 0)
    def _():
        for i in range(ga - 1):
            a_copy(i).wait_send()
        s_copy.wait_send()

    @pl.when(k == 0)
    def _():
        first(0).wait_send()
        first(1).wait_send()

    @pl.when(jnp.logical_and(odd == 0, k > 0))
    def _():
        x_copy.wait_send()

    @pl.when(odd == 1)
    def _():
        c_each(lambda copy: copy.wait_send(), turn_on)
        for i in range(1, ga):
            for copy in same_copy(i):
                copy.wait_send()
        for i in range(ga):
            for copy in mate_copy(i):
                copy.wait_send()

        @pl.when(k < ka - 1)
        def _():
            onward(0).wait_send()
            onward(1).wait_send()

    out_copy.wait()
    phase(None)


def local(ka, ga, coeffs, projectors, proj_deriv, shift_map, atom_of):
    _, _, half, nb = coeffs.shape
    np_ = projectors.shape[2]
    cols = np_ // ga
    rows = nb // ga
    blocks = nb // BANDS
    brows = BANDS // ga
    anywhere = pl.BlockSpec(memory_space=pl.ANY)
    vmem = pl.BlockSpec(memory_space=pltpu.VMEM)
    dma = pltpu.SemaphoreType.DMA
    transport, forces = pl.pallas_call(
        functools.partial(kernel, ka, ga),
        out_shape=(jax.ShapeDtypeStruct((2, nb, nb), F32), jax.ShapeDtypeStruct((1, 128), F32)),
        in_specs=[anywhere, anywhere, anywhere, vmem, vmem],
        out_specs=(anywhere, vmem),
        scratch_shapes=[
            pltpu.VMEM((2 * half, nb), BF16),
            pltpu.VMEM((2 * half, nb), BF16),
            pltpu.VMEM((2 * nb, 2 * half), BF16),
            pltpu.VMEM((blocks, BANDS, 2 * half), BF16),
            pltpu.VMEM((2, TURNED, nb), BF16),
            pltpu.VMEM((2, blocks, BANDS, nb), F32),
            pltpu.VMEM((ga - 1, 2, blocks, brows, nb), F32),
            pltpu.VMEM((2, blocks, brows, nb), F32),
            pltpu.VMEM((2, blocks, brows, nb), F32),
            pltpu.VMEM((3, 2, half, 2 * cols), BF16),
            pltpu.VMEM((ga, 2 * nb, 2 * cols), F32),
            pltpu.VMEM((ga - 2, 2 * nb, 2 * cols), I16),
            pltpu.VMEM((ga - 2, 1, 2 * cols), F32),
            pltpu.VMEM((ga - 2, 2 * nb, 2 * cols), I16),
            pltpu.VMEM((ga - 2, 1, 2 * cols), F32),
            pltpu.VMEM((2 * nb, 2 * cols), I16),
            pltpu.VMEM((1, 2 * cols), F32),
            pltpu.VMEM((2 * nb, 2 * cols), I16),
            pltpu.VMEM((1, 2 * cols), F32),
            pltpu.VMEM((blocks, 2, BANDS, nb), F32),
            pltpu.VMEM((blocks, ga - 1, 2, brows, nb), F32),
            pltpu.VMEM((blocks, 2, brows, nb), F32),
            pltpu.VMEM((2 * blocks * brows, nb), I16),
            pltpu.VMEM((2, 1, nb), F32),
            pltpu.VMEM((ga, 2 * blocks * brows, nb), I16),
            pltpu.VMEM((2, ga, 1, nb), F32),
            pltpu.VMEM((2, nb, nb), F32),
            pltpu.VMEM((2, nb, nb), F32),
            pltpu.VMEM((2, nb, nb), F32),
            pltpu.VMEM((nb, 2 * nb), BF16),
            pltpu.VMEM((nb, 2 * nb), BF16),
            pltpu.VMEM((2, 2, rows // 2, nb), F32),
            pltpu.VMEM((2, 2, 2, rows // 2, nb), F32),
            pltpu.VMEM((2, 2 * rows, nb), I16),
            pltpu.VMEM((2, 1, nb), F32),
            pltpu.VMEM((ga, 2 * rows, nb), I16),
            pltpu.VMEM((ga, 1, nb), F32),
            pltpu.VMEM((2, nb, nb), F32),
            pltpu.VMEM((ka, 1, 128), F32),
            pltpu.VMEM((ga, 1, 128), F32),
            dma, dma((3, 2)), dma((blocks, 6)), dma((blocks, 6)), dma((2,)), dma((2,)),
            dma((4,)), dma((4,)), dma((ga - 1,)), dma((ga - 1,)), dma, dma,
            dma((ga - 2, 2)), dma((ga - 2, 2)),
            dma((blocks, ga - 1)), dma((blocks, ga - 1)), dma((2, ga - 1, 2)), dma((2, ga - 1, 2)),
            dma, dma, dma((2,)), dma((2,)), dma((ga, 2)), dma((ga, 2)), dma((ga, 2)),
            dma((ka - 1,)), dma((ka - 1,)), dma((ga - 1,)), dma((ga - 1,)), dma,
            pltpu.SemaphoreType.REGULAR,
        ],
        compiler_params=pltpu.CompilerParams(
            collective_id=0, has_side_effects=True, vmem_limit_bytes=60 * 1024 * 1024),
        name="string",
    )(
        coeffs.reshape(2 * half, nb), projectors, proj_deriv,
        shift_map.reshape(half // 128, 128), atom_of.reshape(ga, cols),
    )
    return transport[None], forces.reshape(128)


def solution(mesh):
    in_specs = (P("ka", None, "ga", None), P(None, "ga", None), P(None, "ga", None), P("ga"), P())
    out_specs = (P("ka", None, None, None), P())
    body = functools.partial(local, mesh.shape["ka"], mesh.shape["ga"])
    return jax.shard_map(body, mesh=mesh, in_specs=in_specs, out_specs=out_specs, check_vma=False)
```

```python
import functools

import jax
import jax.numpy as jnp
from jax import lax
from jax.experimental import pallas as pl
from jax.experimental.pallas import tpu as pltpu
from jax.sharding import PartitionSpec as P

MESH = pl.DeviceIdType.MESH
F32 = jnp.float32
BF16 = jnp.bfloat16
I16 = jnp.int16
BANDS = 64
SHARED = 640
TURNED = 1024
EARLY = 2
FIRST = 4
HURRY = 12
LATE = 10


def split(value):
    high = value.astype(BF16)
    low = (value - high.astype(F32)).astype(BF16)
    return high, low


def dot(left, right):
    return jnp.dot(left, right, preferred_element_type=F32)


def dot3(left, right_high, right_low):
    left_high, left_low = split(left)
    return dot(left_high, right_high) + (dot(left_high, right_low) + dot(left_low, right_high))


def join(by_re, by_im):
    rows = by_re.shape[0] // 2
    return by_re[:rows] - by_im[rows:], by_im[:rows] + by_re[rows:]


def cmul(left, right_re, right_im):
    return join(dot3(left, *split(right_re)), dot3(left, *split(right_im)))


def kernel(
    ka, ga, coeffs, proj, deriv, shift, atoms, transport, forces,
    own, moved, lhs, nbt, cnat, taken, taken_rows, taken_sum, taken_in, rhs, part, pieces, scales, in_pieces, in_scales, z_piece, z_scale, z_in, z_in_scale, mpart, mrows, erow, ecode, escale, ecodes, escales, efull,
    xfull, xmate, qhigh, qlow, tin, trow, tcode, tscale, tcodes, tscales, tfull, fka, fga,
    load_sem, rhs_sem, nb_send, nb_recv, z_send, z_recv, c_send, c_recv, a_send, a_recv, s_send, s_recv, p_send, p_recv, m_send, m_recv, e_send, e_recv,
    x_send, x_recv, t_send, t_recv, g_send, g_recv, h_send, f_send, f_recv, l_send, l_recv, out_sem, ready_sem,
):
    phases = []

    def phase(name):
        if phases:
            phases.pop().__exit__(None, None, None)
        if name:
            phases.append(jax.named_scope(name))
            phases[-1].__enter__()

    phase("start")
    nb = own.shape[1]
    half = own.shape[0] // 2
    cols = part.shape[2] // 2
    rows = nb // ga
    blocks = nb // BANDS
    brows = BANDS // ga
    kept = half - SHARED
    least = half - TURNED
    k = lax.axis_index("ka")
    g = lax.axis_index("ga")
    odd = lax.rem(k, 2)
    mate = k + 1 - 2 * odd
    ring = ga // 2
    ring_at, place = g // 2, lax.rem(g, 2)

    def ga_at(offset):
        return lax.rem(g + offset, ga)

    def ka_at(offset):
        return lax.rem(k + offset, ka)

    def remote(source, target, send, recv, to_k, to_g):
        return pltpu.make_async_remote_copy(
            src_ref=source, dst_ref=target, send_sem=send, recv_sem=recv,
            device_id={"ka": to_k, "ga": to_g}, device_id_type=MESH)

    def all_of(ref, sem):
        pltpu.make_async_copy(ref, ref, sem).wait()

    own_load = pltpu.make_async_copy(coeffs, own, load_sem)
    own_load.start()

    def along_ring(step):
        return lax.rem(ring_at + step, ring) * 2

    def block_of(i):
        last = i // 4
        step = (1 - last) * (1 + 2 * lax.rem(i, 2)) + last * (6 - 2 * (i // 2))
        other = (1 - last) * (1 - i // 2) + last * (1 - lax.rem(i, 2))
        return step, other

    def rhs_loads(i):
        step, other = block_of(i)
        target = along_ring(step) + place + other - 2 * place * other
        slot = lax.rem(i, 3)
        at = pl.ds(pl.multiple_of(target * cols, cols), cols)
        return (
            pltpu.make_async_copy(proj.at[:, :, at], rhs.at[slot, :, :, pl.ds(0, cols)], rhs_sem.at[slot, 0]),
            pltpu.make_async_copy(deriv.at[:, :, at], rhs.at[slot, :, :, pl.ds(cols, cols)], rhs_sem.at[slot, 1]),
        )

    for i in range(2):
        for copy in rhs_loads(i):
            copy.start()

    phase("barrier")
    barrier = pltpu.get_barrier_semaphore()
    for offset in range(1, ga):
        pl.semaphore_signal(barrier, inc=1, device_id={"ka": k, "ga": ga_at(offset)}, device_id_type=MESH)
    for offset in range(ga):
        pl.semaphore_signal(barrier, inc=1, device_id={"ka": mate, "ga": ga_at(offset)}, device_id_type=MESH)
    for offset in range(1, ka - 1):
        other = lax.rem(lax.max(k, mate) + offset, ka)
        pl.semaphore_signal(barrier, inc=1, device_id={"ka": other, "ga": g}, device_id_type=MESH)
    pl.semaphore_wait(barrier, 2 * ga + ka - 3)

    phase("load")
    own_load.wait()

    phase("lhs")
    for at in range(0, half, 384):
        width = min(384, half - at)
        re = own[at:at + width, :].T
        im = own[half + at:half + at + width, :].T
        lhs[0:nb, at:at + width] = re
        lhs[0:nb, half + at:half + at + width] = im
        lhs[nb:2 * nb, at:at + width] = im
        lhs[nb:2 * nb, half + at:half + at + width] = -re

    plane = ka // 2
    turn_back = lax.rem(k, plane) == 0
    turn_on = lax.rem(k, plane) == plane - 1
    ranges = tuple(
        (part_at + first, last - first) for first, last in ((0, least), (least, kept), (kept, half)) for part_at in (0, half))

    def nb_copy(b, r):
        at = pl.ds(*ranges[r])
        return remote(lhs.at[pl.ds(b * BANDS, BANDS), at], nbt.at[b, :, at], nb_send, nb_recv.at[b],
                      ka_at(ka - 1), g)

    def by_class(turned, act):
        @pl.when(turned)
        def _():
            act(least)

        @pl.when(jnp.logical_and(odd == (0 if turned is turn_back else 1), jnp.logical_not(turned)))
        def _():
            act(kept)

        @pl.when(odd == (1 if turned is turn_back else 0))
        def _():
            act(half)

    for b in range(blocks):
        for r in (0, 1):
            nb_copy(b, r).start()

        @pl.when(jnp.logical_not(turn_back))
        def _():
            for r in (2, 3):
                nb_copy(b, r).start()

        @pl.when(odd == 1)
        def _():
            for r in (4, 5):
                nb_copy(b, r).start()

    phase("permute")

    @pl.when(k == ka - 1)
    def _():
        wanted = jnp.concatenate([shift[r:r + 1, :] for r in range(half // 128)], axis=1) - g * half

        def permute(b, carry):
            at = pl.multiple_of(b * 384, 384)
            index = lax.broadcasted_iota(jnp.int32, (384, half), 0) + at
            chosen = jnp.where(wanted == index, 1.0, 0.0).astype(BF16)
            moved[pl.ds(at, 384), :] = dot(chosen, own[0:half, :]).astype(BF16)
            moved[pl.ds(half + at, 384), :] = dot(chosen, own[half:2 * half, :]).astype(BF16)
            return carry

        lax.fori_loop(0, half // 384, permute, 0)
        own[...] = moved[...]

    def c_copy(r):
        first, count = ranges[2 + r]
        part_at = half * (r % 2)
        return remote(own.at[pl.ds(first, count)], cnat.at[r % 2, pl.ds(first - part_at - least, count)],
                      c_send, c_recv, ka_at(1), g)

    @pl.when(odd == 1)
    def _():
        for r in (2, 3):
            c_copy(r).start()

        @pl.when(turn_on)
        def _():
            for r in (0, 1):
                c_copy(r).start()

    def c_all(sem, short):
        @pl.when(short)
        def _():
            all_of(cnat, sem)

        @pl.when(jnp.logical_not(short))
        def _():
            all_of(cnat.at[:, pl.ds(kept - least, SHARED)], sem)

    def piece_to(i):
        across = (i // 4) * (1 - lax.rem(i, 2))
        return along_ring((1 - across) * block_of(i)[0]) + place + across * (1 - 2 * place)

    def piece_copies(i):
        return (
            remote(pieces.at[i], in_pieces.at[i], p_send.at[0], p_recv.at[lax.max(i, 3) - 3, 0], k, piece_to(i)),
            remote(scales.at[i], in_scales.at[i], p_send.at[1], p_recv.at[lax.max(i, 3) - 3, 1], k, piece_to(i)),
        )

    def coded(values):
        top = jnp.maximum(jnp.max(jnp.abs(values), axis=0, keepdims=True), 1e-30)
        code = jnp.round(values * (32767.0 / top)).astype(jnp.int32).astype(I16)
        return code, top * (1.0 / 32767.0)

    def decoded(code, scale):
        return code.astype(jnp.int32).astype(F32) * scale

    hurry = k < HURRY

    def combine():
        for copy in piece_copies(4):
            copy.wait_recv()
        code, scale = coded(part[5] + decoded(in_pieces[4], in_scales[4]))
        pieces[5] = code
        scales[5] = scale

    def send(first, last):
        for i in range(first, last):
            for copy in piece_copies(i):
                copy.start()

    def project(i, carry):
        for copy in rhs_loads(i):
            copy.wait()

        @pl.when(i + 2 < ga)
        def _():
            for copy in rhs_loads(i + 2):
                copy.start()

        part[i] = dot(lhs[...], rhs[lax.rem(i, 3)].reshape(2 * half, 2 * cols))

        @pl.when(i < ga - 3)
        def _():
            code, scale = coded(part[i])
            pieces[i] = code
            scales[i] = scale

        @pl.when(i < EARLY)
        def _():
            for copy in piece_copies(i):
                copy.start()

        return carry

    def m_copy(b, i):
        target = ga_at(1 + i)
        at = pl.ds(pl.multiple_of(target * brows, brows), brows)
        return remote(mpart.at[b, :, at, :], mrows.at[b, i], m_send.at[b], m_recv.at[b], k, target)

    def intersect(b):
        phase(f"nb_wait{b}")

        def over(count):
            re, im = nbt[b, :, 0:count], nbt[b, :, half:half + count]
            by_re = dot(jnp.concatenate([re, im], axis=0), own[0:count, :])
            by_im = dot(jnp.concatenate([im, -re], axis=0), own[half:half + count, :])
            mpart[b] = (by_re + by_im).reshape(2, BANDS, nb)

        def here(count):
            all_of(nbt.at[b, :, pl.ds(0, 2 * count)], nb_recv.at[b])
            over(count)

        by_class(turn_on, here)
        phase(f"m_dot{b}")
        for i in range(ga - 1):
            m_copy(b, i).start()

    def a_copy(i):
        at = pl.ds(pl.multiple_of(ga_at(1 + i) * brows, brows), brows)
        return remote(taken.at[:, :, at, :], taken_rows.at[i], a_send, a_recv, k, ga_at(1 + i))

    s_copy = remote(taken_sum, taken_in, s_send, s_recv, ka_at(ka - 1), g)

    def take():
        c_all(c_recv, turn_back)

        def from_wave(first):
            out = dot(lhs[:, first:half], cnat[0, first - least:])
            out = out + dot(lhs[:, half + first:2 * half], cnat[1, first - least:])
            taken[...] = out.reshape(2, blocks, BANDS, nb)

        @pl.when(turn_back)
        def _():
            from_wave(least)

        @pl.when(jnp.logical_not(turn_back))
        def _():
            from_wave(kept)

        for i in range(ga - 1):
            a_copy(i).start()

    def give_back():
        out = taken[:, :, pl.ds(pl.multiple_of(g * brows, brows), brows), :]
        all_of(taken_rows, a_recv)
        for i in range(ga - 1):
            out = out + taken_rows[i]
        taken_sum[...] = out
        s_copy.start()

    even = jnp.logical_and(odd == 0, k > 0)

    spans = ((0, blocks - 1), (blocks - 1, blocks))

    def span_rows(span):
        return pl.ds(2 * brows * spans[span][0], 2 * brows * (spans[span][1] - spans[span][0]))

    def e_copies(span, i):
        to = ga_at(1 + i)
        return (
            remote(ecode.at[span_rows(span)], ecodes.at[g, span_rows(span)], e_send.at[span, 0], e_recv.at[span, 0], k, to),
            remote(escale.at[span], escales.at[span, g], e_send.at[span, 1], e_recv.at[span, 1], k, to),
        )

    def spread(span):
        first, last = spans[span]
        code, scale = coded(erow[first:last].reshape(2 * brows * (last - first), nb))
        ecode[span_rows(span), :] = code
        escale[span] = scale
        for i in range(ga - 1):
            for copy in e_copies(span, i):
                copy.start()
        ecodes[g, span_rows(span), :] = code
        escales[span, g] = scale

    def settle(b):
        phase(f"m_rs{b}")
        total = mpart[b, :, pl.ds(pl.multiple_of(g * brows, brows), brows), :]
        all_of(mrows.at[b], m_recv.at[b])
        for i in range(ga - 1):
            total = total + mrows[b, i]
        erow[b] = total

        @pl.when(odd == 1)
        def _():
            if b == 0:
                s_copy.wait_recv()
            erow[b] = total + taken_in[:, b]

        total = erow[b]
        first = b * BANDS + g * brows
        row_at = lax.broadcasted_iota(jnp.int32, (brows, nb), 0) + first
        col_at = lax.broadcasted_iota(jnp.int32, (brows, nb), 1)
        erow[b, 0] = jnp.where(row_at == col_at, 1.0, 0.0) - total[0]
        erow[b, 1] = -total[1]

    phase("project0")
    lax.fori_loop(0, 4, project, 0)

    intersect(0)
    phase("project1")
    lax.fori_loop(4, 6, project, 0)
    intersect(1)
    phase("take")

    @pl.when(even)
    def _():
        take()


    @pl.when(k >= FIRST)
    def _():
        send(EARLY, 4)

    phase("project2")
    lax.fori_loop(6, ga, project, 0)
    intersect(2)
    intersect(3)
    phase("give_back")

    @pl.when(even)
    def _():
        give_back()

    @pl.when(k >= FIRST)
    def _():
        send(4, 5)

    settle(0)
    settle(1)
    settle(2)
    spread(0)
    settle(3)
    spread(1)
    phase("combine")

    @pl.when(k >= FIRST)
    def _():
        combine()

    @pl.when(jnp.logical_not(hurry))
    def _():
        send(5, 6)

    phase("take_last")

    @pl.when(k == 0)
    def _():
        take()

    phase("e_ag")
    def e_all(sem):
        for span in range(2):
            all_of(ecodes.at[pl.ds(0, ga - 1), span_rows(span)], sem.at[span, 0])
            all_of(escales.at[span, pl.ds(0, ga - 1)], sem.at[span, 1])

    e_all(e_recv)
    for i in range(ga):
        for b in range(blocks):
            span = b // (blocks - 1)
            code = ecodes[i, 2 * brows * b:2 * brows * (b + 1), :]
            efull[:, b * BANDS + i * brows:b * BANDS + (i + 1) * brows, :] = decoded(code, escales[span, i]).reshape(
                2, brows, nb)

    @pl.when(hurry)
    def _():
        pl.semaphore_signal(ready_sem, inc=1, device_id={"ka": mate, "ga": g}, device_id_type=MESH)

    phase("newton")
    e_re, e_im = efull[0], efull[1]
    both = efull[...].reshape(2 * nb, nb)
    sq_re, sq_im = cmul(both, e_re, e_im)
    eye = jnp.where(
        lax.broadcasted_iota(jnp.int32, (nb, nb), 0) == lax.broadcasted_iota(jnp.int32, (nb, nb), 1), 1.0, 0.0)
    cu_re, cu_im = cmul(both, sq_re, sq_im)
    xfull[0] = (eye + (e_re + (sq_re + cu_re))).T
    xfull[1] = (e_im + (sq_im + cu_im)).T

    phase("chain")
    mine = pl.ds(pl.multiple_of(g * rows, rows), rows)
    x_copy = remote(xfull, xmate, x_send, x_recv, mate, g)
    few = rows // 2

    def onward(h):
        return remote(trow.at[1, h], tin.at[h], t_send.at[h], t_recv.at[h], ka_at(2), g)

    def first(h):
        at = pl.ds(pl.multiple_of(g * rows + h * few, few), few)
        return remote(xfull.at[:, at, :], tin.at[h], t_send.at[h], t_recv.at[h], 1, g)

    def same_copy(i):
        return (
            remote(tcode.at[1], tcodes.at[g], g_send.at[0], g_recv.at[0], k, ga_at(i)),
            remote(tscale.at[1], tscales.at[g], g_send.at[1], g_recv.at[1], k, ga_at(i)),
        )

    def mate_copy(i):
        return (
            remote(tcode.at[0], tcodes.at[g], h_send.at[0], g_recv.at[0], mate, ga_at(i)),
            remote(tscale.at[0], tscales.at[g], h_send.at[1], g_recv.at[1], mate, ga_at(i)),
        )

    def encode(which):
        code, scale = coded(trow[which].reshape(2 * rows, nb))
        tcode[which] = code
        tscale[which] = scale

    @pl.when(k == 0)
    def _():
        first(0).start()
        first(1).start()
        give_back()

    @pl.when(jnp.logical_and(odd == 0, k > 0))
    def _():
        x_copy.start()

    phase("token")
    @pl.when(hurry)
    def _():
        pl.semaphore_wait(ready_sem, 1)

        @pl.when(k < FIRST)
        def _():
            send(EARLY, 5)

        @pl.when(k >= FIRST)
        def _():
            send(5, 6)

    z_copies = (
        remote(z_piece, z_in, z_send.at[0], z_recv.at[0], k, ring_at * 2 + 1 - place),
        remote(z_scale, z_in_scale, z_send.at[1], z_recv.at[1], k, ring_at * 2 + 1 - place),
    )

    def sum_ring():
        phase("p_combine")

        @pl.when(k < FIRST)
        def _():
            combine()
            send(5, 6)

        phase("p_wait")
        all_of(in_pieces.at[pl.ds(0, 4)], p_recv.at[0, 0])
        all_of(in_scales.at[pl.ds(0, 4)], p_recv.at[0, 1])
        for copy in piece_copies(5):
            copy.wait_recv()
        phase("p_sum")
        out = part[ga - 2]
        for i in (0, 1):
            out = out + decoded(in_pieces[i], in_scales[i])
        code, scale = coded(out)
        z_piece[...] = code
        z_scale[...] = scale
        for copy in z_copies:
            copy.start()
        out = part[ga - 1]
        for i in (2, 3, 5):
            out = out + decoded(in_pieces[i], in_scales[i])
        part[ga - 1] = out

    late = jnp.logical_or(odd == 0, k > LATE)

    @pl.when(late)
    def _():
        sum_ring()

    phase("chain")

    @pl.when(odd == 1)
    def _():
        def keep(re, im):
            high, low = split(re)
            qhigh[:, 0:nb] = high
            qlow[:, 0:nb] = low
            high, low = split(im)
            qhigh[:, nb:2 * nb] = high
            qlow[:, nb:2 * nb] = low

        def step(left, high, low):
            out = dot3(left, high, low)
            return join(out[:, 0:nb], out[:, nb:2 * nb])

        phase("q")

        @pl.when(k == 1)
        def _():
            keep(xfull[0], xfull[1])

        @pl.when(k > 1)
        def _():
            x_copy.wait_recv()
            keep(*cmul(xmate[...].reshape(2 * nb, nb), xfull[0], xfull[1]))

        for h in range(2):
            phase("t_in")
            onward(h).wait_recv()
            phase("t_step")
            re, im = step(tin[h].reshape(rows, nb), qhigh[...], qlow[...])
            trow[1, h, 0] = re
            trow[1, h, 1] = im

            @pl.when(k < ka - 1)
            def _():
                onward(h).start()

        encode(1)
        for i in range(1, ga):
            for copy in same_copy(i):
                copy.start()
        tcodes[g] = tcode[1]
        tscales[g] = tscale[1]

        phase("t_mate")

        @pl.when(k == 1)
        def _():
            trow[0] = tin[...]

        @pl.when(k > 1)
        def _():
            left = jnp.concatenate([tin[0, 0], tin[1, 0], tin[0, 1], tin[1, 1]], axis=0)
            re, im = cmul(left, xmate[0], xmate[1])
            for h in range(2):
                trow[0, h, 0] = re[h * few:(h + 1) * few]
                trow[0, h, 1] = im[h * few:(h + 1) * few]

        encode(0)
        for i in range(ga):
            for copy in mate_copy(i):
                copy.start()

    @pl.when(jnp.logical_not(late))
    def _():
        sum_ring()

    phase("z_wait")
    for copy in z_copies:
        copy.wait_recv()
    phase("z_sum")
    whole = part[ga - 1] + decoded(z_in[...], z_in_scale[...])
    b_both = jnp.concatenate([whole[0:nb, 0:cols].T, whole[nb:2 * nb, 0:cols].T], axis=0)
    d_re = whole[0:nb, cols:2 * cols].T
    d_im = whole[nb:2 * nb, cols:2 * cols].T
    atom_column = jnp.broadcast_to(atoms[pl.ds(g, 1), :].astype(F32), (cols, 128)).T

    phase("t_ag")
    def t_all(sem, count):
        all_of(tcodes.at[pl.ds(0, count)], sem.at[0])
        all_of(tscales.at[pl.ds(0, count)], sem.at[1])

    @pl.when(odd == 1)
    def _():
        t_all(g_recv, ga - 1)

    @pl.when(odd == 0)
    def _():
        t_all(g_recv, ga)

    for i in range(ga):
        lines = decoded(tcodes[i], tscales[i]).reshape(2, 2, few, nb)
        for h in range(2):
            tfull[:, i * rows + h * few:i * rows + (h + 1) * few, :] = lines[h]

    phase("w")
    out_copy = pltpu.make_async_copy(tfull, transport, out_sem)
    out_copy.start()
    w_re, w_im = cmul(b_both, tfull[0], tfull[1])
    per_proj = jnp.sum(d_re * w_im - d_im * w_re, axis=1, keepdims=True) * (1.0 / ka)
    atom_ids = lax.broadcasted_iota(jnp.int32, (cols, 128), 1).astype(F32)
    force = jnp.sum(jnp.where(atom_column == atom_ids, per_proj, 0.0), axis=0, keepdims=True)
    fka[k] = force

    def along_ka(i):
        return remote(fka.at[k], fka.at[k], f_send, f_recv, ka_at(1 + i), g)

    def along_ga(i):
        return remote(fga.at[g], fga.at[g], l_send, l_recv, k, ga_at(1 + i))

    phase("f_ka")
    for i in range(ka - 1):
        along_ka(i).start()
    all_of(fka.at[pl.ds(0, ka - 1)], f_recv)
    phase("f_ga")
    fga[g] = jnp.sum(fka[...], axis=0)
    for i in range(ga - 1):
        along_ga(i).start()
    all_of(fga.at[pl.ds(0, ga - 1)], l_recv)
    forces[...] = jnp.sum(fga[...], axis=0)

    phase("drain")
    by_class(turn_back, lambda count: all_of(nbt.at[:, :, pl.ds(0, 2 * count)], nb_send))
    for b in range(blocks):
        all_of(mrows.at[b], m_send.at[b])
    e_all(e_send)
    all_of(in_pieces, p_send.at[0])
    all_of(in_scales, p_send.at[1])
    for copy in z_copies:
        copy.wait_send()
    all_of(fga.at[pl.ds(0, ga - 1)], l_send)
    all_of(fka.at[pl.ds(0, ka - 1)], f_send)

    @pl.when(odd == 0)
    def _():
        all_of(taken_rows, a_send)
        s_copy.wait_send()

    @pl.when(k == 0)
    def _():
        first(0).wait_send()
        first(1).wait_send()

    @pl.when(jnp.logical_and(odd == 0, k > 0))
    def _():
        x_copy.wait_send()

    @pl.when(odd == 1)
    def _():
        c_all(c_send, turn_on)
        t_all(g_send, ga - 1)
        t_all(h_send, ga)

        @pl.when(k < ka - 1)
        def _():
            onward(0).wait_send()
            onward(1).wait_send()

    out_copy.wait()
    phase(None)


def local(ka, ga, coeffs, projectors, proj_deriv, shift_map, atom_of):
    _, _, half, nb = coeffs.shape
    np_ = projectors.shape[2]
    cols = np_ // ga
    rows = nb // ga
    blocks = nb // BANDS
    brows = BANDS // ga
    anywhere = pl.BlockSpec(memory_space=pl.ANY)
    vmem = pl.BlockSpec(memory_space=pltpu.VMEM)
    dma = pltpu.SemaphoreType.DMA
    transport, forces = pl.pallas_call(
        functools.partial(kernel, ka, ga),
        out_shape=(jax.ShapeDtypeStruct((2, nb, nb), F32), jax.ShapeDtypeStruct((1, 128), F32)),
        in_specs=[anywhere, anywhere, anywhere, vmem, vmem],
        out_specs=(anywhere, vmem),
        scratch_shapes=[
            pltpu.VMEM((2 * half, nb), BF16),
            pltpu.VMEM((2 * half, nb), BF16),
            pltpu.VMEM((2 * nb, 2 * half), BF16),
            pltpu.VMEM((blocks, BANDS, 2 * half), BF16),
            pltpu.VMEM((2, TURNED, nb), BF16),
            pltpu.VMEM((2, blocks, BANDS, nb), F32),
            pltpu.VMEM((ga - 1, 2, blocks, brows, nb), F32),
            pltpu.VMEM((2, blocks, brows, nb), F32),
            pltpu.VMEM((2, blocks, brows, nb), F32),
            pltpu.VMEM((3, 2, half, 2 * cols), BF16),
            pltpu.VMEM((ga, 2 * nb, 2 * cols), F32),
            pltpu.VMEM((ga - 2, 2 * nb, 2 * cols), I16),
            pltpu.VMEM((ga - 2, 1, 2 * cols), F32),
            pltpu.VMEM((ga - 2, 2 * nb, 2 * cols), I16),
            pltpu.VMEM((ga - 2, 1, 2 * cols), F32),
            pltpu.VMEM((2 * nb, 2 * cols), I16),
            pltpu.VMEM((1, 2 * cols), F32),
            pltpu.VMEM((2 * nb, 2 * cols), I16),
            pltpu.VMEM((1, 2 * cols), F32),
            pltpu.VMEM((blocks, 2, BANDS, nb), F32),
            pltpu.VMEM((blocks, ga - 1, 2, brows, nb), F32),
            pltpu.VMEM((blocks, 2, brows, nb), F32),
            pltpu.VMEM((2 * blocks * brows, nb), I16),
            pltpu.VMEM((2, 1, nb), F32),
            pltpu.VMEM((ga, 2 * blocks * brows, nb), I16),
            pltpu.VMEM((2, ga, 1, nb), F32),
            pltpu.VMEM((2, nb, nb), F32),
            pltpu.VMEM((2, nb, nb), F32),
            pltpu.VMEM((2, nb, nb), F32),
            pltpu.VMEM((nb, 2 * nb), BF16),
            pltpu.VMEM((nb, 2 * nb), BF16),
            pltpu.VMEM((2, 2, rows // 2, nb), F32),
            pltpu.VMEM((2, 2, 2, rows // 2, nb), F32),
            pltpu.VMEM((2, 2 * rows, nb), I16),
            pltpu.VMEM((2, 1, nb), F32),
            pltpu.VMEM((ga, 2 * rows, nb), I16),
            pltpu.VMEM((ga, 1, nb), F32),
            pltpu.VMEM((2, nb, nb), F32),
            pltpu.VMEM((ka, 1, 128), F32),
            pltpu.VMEM((ga, 1, 128), F32),
            dma, dma((3, 2)), dma, dma((blocks,)), dma((2,)), dma((2,)), dma, dma, dma, dma, dma, dma,
            dma((2,)), dma((3, 2)), dma((blocks,)), dma((blocks,)), dma((2, 2)), dma((2, 2)),
            dma, dma, dma((2,)), dma((2,)), dma((2,)), dma((2,)), dma((2,)), dma, dma, dma, dma, dma,
            pltpu.SemaphoreType.REGULAR,
        ],
        compiler_params=pltpu.CompilerParams(
            collective_id=0, has_side_effects=True, vmem_limit_bytes=60 * 1024 * 1024),
        name="string",
    )(
        coeffs.reshape(2 * half, nb), projectors, proj_deriv,
        shift_map.reshape(half // 128, 128), atom_of.reshape(ga, cols),
    )
    return transport[None], forces.reshape(128)


def solution(mesh):
    in_specs = (P("ka", None, "ga", None), P(None, "ga", None), P(None, "ga", None), P("ga"), P())
    out_specs = (P("ka", None, None, None), P())
    body = functools.partial(local, mesh.shape["ka"], mesh.shape["ga"])
    return jax.shard_map(body, mesh=mesh, in_specs=in_specs, out_specs=out_specs, check_vma=False)
```

```python
import functools

import jax
import jax.numpy as jnp
from jax import lax
from jax.experimental import pallas as pl
from jax.experimental.pallas import tpu as pltpu
from jax.sharding import PartitionSpec as P

MESH = pl.DeviceIdType.MESH
F32 = jnp.float32
BF16 = jnp.bfloat16
I16 = jnp.int16
BANDS = 64
SHARED = 640
TURNED = 1024
EARLY = 2
FIRST = 4
HURRY = 12
LATE = 10


def split(value):
    high = value.astype(BF16)
    low = (value - high.astype(F32)).astype(BF16)
    return high, low


def dot(left, right):
    return jnp.dot(left, right, preferred_element_type=F32)


def dot3(left, right_high, right_low):
    left_high, left_low = split(left)
    return dot(left_high, right_high) + (dot(left_high, right_low) + dot(left_low, right_high))


def join(by_re, by_im):
    rows = by_re.shape[0] // 2
    return by_re[:rows] - by_im[rows:], by_im[:rows] + by_re[rows:]


def cmul(left, right_re, right_im):
    return join(dot3(left, *split(right_re)), dot3(left, *split(right_im)))


def kernel(
    ka, ga, coeffs, proj, deriv, shift, atoms, tfull, forces,
    own, moved, lhs, nbt, cnat, taken, taken_rows, taken_sum, taken_in, rhs, part, pieces, scales, in_pieces, in_scales, z_piece, z_scale, z_in, z_in_scale, mpart, mrows, erow, ecode, escale, ecodes, escales, efull,
    xfull, xmate, qhigh, qlow, tin, trow, tcode, tscale, tcodes, tscales, fka, fga,
    load_sem, rhs_sem, nb_send, nb_recv, z_send, z_recv, c_send, c_recv, a_send, a_recv, s_send, s_recv, p_send, p_recv, m_send, m_recv, e_send, e_recv,
    x_send, x_recv, t_send, t_recv, g_send, g_recv, h_send, f_send, f_recv, l_send, l_recv, ready_sem,
):
    phases = []

    def phase(name):
        if phases:
            phases.pop().__exit__(None, None, None)
        if name:
            phases.append(jax.named_scope(name))
            phases[-1].__enter__()

    phase("start")
    nb = own.shape[1]
    half = own.shape[0] // 2
    cols = part.shape[2] // 2
    rows = nb // ga
    blocks = nb // BANDS
    brows = BANDS // ga
    kept = half - SHARED
    least = half - TURNED
    k = lax.axis_index("ka")
    g = lax.axis_index("ga")
    odd = lax.rem(k, 2)
    mate = k + 1 - 2 * odd
    ring = ga // 2
    ring_at, place = g // 2, lax.rem(g, 2)

    def ga_at(offset):
        return lax.rem(g + offset, ga)

    def ka_at(offset):
        return lax.rem(k + offset, ka)

    def remote(source, target, send, recv, to_k, to_g):
        return pltpu.make_async_remote_copy(
            src_ref=source, dst_ref=target, send_sem=send, recv_sem=recv,
            device_id={"ka": to_k, "ga": to_g}, device_id_type=MESH)

    def all_of(ref, sem):
        pltpu.make_async_copy(ref, ref, sem).wait()

    own_load = pltpu.make_async_copy(coeffs, own, load_sem)
    own_load.start()

    def along_ring(step):
        return lax.rem(ring_at + step, ring) * 2

    def block_of(i):
        last = i // 4
        step = (1 - last) * (1 + 2 * lax.rem(i, 2)) + last * (6 - 2 * (i // 2))
        other = (1 - last) * (1 - i // 2) + last * (1 - lax.rem(i, 2))
        return step, other

    def rhs_loads(i):
        step, other = block_of(i)
        target = along_ring(step) + place + other - 2 * place * other
        slot = lax.rem(i, 3)
        at = pl.ds(pl.multiple_of(target * cols, cols), cols)
        return (
            pltpu.make_async_copy(proj.at[:, :, at], rhs.at[slot, :, :, pl.ds(0, cols)], rhs_sem.at[slot, 0]),
            pltpu.make_async_copy(deriv.at[:, :, at], rhs.at[slot, :, :, pl.ds(cols, cols)], rhs_sem.at[slot, 1]),
        )

    for i in range(2):
        for copy in rhs_loads(i):
            copy.start()

    phase("barrier")
    barrier = pltpu.get_barrier_semaphore()
    for offset in range(1, ga):
        pl.semaphore_signal(barrier, inc=1, device_id={"ka": k, "ga": ga_at(offset)}, device_id_type=MESH)
    for offset in range(ga):
        pl.semaphore_signal(barrier, inc=1, device_id={"ka": mate, "ga": ga_at(offset)}, device_id_type=MESH)
    for offset in range(1, ka - 1):
        other = lax.rem(lax.max(k, mate) + offset, ka)
        pl.semaphore_signal(barrier, inc=1, device_id={"ka": other, "ga": g}, device_id_type=MESH)
    pl.semaphore_wait(barrier, 2 * ga + ka - 3)

    phase("load")
    own_load.wait()

    phase("lhs")
    for at in range(0, half, 384):
        width = min(384, half - at)
        re = own[at:at + width, :].T
        im = own[half + at:half + at + width, :].T
        lhs[0:nb, at:at + width] = re
        lhs[0:nb, half + at:half + at + width] = im
        lhs[nb:2 * nb, at:at + width] = im
        lhs[nb:2 * nb, half + at:half + at + width] = -re

    plane = ka // 2
    turn_back = lax.rem(k, plane) == 0
    turn_on = lax.rem(k, plane) == plane - 1
    ranges = tuple(
        (part_at + first, last - first) for first, last in ((0, least), (least, kept), (kept, half)) for part_at in (0, half))

    def nb_copy(b, r):
        at = pl.ds(*ranges[r])
        return remote(lhs.at[pl.ds(b * BANDS, BANDS), at], nbt.at[b, :, at], nb_send, nb_recv.at[b],
                      ka_at(ka - 1), g)

    def by_class(turned, act):
        @pl.when(turned)
        def _():
            act(least)

        @pl.when(jnp.logical_and(odd == (0 if turned is turn_back else 1), jnp.logical_not(turned)))
        def _():
            act(kept)

        @pl.when(odd == (1 if turned is turn_back else 0))
        def _():
            act(half)

    for b in range(blocks):
        for r in (0, 1):
            nb_copy(b, r).start()

        @pl.when(jnp.logical_not(turn_back))
        def _():
            for r in (2, 3):
                nb_copy(b, r).start()

        @pl.when(odd == 1)
        def _():
            for r in (4, 5):
                nb_copy(b, r).start()

    phase("permute")

    @pl.when(k == ka - 1)
    def _():
        wanted = jnp.concatenate([shift[r:r + 1, :] for r in range(half // 128)], axis=1) - g * half

        def permute(b, carry):
            at = pl.multiple_of(b * 384, 384)
            index = lax.broadcasted_iota(jnp.int32, (384, half), 0) + at
            chosen = jnp.where(wanted == index, 1.0, 0.0).astype(BF16)
            moved[pl.ds(at, 384), :] = dot(chosen, own[0:half, :]).astype(BF16)
            moved[pl.ds(half + at, 384), :] = dot(chosen, own[half:2 * half, :]).astype(BF16)
            return carry

        lax.fori_loop(0, half // 384, permute, 0)
        own[...] = moved[...]

    def c_copy(r):
        first, count = ranges[2 + r]
        part_at = half * (r % 2)
        return remote(own.at[pl.ds(first, count)], cnat.at[r % 2, pl.ds(first - part_at - least, count)],
                      c_send, c_recv, ka_at(1), g)

    @pl.when(odd == 1)
    def _():
        for r in (2, 3):
            c_copy(r).start()

        @pl.when(turn_on)
        def _():
            for r in (0, 1):
                c_copy(r).start()

    def c_all(sem, short):
        @pl.when(short)
        def _():
            all_of(cnat, sem)

        @pl.when(jnp.logical_not(short))
        def _():
            all_of(cnat.at[:, pl.ds(kept - least, SHARED)], sem)

    def piece_to(i):
        across = (i // 4) * (1 - lax.rem(i, 2))
        return along_ring((1 - across) * block_of(i)[0]) + place + across * (1 - 2 * place)

    def piece_copies(i):
        return (
            remote(pieces.at[i], in_pieces.at[i], p_send.at[0], p_recv.at[lax.max(i, 3) - 3, 0], k, piece_to(i)),
            remote(scales.at[i], in_scales.at[i], p_send.at[1], p_recv.at[lax.max(i, 3) - 3, 1], k, piece_to(i)),
        )

    def coded(values):
        top = jnp.maximum(jnp.max(jnp.abs(values), axis=0, keepdims=True), 1e-30)
        code = jnp.round(values * (32767.0 / top)).astype(jnp.int32).astype(I16)
        return code, top * (1.0 / 32767.0)

    def decoded(code, scale):
        return code.astype(jnp.int32).astype(F32) * scale

    hurry = k < HURRY

    def combine():
        for copy in piece_copies(4):
            copy.wait_recv()
        code, scale = coded(part[5] + decoded(in_pieces[4], in_scales[4]))
        pieces[5] = code
        scales[5] = scale

    def send(first, last):
        for i in range(first, last):
            for copy in piece_copies(i):
                copy.start()

    def project(i, carry):
        for copy in rhs_loads(i):
            copy.wait()

        @pl.when(i + 2 < ga)
        def _():
            for copy in rhs_loads(i + 2):
                copy.start()

        part[i] = dot(lhs[...], rhs[lax.rem(i, 3)].reshape(2 * half, 2 * cols))

        @pl.when(i < ga - 3)
        def _():
            code, scale = coded(part[i])
            pieces[i] = code
            scales[i] = scale

        @pl.when(i < EARLY)
        def _():
            for copy in piece_copies(i):
                copy.start()

        return carry

    def m_copy(b, i):
        target = ga_at(1 + i)
        at = pl.ds(pl.multiple_of(target * brows, brows), brows)
        return remote(mpart.at[b, :, at, :], mrows.at[b, i], m_send.at[b], m_recv.at[b], k, target)

    def intersect(b):
        phase(f"nb_wait{b}")

        def over(count):
            re, im = nbt[b, :, 0:count], nbt[b, :, half:half + count]
            by_re = dot(jnp.concatenate([re, im], axis=0), own[0:count, :])
            by_im = dot(jnp.concatenate([im, -re], axis=0), own[half:half + count, :])
            mpart[b] = (by_re + by_im).reshape(2, BANDS, nb)

        def here(count):
            all_of(nbt.at[b, :, pl.ds(0, 2 * count)], nb_recv.at[b])
            over(count)

        by_class(turn_on, here)
        phase(f"m_dot{b}")
        for i in range(ga - 1):
            m_copy(b, i).start()

    def a_copy(i):
        at = pl.ds(pl.multiple_of(ga_at(1 + i) * brows, brows), brows)
        return remote(taken.at[:, :, at, :], taken_rows.at[i], a_send, a_recv, k, ga_at(1 + i))

    s_copy = remote(taken_sum, taken_in, s_send, s_recv, ka_at(ka - 1), g)

    def take():
        c_all(c_recv, turn_back)

        def from_wave(first):
            out = dot(lhs[:, first:half], cnat[0, first - least:])
            out = out + dot(lhs[:, half + first:2 * half], cnat[1, first - least:])
            taken[...] = out.reshape(2, blocks, BANDS, nb)

        @pl.when(turn_back)
        def _():
            from_wave(least)

        @pl.when(jnp.logical_not(turn_back))
        def _():
            from_wave(kept)

        for i in range(ga - 1):
            a_copy(i).start()

    def give_back():
        out = taken[:, :, pl.ds(pl.multiple_of(g * brows, brows), brows), :]
        all_of(taken_rows, a_recv)
        for i in range(ga - 1):
            out = out + taken_rows[i]
        taken_sum[...] = out
        s_copy.start()

    even = jnp.logical_and(odd == 0, k > 0)

    spans = ((0, blocks - 1), (blocks - 1, blocks))

    def span_rows(span):
        return pl.ds(2 * brows * spans[span][0], 2 * brows * (spans[span][1] - spans[span][0]))

    def e_copies(span, i):
        to = ga_at(1 + i)
        return (
            remote(ecode.at[span_rows(span)], ecodes.at[g, span_rows(span)], e_send.at[span, 0], e_recv.at[span, 0], k, to),
            remote(escale.at[span], escales.at[span, g], e_send.at[span, 1], e_recv.at[span, 1], k, to),
        )

    def spread(span):
        first, last = spans[span]
        code, scale = coded(erow[first:last].reshape(2 * brows * (last - first), nb))
        ecode[span_rows(span), :] = code
        escale[span] = scale
        for i in range(ga - 1):
            for copy in e_copies(span, i):
                copy.start()
        ecodes[g, span_rows(span), :] = code
        escales[span, g] = scale

    def settle(b):
        phase(f"m_rs{b}")
        total = mpart[b, :, pl.ds(pl.multiple_of(g * brows, brows), brows), :]
        all_of(mrows.at[b], m_recv.at[b])
        for i in range(ga - 1):
            total = total + mrows[b, i]
        erow[b] = total

        @pl.when(odd == 1)
        def _():
            if b == 0:
                s_copy.wait_recv()
            erow[b] = total + taken_in[:, b]

        total = erow[b]
        first = b * BANDS + g * brows
        row_at = lax.broadcasted_iota(jnp.int32, (brows, nb), 0) + first
        col_at = lax.broadcasted_iota(jnp.int32, (brows, nb), 1)
        erow[b, 0] = jnp.where(row_at == col_at, 1.0, 0.0) - total[0]
        erow[b, 1] = -total[1]

    phase("project0")
    lax.fori_loop(0, 4, project, 0)

    intersect(0)
    phase("project1")
    lax.fori_loop(4, 6, project, 0)
    intersect(1)
    phase("take")

    @pl.when(even)
    def _():
        take()


    @pl.when(k >= FIRST)
    def _():
        send(EARLY, 4)

    phase("project2")
    lax.fori_loop(6, ga, project, 0)
    intersect(2)
    intersect(3)
    phase("give_back")

    @pl.when(even)
    def _():
        give_back()

    @pl.when(k >= FIRST)
    def _():
        send(4, 5)

    settle(0)
    settle(1)
    settle(2)
    spread(0)
    settle(3)
    spread(1)
    phase("combine")

    @pl.when(k >= FIRST)
    def _():
        combine()

    @pl.when(jnp.logical_not(hurry))
    def _():
        send(5, 6)

    phase("take_last")

    @pl.when(k == 0)
    def _():
        take()

    phase("e_ag")
    def e_all(sem):
        for span in range(2):
            all_of(ecodes.at[pl.ds(0, ga - 1), span_rows(span)], sem.at[span, 0])
            all_of(escales.at[span, pl.ds(0, ga - 1)], sem.at[span, 1])

    e_all(e_recv)
    for i in range(ga):
        for b in range(blocks):
            span = b // (blocks - 1)
            code = ecodes[i, 2 * brows * b:2 * brows * (b + 1), :]
            efull[:, b * BANDS + i * brows:b * BANDS + (i + 1) * brows, :] = decoded(code, escales[span, i]).reshape(
                2, brows, nb)

    @pl.when(hurry)
    def _():
        pl.semaphore_signal(ready_sem, inc=1, device_id={"ka": mate, "ga": g}, device_id_type=MESH)

    phase("newton")
    e_re, e_im = efull[0], efull[1]
    both = efull[...].reshape(2 * nb, nb)
    sq_re, sq_im = cmul(both, e_re, e_im)
    eye = jnp.where(
        lax.broadcasted_iota(jnp.int32, (nb, nb), 0) == lax.broadcasted_iota(jnp.int32, (nb, nb), 1), 1.0, 0.0)
    cu_re, cu_im = cmul(both, sq_re, sq_im)
    xfull[0] = (eye + (e_re + (sq_re + cu_re))).T
    xfull[1] = (e_im + (sq_im + cu_im)).T

    phase("chain")
    mine = pl.ds(pl.multiple_of(g * rows, rows), rows)
    x_copy = remote(xfull, xmate, x_send, x_recv, mate, g)
    few = rows // 2

    def onward(h):
        return remote(trow.at[1, h], tin.at[h], t_send.at[h], t_recv.at[h], ka_at(2), g)

    def first(h):
        at = pl.ds(pl.multiple_of(g * rows + h * few, few), few)
        return remote(xfull.at[:, at, :], tin.at[h], t_send.at[h], t_recv.at[h], 1, g)

    def same_copy(i):
        return (
            remote(tcode.at[1], tcodes.at[g], g_send.at[0], g_recv.at[0], k, ga_at(i)),
            remote(tscale.at[1], tscales.at[g], g_send.at[1], g_recv.at[1], k, ga_at(i)),
        )

    def mate_copy(i):
        return (
            remote(tcode.at[0], tcodes.at[g], h_send.at[0], g_recv.at[0], mate, ga_at(i)),
            remote(tscale.at[0], tscales.at[g], h_send.at[1], g_recv.at[1], mate, ga_at(i)),
        )

    def encode(which):
        code, scale = coded(trow[which].reshape(2 * rows, nb))
        tcode[which] = code
        tscale[which] = scale

    @pl.when(k == 0)
    def _():
        first(0).start()
        first(1).start()
        give_back()

    @pl.when(jnp.logical_and(odd == 0, k > 0))
    def _():
        x_copy.start()

    phase("token")
    @pl.when(hurry)
    def _():
        pl.semaphore_wait(ready_sem, 1)

        @pl.when(k < FIRST)
        def _():
            send(EARLY, 5)

        @pl.when(k >= FIRST)
        def _():
            send(5, 6)

    z_copies = (
        remote(z_piece, z_in, z_send.at[0], z_recv.at[0], k, ring_at * 2 + 1 - place),
        remote(z_scale, z_in_scale, z_send.at[1], z_recv.at[1], k, ring_at * 2 + 1 - place),
    )

    def sum_ring():
        phase("p_combine")

        @pl.when(k < FIRST)
        def _():
            combine()
            send(5, 6)

        phase("p_wait")
        all_of(in_pieces.at[pl.ds(0, 4)], p_recv.at[0, 0])
        all_of(in_scales.at[pl.ds(0, 4)], p_recv.at[0, 1])
        for copy in piece_copies(5):
            copy.wait_recv()
        phase("p_sum")
        out = part[ga - 2]
        for i in (0, 1):
            out = out + decoded(in_pieces[i], in_scales[i])
        code, scale = coded(out)
        z_piece[...] = code
        z_scale[...] = scale
        for copy in z_copies:
            copy.start()
        out = part[ga - 1]
        for i in (2, 3, 5):
            out = out + decoded(in_pieces[i], in_scales[i])
        part[ga - 1] = out

    late = jnp.logical_or(odd == 0, k > LATE)

    @pl.when(late)
    def _():
        sum_ring()

    phase("chain")

    @pl.when(odd == 1)
    def _():
        def keep(re, im):
            high, low = split(re)
            qhigh[:, 0:nb] = high
            qlow[:, 0:nb] = low
            high, low = split(im)
            qhigh[:, nb:2 * nb] = high
            qlow[:, nb:2 * nb] = low

        def step(left, high, low):
            out = dot3(left, high, low)
            return join(out[:, 0:nb], out[:, nb:2 * nb])

        phase("q")

        @pl.when(k == 1)
        def _():
            keep(xfull[0], xfull[1])

        @pl.when(k > 1)
        def _():
            x_copy.wait_recv()
            keep(*cmul(xmate[...].reshape(2 * nb, nb), xfull[0], xfull[1]))

        for h in range(2):
            phase("t_in")
            onward(h).wait_recv()
            phase("t_step")
            re, im = step(tin[h].reshape(rows, nb), qhigh[...], qlow[...])
            trow[1, h, 0] = re
            trow[1, h, 1] = im

            @pl.when(k < ka - 1)
            def _():
                onward(h).start()

        encode(1)
        for i in range(1, ga):
            for copy in same_copy(i):
                copy.start()
        tcodes[g] = tcode[1]
        tscales[g] = tscale[1]

        phase("t_mate")

        @pl.when(k == 1)
        def _():
            trow[0] = tin[...]

        @pl.when(k > 1)
        def _():
            left = jnp.concatenate([tin[0, 0], tin[1, 0], tin[0, 1], tin[1, 1]], axis=0)
            re, im = cmul(left, xmate[0], xmate[1])
            for h in range(2):
                trow[0, h, 0] = re[h * few:(h + 1) * few]
                trow[0, h, 1] = im[h * few:(h + 1) * few]

        encode(0)
        for i in range(ga):
            for copy in mate_copy(i):
                copy.start()

    @pl.when(jnp.logical_not(late))
    def _():
        sum_ring()

    phase("z_wait")
    for copy in z_copies:
        copy.wait_recv()
    phase("z_sum")
    whole = part[ga - 1] + decoded(z_in[...], z_in_scale[...])
    b_both = jnp.concatenate([whole[0:nb, 0:cols].T, whole[nb:2 * nb, 0:cols].T], axis=0)
    d_re = whole[0:nb, cols:2 * cols].T
    d_im = whole[nb:2 * nb, cols:2 * cols].T
    atom_column = jnp.broadcast_to(atoms[pl.ds(g, 1), :].astype(F32), (cols, 128)).T

    phase("t_ag")
    def t_all(sem, count):
        all_of(tcodes.at[pl.ds(0, count)], sem.at[0])
        all_of(tscales.at[pl.ds(0, count)], sem.at[1])

    @pl.when(odd == 1)
    def _():
        t_all(g_recv, ga - 1)

    @pl.when(odd == 0)
    def _():
        t_all(g_recv, ga)

    for i in range(ga):
        lines = decoded(tcodes[i], tscales[i]).reshape(2, 2, few, nb)
        for h in range(2):
            tfull[:, i * rows + h * few:i * rows + (h + 1) * few, :] = lines[h]

    phase("w")
    w_re, w_im = cmul(b_both, tfull[0], tfull[1])
    per_proj = jnp.sum(d_re * w_im - d_im * w_re, axis=1, keepdims=True) * (1.0 / ka)
    atom_ids = lax.broadcasted_iota(jnp.int32, (cols, 128), 1).astype(F32)
    force = jnp.sum(jnp.where(atom_column == atom_ids, per_proj, 0.0), axis=0, keepdims=True)
    fka[k] = force

    def along_ka(i):
        return remote(fka.at[k], fka.at[k], f_send, f_recv, ka_at(1 + i), g)

    def along_ga(i):
        return remote(fga.at[g], fga.at[g], l_send, l_recv, k, ga_at(1 + i))

    phase("f_ka")
    for i in range(ka - 1):
        along_ka(i).start()
    all_of(fka.at[pl.ds(0, ka - 1)], f_recv)
    phase("f_ga")
    fga[g] = jnp.sum(fka[...], axis=0)
    for i in range(ga - 1):
        along_ga(i).start()
    all_of(fga.at[pl.ds(0, ga - 1)], l_recv)
    forces[...] = jnp.sum(fga[...], axis=0)

    phase("drain")
    by_class(turn_back, lambda count: all_of(nbt.at[:, :, pl.ds(0, 2 * count)], nb_send))
    for b in range(blocks):
        all_of(mrows.at[b], m_send.at[b])
    e_all(e_send)
    all_of(in_pieces, p_send.at[0])
    all_of(in_scales, p_send.at[1])
    for copy in z_copies:
        copy.wait_send()
    all_of(fga.at[pl.ds(0, ga - 1)], l_send)
    all_of(fka.at[pl.ds(0, ka - 1)], f_send)

    @pl.when(odd == 0)
    def _():
        all_of(taken_rows, a_send)
        s_copy.wait_send()

    @pl.when(k == 0)
    def _():
        first(0).wait_send()
        first(1).wait_send()

    @pl.when(jnp.logical_and(odd == 0, k > 0))
    def _():
        x_copy.wait_send()

    @pl.when(odd == 1)
    def _():
        c_all(c_send, turn_on)
        t_all(g_send, ga - 1)
        t_all(h_send, ga)

        @pl.when(k < ka - 1)
        def _():
            onward(0).wait_send()
            onward(1).wait_send()

    phase(None)


def local(ka, ga, coeffs, projectors, proj_deriv, shift_map, atom_of):
    _, _, half, nb = coeffs.shape
    np_ = projectors.shape[2]
    cols = np_ // ga
    rows = nb // ga
    blocks = nb // BANDS
    brows = BANDS // ga
    anywhere = pl.BlockSpec(memory_space=pl.ANY)
    vmem = pl.BlockSpec(memory_space=pltpu.VMEM)
    dma = pltpu.SemaphoreType.DMA
    transport, forces = pl.pallas_call(
        functools.partial(kernel, ka, ga),
        out_shape=(jax.ShapeDtypeStruct((2, nb, nb), F32), jax.ShapeDtypeStruct((1, 128), F32)),
        in_specs=[anywhere, anywhere, anywhere, vmem, vmem],
        out_specs=(vmem, vmem),
        scratch_shapes=[
            pltpu.VMEM((2 * half, nb), BF16),
            pltpu.VMEM((2 * half, nb), BF16),
            pltpu.VMEM((2 * nb, 2 * half), BF16),
            pltpu.VMEM((blocks, BANDS, 2 * half), BF16),
            pltpu.VMEM((2, TURNED, nb), BF16),
            pltpu.VMEM((2, blocks, BANDS, nb), F32),
            pltpu.VMEM((ga - 1, 2, blocks, brows, nb), F32),
            pltpu.VMEM((2, blocks, brows, nb), F32),
            pltpu.VMEM((2, blocks, brows, nb), F32),
            pltpu.VMEM((3, 2, half, 2 * cols), BF16),
            pltpu.VMEM((ga, 2 * nb, 2 * cols), F32),
            pltpu.VMEM((ga - 2, 2 * nb, 2 * cols), I16),
            pltpu.VMEM((ga - 2, 1, 2 * cols), F32),
            pltpu.VMEM((ga - 2, 2 * nb, 2 * cols), I16),
            pltpu.VMEM((ga - 2, 1, 2 * cols), F32),
            pltpu.VMEM((2 * nb, 2 * cols), I16),
            pltpu.VMEM((1, 2 * cols), F32),
            pltpu.VMEM((2 * nb, 2 * cols), I16),
            pltpu.VMEM((1, 2 * cols), F32),
            pltpu.VMEM((blocks, 2, BANDS, nb), F32),
            pltpu.VMEM((blocks, ga - 1, 2, brows, nb), F32),
            pltpu.VMEM((blocks, 2, brows, nb), F32),
            pltpu.VMEM((2 * blocks * brows, nb), I16),
            pltpu.VMEM((2, 1, nb), F32),
            pltpu.VMEM((ga, 2 * blocks * brows, nb), I16),
            pltpu.VMEM((2, ga, 1, nb), F32),
            pltpu.VMEM((2, nb, nb), F32),
            pltpu.VMEM((2, nb, nb), F32),
            pltpu.VMEM((2, nb, nb), F32),
            pltpu.VMEM((nb, 2 * nb), BF16),
            pltpu.VMEM((nb, 2 * nb), BF16),
            pltpu.VMEM((2, 2, rows // 2, nb), F32),
            pltpu.VMEM((2, 2, 2, rows // 2, nb), F32),
            pltpu.VMEM((2, 2 * rows, nb), I16),
            pltpu.VMEM((2, 1, nb), F32),
            pltpu.VMEM((ga, 2 * rows, nb), I16),
            pltpu.VMEM((ga, 1, nb), F32),
            pltpu.VMEM((ka, 1, 128), F32),
            pltpu.VMEM((ga, 1, 128), F32),
            dma, dma((3, 2)), dma, dma((blocks,)), dma((2,)), dma((2,)), dma, dma, dma, dma, dma, dma,
            dma((2,)), dma((3, 2)), dma((blocks,)), dma((blocks,)), dma((2, 2)), dma((2, 2)),
            dma, dma, dma((2,)), dma((2,)), dma((2,)), dma((2,)), dma((2,)), dma, dma, dma, dma,
            pltpu.SemaphoreType.REGULAR,
        ],
        compiler_params=pltpu.CompilerParams(
            collective_id=0, has_side_effects=True, vmem_limit_bytes=53 * 1024 * 1024),
        name="string",
    )(
        coeffs.reshape(2 * half, nb), projectors, proj_deriv,
        shift_map.reshape(half // 128, 128), atom_of.reshape(ga, cols),
    )
    return transport[None], forces.reshape(128)


def solution(mesh):
    in_specs = (P("ka", None, "ga", None), P(None, "ga", None), P(None, "ga", None), P("ga"), P())
    out_specs = (P("ka", None, None, None), P())
    body = functools.partial(local, mesh.shape["ka"], mesh.shape["ga"])
    return jax.shard_map(body, mesh=mesh, in_specs=in_specs, out_specs=out_specs, check_vma=False)
```

```python
import functools

import jax
import jax.numpy as jnp
from jax import lax
from jax.experimental import pallas as pl
from jax.experimental.pallas import tpu as pltpu
from jax.sharding import PartitionSpec as P

MESH = pl.DeviceIdType.MESH
F32 = jnp.float32
BF16 = jnp.bfloat16
I16 = jnp.int16
BANDS = 64
SHARED = 768
TURNED = 896
EARLY = 2
FIRST = 4
HURRY = 12
LATE = 10


def split(value):
    high = value.astype(BF16)
    low = (value - high.astype(F32)).astype(BF16)
    return high, low


def dot(left, right):
    return jnp.dot(left, right, preferred_element_type=F32)


def dot3(left, right_high, right_low):
    left_high, left_low = split(left)
    return dot(left_high, right_high) + (dot(left_high, right_low) + dot(left_low, right_high))


def join(by_re, by_im):
    rows = by_re.shape[0] // 2
    return by_re[:rows] - by_im[rows:], by_im[:rows] + by_re[rows:]


def cmul(left, right_re, right_im):
    return join(dot3(left, *split(right_re)), dot3(left, *split(right_im)))


def kernel(
    ka, ga, coeffs, proj, deriv, shift, atoms, tfull, forces,
    own, moved, lhs, nbt, cnat, taken, taken_rows, taken_sum, taken_in, rhs, part, pieces, scales, in_pieces, in_scales, z_piece, z_scale, z_in, z_in_scale, mpart, mrows, erow, ecode, escale, ecodes, escales, efull,
    xfull, xmate, qhigh, qlow, tin, trow, tcode, tscale, tcodes, tscales, fka, fga,
    load_sem, rhs_sem, nb_send, nb_recv, z_send, z_recv, c_send, c_recv, a_send, a_recv, s_send, s_recv, p_send, p_recv, m_send, m_recv, e_send, e_recv,
    x_send, x_recv, t_send, t_recv, g_send, g_recv, h_send, f_send, f_recv, l_send, l_recv, ready_sem,
):
    phases = []

    def phase(name):
        if phases:
            phases.pop().__exit__(None, None, None)
        if name:
            phases.append(jax.named_scope(name))
            phases[-1].__enter__()

    phase("start")
    nb = own.shape[1]
    half = own.shape[0] // 2
    cols = part.shape[2] // 2
    rows = nb // ga
    blocks = nb // BANDS
    brows = BANDS // ga
    kept = half - SHARED
    least = half - TURNED
    k = lax.axis_index("ka")
    g = lax.axis_index("ga")
    odd = lax.rem(k, 2)
    mate = k + 1 - 2 * odd
    ring = ga // 2
    ring_at, place = g // 2, lax.rem(g, 2)

    def ga_at(offset):
        return lax.rem(g + offset, ga)

    def ka_at(offset):
        return lax.rem(k + offset, ka)

    def remote(source, target, send, recv, to_k, to_g):
        return pltpu.make_async_remote_copy(
            src_ref=source, dst_ref=target, send_sem=send, recv_sem=recv,
            device_id={"ka": to_k, "ga": to_g}, device_id_type=MESH)

    def all_of(ref, sem):
        pltpu.make_async_copy(ref, ref, sem).wait()

    own_load = pltpu.make_async_copy(coeffs, own, load_sem)
    own_load.start()

    def along_ring(step):
        return lax.rem(ring_at + step, ring) * 2

    def block_of(i):
        last = i // 4
        step = (1 - last) * (1 + 2 * lax.rem(i, 2)) + last * (6 - 2 * (i // 2))
        other = (1 - last) * (1 - i // 2) + last * (1 - lax.rem(i, 2))
        return step, other

    def rhs_loads(i):
        step, other = block_of(i)
        target = along_ring(step) + place + other - 2 * place * other
        slot = lax.rem(i, 3)
        at = pl.ds(pl.multiple_of(target * cols, cols), cols)
        return (
            pltpu.make_async_copy(proj.at[:, :, at], rhs.at[slot, :, :, pl.ds(0, cols)], rhs_sem.at[slot, 0]),
            pltpu.make_async_copy(deriv.at[:, :, at], rhs.at[slot, :, :, pl.ds(cols, cols)], rhs_sem.at[slot, 1]),
        )

    for i in range(2):
        for copy in rhs_loads(i):
            copy.start()

    phase("barrier")
    barrier = pltpu.get_barrier_semaphore()
    for offset in range(1, ga):
        pl.semaphore_signal(barrier, inc=1, device_id={"ka": k, "ga": ga_at(offset)}, device_id_type=MESH)
    for offset in range(ga):
        pl.semaphore_signal(barrier, inc=1, device_id={"ka": mate, "ga": ga_at(offset)}, device_id_type=MESH)
    for offset in range(1, ka - 1):
        other = lax.rem(lax.max(k, mate) + offset, ka)
        pl.semaphore_signal(barrier, inc=1, device_id={"ka": other, "ga": g}, device_id_type=MESH)
    pl.semaphore_wait(barrier, 2 * ga + ka - 3)

    phase("load")
    own_load.wait()

    phase("lhs")
    for at in range(0, half, 384):
        width = min(384, half - at)
        re = own[at:at + width, :].T
        im = own[half + at:half + at + width, :].T
        lhs[0:nb, at:at + width] = re
        lhs[0:nb, half + at:half + at + width] = im
        lhs[nb:2 * nb, at:at + width] = im
        lhs[nb:2 * nb, half + at:half + at + width] = -re

    plane = ka // 2
    turn_back = lax.rem(k, plane) == 0
    turn_on = lax.rem(k, plane) == plane - 1
    ranges = tuple(
        (part_at + first, last - first) for first, last in ((0, least), (least, kept), (kept, half)) for part_at in (0, half))

    def nb_copy(b, r):
        at = pl.ds(*ranges[r])
        return remote(lhs.at[pl.ds(b * BANDS, BANDS), at], nbt.at[b, :, at], nb_send, nb_recv.at[b],
                      ka_at(ka - 1), g)

    def by_class(turned, act):
        @pl.when(turned)
        def _():
            act(least)

        @pl.when(jnp.logical_and(odd == (0 if turned is turn_back else 1), jnp.logical_not(turned)))
        def _():
            act(kept)

        @pl.when(odd == (1 if turned is turn_back else 0))
        def _():
            act(half)

    for b in range(blocks):
        for r in (0, 1):
            nb_copy(b, r).start()

        @pl.when(jnp.logical_not(turn_back))
        def _():
            for r in (2, 3):
                nb_copy(b, r).start()

        @pl.when(odd == 1)
        def _():
            for r in (4, 5):
                nb_copy(b, r).start()

    phase("permute")

    @pl.when(k == ka - 1)
    def _():
        wanted = jnp.concatenate([shift[r:r + 1, :] for r in range(half // 128)], axis=1) - g * half

        def permute(b, carry):
            at = pl.multiple_of(b * 384, 384)
            index = lax.broadcasted_iota(jnp.int32, (384, half), 0) + at
            chosen = jnp.where(wanted == index, 1.0, 0.0).astype(BF16)
            moved[pl.ds(at, 384), :] = dot(chosen, own[0:half, :]).astype(BF16)
            moved[pl.ds(half + at, 384), :] = dot(chosen, own[half:2 * half, :]).astype(BF16)
            return carry

        lax.fori_loop(0, half // 384, permute, 0)
        own[...] = moved[...]

    def c_copy(r):
        first, count = ranges[2 + r]
        part_at = half * (r % 2)
        return remote(own.at[pl.ds(first, count)], cnat.at[r % 2, pl.ds(first - part_at - least, count)],
                      c_send, c_recv, ka_at(1), g)

    @pl.when(odd == 1)
    def _():
        for r in (2, 3):
            c_copy(r).start()

        @pl.when(turn_on)
        def _():
            for r in (0, 1):
                c_copy(r).start()

    def c_all(sem, short):
        @pl.when(short)
        def _():
            all_of(cnat, sem)

        @pl.when(jnp.logical_not(short))
        def _():
            all_of(cnat.at[:, pl.ds(kept - least, SHARED)], sem)

    def piece_to(i):
        across = (i // 4) * (1 - lax.rem(i, 2))
        return along_ring((1 - across) * block_of(i)[0]) + place + across * (1 - 2 * place)

    def piece_copies(i):
        return (
            remote(pieces.at[i], in_pieces.at[i], p_send.at[0], p_recv.at[lax.max(i, 3) - 3, 0], k, piece_to(i)),
            remote(scales.at[i], in_scales.at[i], p_send.at[1], p_recv.at[lax.max(i, 3) - 3, 1], k, piece_to(i)),
        )

    def coded(values):
        top = jnp.maximum(jnp.max(jnp.abs(values), axis=0, keepdims=True), 1e-30)
        code = jnp.round(values * (32767.0 / top)).astype(jnp.int32).astype(I16)
        return code, top * (1.0 / 32767.0)

    def decoded(code, scale):
        return code.astype(jnp.int32).astype(F32) * scale

    hurry = k < HURRY

    def combine():
        for copy in piece_copies(4):
            copy.wait_recv()
        code, scale = coded(part[5] + decoded(in_pieces[4], in_scales[4]))
        pieces[5] = code
        scales[5] = scale

    def send(first, last):
        for i in range(first, last):
            for copy in piece_copies(i):
                copy.start()

    def project(i, carry):
        for copy in rhs_loads(i):
            copy.wait()

        @pl.when(i + 2 < ga)
        def _():
            for copy in rhs_loads(i + 2):
                copy.start()

        part[i] = dot(lhs[...], rhs[lax.rem(i, 3)].reshape(2 * half, 2 * cols))

        @pl.when(i < ga - 3)
        def _():
            code, scale = coded(part[i])
            pieces[i] = code
            scales[i] = scale

        @pl.when(i < EARLY)
        def _():
            for copy in piece_copies(i):
                copy.start()

        return carry

    def m_copy(b, i):
        target = ga_at(1 + i)
        at = pl.ds(pl.multiple_of(target * brows, brows), brows)
        return remote(mpart.at[b, :, at, :], mrows.at[b, i], m_send.at[b], m_recv.at[b], k, target)

    def intersect(b):
        phase(f"nb_wait{b}")

        def over(count):
            re, im = nbt[b, :, 0:count], nbt[b, :, half:half + count]
            by_re = dot(jnp.concatenate([re, im], axis=0), own[0:count, :])
            by_im = dot(jnp.concatenate([im, -re], axis=0), own[half:half + count, :])
            mpart[b] = (by_re + by_im).reshape(2, BANDS, nb)

        def here(count):
            all_of(nbt.at[b, :, pl.ds(0, 2 * count)], nb_recv.at[b])
            over(count)

        by_class(turn_on, here)
        phase(f"m_dot{b}")
        for i in range(ga - 1):
            m_copy(b, i).start()

    def a_copy(i):
        at = pl.ds(pl.multiple_of(ga_at(1 + i) * brows, brows), brows)
        return remote(taken.at[:, :, at, :], taken_rows.at[i], a_send, a_recv, k, ga_at(1 + i))

    s_copy = remote(taken_sum, taken_in, s_send, s_recv, ka_at(ka - 1), g)

    def take():
        c_all(c_recv, turn_back)

        def from_wave(first):
            out = dot(lhs[:, first:half], cnat[0, first - least:])
            out = out + dot(lhs[:, half + first:2 * half], cnat[1, first - least:])
            taken[...] = out.reshape(2, blocks, BANDS, nb)

        @pl.when(turn_back)
        def _():
            from_wave(least)

        @pl.when(jnp.logical_not(turn_back))
        def _():
            from_wave(kept)

        for i in range(ga - 1):
            a_copy(i).start()

    def give_back():
        out = taken[:, :, pl.ds(pl.multiple_of(g * brows, brows), brows), :]
        all_of(taken_rows, a_recv)
        for i in range(ga - 1):
            out = out + taken_rows[i]
        taken_sum[...] = out
        s_copy.start()

    even = jnp.logical_and(odd == 0, k > 0)

    spans = ((0, blocks - 1), (blocks - 1, blocks))

    def span_rows(span):
        return pl.ds(2 * brows * spans[span][0], 2 * brows * (spans[span][1] - spans[span][0]))

    def e_copies(span, i):
        to = ga_at(1 + i)
        return (
            remote(ecode.at[span_rows(span)], ecodes.at[g, span_rows(span)], e_send.at[span, 0], e_recv.at[span, 0], k, to),
            remote(escale.at[span], escales.at[span, g], e_send.at[span, 1], e_recv.at[span, 1], k, to),
        )

    def spread(span):
        first, last = spans[span]
        code, scale = coded(erow[first:last].reshape(2 * brows * (last - first), nb))
        ecode[span_rows(span), :] = code
        escale[span] = scale
        for i in range(ga - 1):
            for copy in e_copies(span, i):
                copy.start()
        ecodes[g, span_rows(span), :] = code
        escales[span, g] = scale

    def settle(b):
        phase(f"m_rs{b}")
        total = mpart[b, :, pl.ds(pl.multiple_of(g * brows, brows), brows), :]
        all_of(mrows.at[b], m_recv.at[b])
        for i in range(ga - 1):
            total = total + mrows[b, i]
        erow[b] = total

        @pl.when(odd == 1)
        def _():
            if b == 0:
                s_copy.wait_recv()
            erow[b] = total + taken_in[:, b]

        total = erow[b]
        first = b * BANDS + g * brows
        row_at = lax.broadcasted_iota(jnp.int32, (brows, nb), 0) + first
        col_at = lax.broadcasted_iota(jnp.int32, (brows, nb), 1)
        erow[b, 0] = jnp.where(row_at == col_at, 1.0, 0.0) - total[0]
        erow[b, 1] = -total[1]

    phase("project0")
    lax.fori_loop(0, 4, project, 0)

    intersect(0)
    phase("project1")
    lax.fori_loop(4, 6, project, 0)
    intersect(1)
    phase("take")

    @pl.when(even)
    def _():
        take()


    @pl.when(k >= FIRST)
    def _():
        send(EARLY, 4)

    phase("project2")
    lax.fori_loop(6, ga, project, 0)
    intersect(2)
    intersect(3)
    phase("give_back")

    @pl.when(even)
    def _():
        give_back()

    @pl.when(k >= FIRST)
    def _():
        send(4, 5)

    settle(0)
    settle(1)
    settle(2)
    spread(0)
    settle(3)
    spread(1)
    phase("combine")

    @pl.when(k >= FIRST)
    def _():
        combine()

    @pl.when(jnp.logical_not(hurry))
    def _():
        send(5, 6)

    phase("take_last")

    @pl.when(k == 0)
    def _():
        take()

    phase("e_ag")
    def e_all(sem):
        for span in range(2):
            all_of(ecodes.at[pl.ds(0, ga - 1), span_rows(span)], sem.at[span, 0])
            all_of(escales.at[span, pl.ds(0, ga - 1)], sem.at[span, 1])

    e_all(e_recv)
    for i in range(ga):
        for b in range(blocks):
            span = b // (blocks - 1)
            code = ecodes[i, 2 * brows * b:2 * brows * (b + 1), :]
            efull[:, b * BANDS + i * brows:b * BANDS + (i + 1) * brows, :] = decoded(code, escales[span, i]).reshape(
                2, brows, nb)

    @pl.when(hurry)
    def _():
        pl.semaphore_signal(ready_sem, inc=1, device_id={"ka": mate, "ga": g}, device_id_type=MESH)

    phase("newton")
    e_re, e_im = efull[0], efull[1]
    both = efull[...].reshape(2 * nb, nb)
    sq_re, sq_im = cmul(both, e_re, e_im)
    eye = jnp.where(
        lax.broadcasted_iota(jnp.int32, (nb, nb), 0) == lax.broadcasted_iota(jnp.int32, (nb, nb), 1), 1.0, 0.0)
    cu_re, cu_im = cmul(both, sq_re, sq_im)
    xfull[0] = (eye + (e_re + (sq_re + cu_re))).T
    xfull[1] = (e_im + (sq_im + cu_im)).T

    phase("chain")
    mine = pl.ds(pl.multiple_of(g * rows, rows), rows)
    x_copy = remote(xfull, xmate, x_send, x_recv, mate, g)
    few = rows // 2

    def onward(h):
        return remote(trow.at[1, h], tin.at[h], t_send.at[h], t_recv.at[h], ka_at(2), g)

    def first(h):
        at = pl.ds(pl.multiple_of(g * rows + h * few, few), few)
        return remote(xfull.at[:, at, :], tin.at[h], t_send.at[h], t_recv.at[h], 1, g)

    def same_copy(i):
        return (
            remote(tcode.at[1], tcodes.at[g], g_send.at[0], g_recv.at[0], k, ga_at(i)),
            remote(tscale.at[1], tscales.at[g], g_send.at[1], g_recv.at[1], k, ga_at(i)),
        )

    def mate_copy(i):
        return (
            remote(tcode.at[0], tcodes.at[g], h_send.at[0], g_recv.at[0], mate, ga_at(i)),
            remote(tscale.at[0], tscales.at[g], h_send.at[1], g_recv.at[1], mate, ga_at(i)),
        )

    def encode(which):
        code, scale = coded(trow[which].reshape(2 * rows, nb))
        tcode[which] = code
        tscale[which] = scale

    @pl.when(k == 0)
    def _():
        first(0).start()
        first(1).start()
        give_back()

    @pl.when(jnp.logical_and(odd == 0, k > 0))
    def _():
        x_copy.start()

    phase("token")
    @pl.when(hurry)
    def _():
        pl.semaphore_wait(ready_sem, 1)

        @pl.when(k < FIRST)
        def _():
            send(EARLY, 5)

        @pl.when(k >= FIRST)
        def _():
            send(5, 6)

    z_copies = (
        remote(z_piece, z_in, z_send.at[0], z_recv.at[0], k, ring_at * 2 + 1 - place),
        remote(z_scale, z_in_scale, z_send.at[1], z_recv.at[1], k, ring_at * 2 + 1 - place),
    )

    def sum_ring():
        phase("p_combine")

        @pl.when(k < FIRST)
        def _():
            combine()
            send(5, 6)

        phase("p_wait")
        all_of(in_pieces.at[pl.ds(0, 4)], p_recv.at[0, 0])
        all_of(in_scales.at[pl.ds(0, 4)], p_recv.at[0, 1])
        for copy in piece_copies(5):
            copy.wait_recv()
        phase("p_sum")
        out = part[ga - 2]
        for i in (0, 1):
            out = out + decoded(in_pieces[i], in_scales[i])
        code, scale = coded(out)
        z_piece[...] = code
        z_scale[...] = scale
        for copy in z_copies:
            copy.start()
        out = part[ga - 1]
        for i in (2, 3, 5):
            out = out + decoded(in_pieces[i], in_scales[i])
        part[ga - 1] = out

    late = jnp.logical_or(odd == 0, k > LATE)

    @pl.when(late)
    def _():
        sum_ring()

    phase("chain")

    @pl.when(odd == 1)
    def _():
        def keep(re, im):
            high, low = split(re)
            qhigh[:, 0:nb] = high
            qlow[:, 0:nb] = low
            high, low = split(im)
            qhigh[:, nb:2 * nb] = high
            qlow[:, nb:2 * nb] = low

        def step(left, high, low):
            out = dot3(left, high, low)
            return join(out[:, 0:nb], out[:, nb:2 * nb])

        phase("q")

        @pl.when(k == 1)
        def _():
            keep(xfull[0], xfull[1])

        @pl.when(k > 1)
        def _():
            x_copy.wait_recv()
            keep(*cmul(xmate[...].reshape(2 * nb, nb), xfull[0], xfull[1]))

        for h in range(2):
            phase("t_in")
            onward(h).wait_recv()
            phase("t_step")
            re, im = step(tin[h].reshape(rows, nb), qhigh[...], qlow[...])
            trow[1, h, 0] = re
            trow[1, h, 1] = im

            @pl.when(k < ka - 1)
            def _():
                onward(h).start()

        encode(1)
        for i in range(1, ga):
            for copy in same_copy(i):
                copy.start()
        tcodes[g] = tcode[1]
        tscales[g] = tscale[1]

        phase("t_mate")

        @pl.when(k == 1)
        def _():
            trow[0] = tin[...]

        @pl.when(k > 1)
        def _():
            left = jnp.concatenate([tin[0, 0], tin[1, 0], tin[0, 1], tin[1, 1]], axis=0)
            re, im = cmul(left, xmate[0], xmate[1])
            for h in range(2):
                trow[0, h, 0] = re[h * few:(h + 1) * few]
                trow[0, h, 1] = im[h * few:(h + 1) * few]

        encode(0)
        for i in range(ga):
            for copy in mate_copy(i):
                copy.start()

    @pl.when(jnp.logical_not(late))
    def _():
        sum_ring()

    phase("z_wait")
    for copy in z_copies:
        copy.wait_recv()
    phase("z_sum")
    whole = part[ga - 1] + decoded(z_in[...], z_in_scale[...])
    b_both = jnp.concatenate([whole[0:nb, 0:cols].T, whole[nb:2 * nb, 0:cols].T], axis=0)
    d_re = whole[0:nb, cols:2 * cols].T
    d_im = whole[nb:2 * nb, cols:2 * cols].T
    atom_column = jnp.broadcast_to(atoms[pl.ds(g, 1), :].astype(F32), (cols, 128)).T

    phase("t_ag")
    def t_all(sem, count):
        all_of(tcodes.at[pl.ds(0, count)], sem.at[0])
        all_of(tscales.at[pl.ds(0, count)], sem.at[1])

    @pl.when(odd == 1)
    def _():
        t_all(g_recv, ga - 1)

    @pl.when(odd == 0)
    def _():
        t_all(g_recv, ga)

    for i in range(ga):
        lines = decoded(tcodes[i], tscales[i]).reshape(2, 2, few, nb)
        for h in range(2):
            tfull[:, i * rows + h * few:i * rows + (h + 1) * few, :] = lines[h]

    phase("w")
    w_re, w_im = cmul(b_both, tfull[0], tfull[1])
    per_proj = jnp.sum(d_re * w_im - d_im * w_re, axis=1, keepdims=True) * (1.0 / ka)
    atom_ids = lax.broadcasted_iota(jnp.int32, (cols, 128), 1).astype(F32)
    force = jnp.sum(jnp.where(atom_column == atom_ids, per_proj, 0.0), axis=0, keepdims=True)
    fka[k] = force

    def along_ka(i):
        return remote(fka.at[k], fka.at[k], f_send, f_recv, ka_at(1 + i), g)

    def along_ga(i):
        return remote(fga.at[g], fga.at[g], l_send, l_recv, k, ga_at(1 + i))

    phase("f_ka")
    for i in range(ka - 1):
        along_ka(i).start()
    all_of(fka.at[pl.ds(0, ka - 1)], f_recv)
    phase("f_ga")
    fga[g] = jnp.sum(fka[...], axis=0)
    for i in range(ga - 1):
        along_ga(i).start()
    all_of(fga.at[pl.ds(0, ga - 1)], l_recv)
    forces[...] = jnp.sum(fga[...], axis=0)

    phase("drain")
    by_class(turn_back, lambda count: all_of(nbt.at[:, :, pl.ds(0, 2 * count)], nb_send))
    for b in range(blocks):
        all_of(mrows.at[b], m_send.at[b])
    e_all(e_send)
    all_of(in_pieces, p_send.at[0])
    all_of(in_scales, p_send.at[1])
    for copy in z_copies:
        copy.wait_send()
    all_of(fga.at[pl.ds(0, ga - 1)], l_send)
    all_of(fka.at[pl.ds(0, ka - 1)], f_send)

    @pl.when(odd == 0)
    def _():
        all_of(taken_rows, a_send)
        s_copy.wait_send()

    @pl.when(k == 0)
    def _():
        first(0).wait_send()
        first(1).wait_send()

    @pl.when(jnp.logical_and(odd == 0, k > 0))
    def _():
        x_copy.wait_send()

    @pl.when(odd == 1)
    def _():
        c_all(c_send, turn_on)
        t_all(g_send, ga - 1)
        t_all(h_send, ga)

        @pl.when(k < ka - 1)
        def _():
            onward(0).wait_send()
            onward(1).wait_send()

    phase(None)


def local(ka, ga, coeffs, projectors, proj_deriv, shift_map, atom_of):
    _, _, half, nb = coeffs.shape
    np_ = projectors.shape[2]
    cols = np_ // ga
    rows = nb // ga
    blocks = nb // BANDS
    brows = BANDS // ga
    anywhere = pl.BlockSpec(memory_space=pl.ANY)
    vmem = pl.BlockSpec(memory_space=pltpu.VMEM)
    dma = pltpu.SemaphoreType.DMA
    transport, forces = pl.pallas_call(
        functools.partial(kernel, ka, ga),
        out_shape=(jax.ShapeDtypeStruct((2, nb, nb), F32), jax.ShapeDtypeStruct((1, 128), F32)),
        in_specs=[anywhere, anywhere, anywhere, vmem, vmem],
        out_specs=(vmem, vmem),
        scratch_shapes=[
            pltpu.VMEM((2 * half, nb), BF16),
            pltpu.VMEM((2 * half, nb), BF16),
            pltpu.VMEM((2 * nb, 2 * half), BF16),
            pltpu.VMEM((blocks, BANDS, 2 * half), BF16),
            pltpu.VMEM((2, TURNED, nb), BF16),
            pltpu.VMEM((2, blocks, BANDS, nb), F32),
            pltpu.VMEM((ga - 1, 2, blocks, brows, nb), F32),
            pltpu.VMEM((2, blocks, brows, nb), F32),
            pltpu.VMEM((2, blocks, brows, nb), F32),
            pltpu.VMEM((3, 2, half, 2 * cols), BF16),
            pltpu.VMEM((ga, 2 * nb, 2 * cols), F32),
            pltpu.VMEM((ga - 2, 2 * nb, 2 * cols), I16),
            pltpu.VMEM((ga - 2, 1, 2 * cols), F32),
            pltpu.VMEM((ga - 2, 2 * nb, 2 * cols), I16),
            pltpu.VMEM((ga - 2, 1, 2 * cols), F32),
            pltpu.VMEM((2 * nb, 2 * cols), I16),
            pltpu.VMEM((1, 2 * cols), F32),
            pltpu.VMEM((2 * nb, 2 * cols), I16),
            pltpu.VMEM((1, 2 * cols), F32),
            pltpu.VMEM((blocks, 2, BANDS, nb), F32),
            pltpu.VMEM((blocks, ga - 1, 2, brows, nb), F32),
            pltpu.VMEM((blocks, 2, brows, nb), F32),
            pltpu.VMEM((2 * blocks * brows, nb), I16),
            pltpu.VMEM((2, 1, nb), F32),
            pltpu.VMEM((ga, 2 * blocks * brows, nb), I16),
            pltpu.VMEM((2, ga, 1, nb), F32),
            pltpu.VMEM((2, nb, nb), F32),
            pltpu.VMEM((2, nb, nb), F32),
            pltpu.VMEM((2, nb, nb), F32),
            pltpu.VMEM((nb, 2 * nb), BF16),
            pltpu.VMEM((nb, 2 * nb), BF16),
            pltpu.VMEM((2, 2, rows // 2, nb), F32),
            pltpu.VMEM((2, 2, 2, rows // 2, nb), F32),
            pltpu.VMEM((2, 2 * rows, nb), I16),
            pltpu.VMEM((2, 1, nb), F32),
            pltpu.VMEM((ga, 2 * rows, nb), I16),
            pltpu.VMEM((ga, 1, nb), F32),
            pltpu.VMEM((ka, 1, 128), F32),
            pltpu.VMEM((ga, 1, 128), F32),
            dma, dma((3, 2)), dma, dma((blocks,)), dma((2,)), dma((2,)), dma, dma, dma, dma, dma, dma,
            dma((2,)), dma((3, 2)), dma((blocks,)), dma((blocks,)), dma((2, 2)), dma((2, 2)),
            dma, dma, dma((2,)), dma((2,)), dma((2,)), dma((2,)), dma((2,)), dma, dma, dma, dma,
            pltpu.SemaphoreType.REGULAR,
        ],
        compiler_params=pltpu.CompilerParams(
            collective_id=0, has_side_effects=True, vmem_limit_bytes=53 * 1024 * 1024),
        name="string",
    )(
        coeffs.reshape(2 * half, nb), projectors, proj_deriv,
        shift_map.reshape(half // 128, 128), atom_of.reshape(ga, cols),
    )
    return transport[None], forces.reshape(128)


def solution(mesh):
    in_specs = (P("ka", None, "ga", None), P(None, "ga", None), P(None, "ga", None), P("ga"), P())
    out_specs = (P("ka", None, None, None), P())
    body = functools.partial(local, mesh.shape["ka"], mesh.shape["ga"])
    return jax.shard_map(body, mesh=mesh, in_specs=in_specs, out_specs=out_specs, check_vma=False)
```

```python
import functools

import jax
import jax.numpy as jnp
from jax import lax
from jax.experimental import pallas as pl
from jax.experimental.pallas import tpu as pltpu
from jax.sharding import PartitionSpec as P

MESH = pl.DeviceIdType.MESH
F32 = jnp.float32
BF16 = jnp.bfloat16
I16 = jnp.int16
BANDS = 64
SHARED = 768
TURNED = 896
EARLY = 2
FIRST = 4
FAR_FIRST = (3, 5, 4, 7, 1, 2, 6)
HURRY = 12
LATE = 10


def split(value):
    high = value.astype(BF16)
    low = (value - high.astype(F32)).astype(BF16)
    return high, low


def dot(left, right):
    return jnp.dot(left, right, preferred_element_type=F32)


def dot3(left, right_high, right_low):
    left_high, left_low = split(left)
    return dot(left_high, right_high) + (dot(left_high, right_low) + dot(left_low, right_high))


def join(by_re, by_im):
    rows = by_re.shape[0] // 2
    return by_re[:rows] - by_im[rows:], by_im[:rows] + by_re[rows:]


def cmul(left, right_re, right_im):
    return join(dot3(left, *split(right_re)), dot3(left, *split(right_im)))


def kernel(
    ka, ga, coeffs, proj, deriv, shift, atoms, tfull, forces,
    own, moved, lhs, nbt, cnat, taken, taken_rows, taken_sum, taken_in, rhs, part, pieces, scales, in_pieces, in_scales, z_piece, z_scale, z_in, z_in_scale, mpart, mrows, erow, ecode, escale, ecodes, escales, efull,
    xfull, xmate, qhigh, qlow, tin, trow, tcode, tscale, tcodes, tscales, fka, fga,
    load_sem, rhs_sem, nb_send, nb_recv, z_send, z_recv, c_send, c_recv, a_send, a_recv, s_send, s_recv, p_send, p_recv, m_send, m_recv, e_send, e_recv,
    x_send, x_recv, t_send, t_recv, g_send, g_recv, h_send, f_send, f_recv, l_send, l_recv, ready_sem,
):
    phases = []

    def phase(name):
        if phases:
            phases.pop().__exit__(None, None, None)
        if name:
            phases.append(jax.named_scope(name))
            phases[-1].__enter__()

    phase("start")
    nb = own.shape[1]
    half = own.shape[0] // 2
    cols = part.shape[2] // 2
    rows = nb // ga
    blocks = nb // BANDS
    brows = BANDS // ga
    kept = half - SHARED
    least = half - TURNED
    k = lax.axis_index("ka")
    g = lax.axis_index("ga")
    odd = lax.rem(k, 2)
    mate = k + 1 - 2 * odd
    ring = ga // 2
    ring_at, place = g // 2, lax.rem(g, 2)

    def ga_at(offset):
        return lax.rem(g + offset, ga)

    def ka_at(offset):
        return lax.rem(k + offset, ka)

    def remote(source, target, send, recv, to_k, to_g):
        return pltpu.make_async_remote_copy(
            src_ref=source, dst_ref=target, send_sem=send, recv_sem=recv,
            device_id={"ka": to_k, "ga": to_g}, device_id_type=MESH)

    def all_of(ref, sem):
        pltpu.make_async_copy(ref, ref, sem).wait()

    own_load = pltpu.make_async_copy(coeffs, own, load_sem)
    own_load.start()

    def along_ring(step):
        return lax.rem(ring_at + step, ring) * 2

    def block_of(i):
        last = i // 4
        step = (1 - last) * (1 + 2 * lax.rem(i, 2)) + last * (6 - 2 * (i // 2))
        other = (1 - last) * (1 - i // 2) + last * (1 - lax.rem(i, 2))
        return step, other

    def rhs_loads(i):
        step, other = block_of(i)
        target = along_ring(step) + place + other - 2 * place * other
        slot = lax.rem(i, 3)
        at = pl.ds(pl.multiple_of(target * cols, cols), cols)
        return (
            pltpu.make_async_copy(proj.at[:, :, at], rhs.at[slot, :, :, pl.ds(0, cols)], rhs_sem.at[slot, 0]),
            pltpu.make_async_copy(deriv.at[:, :, at], rhs.at[slot, :, :, pl.ds(cols, cols)], rhs_sem.at[slot, 1]),
        )

    for i in range(2):
        for copy in rhs_loads(i):
            copy.start()

    phase("barrier")
    barrier = pltpu.get_barrier_semaphore()
    for offset in range(1, ga):
        pl.semaphore_signal(barrier, inc=1, device_id={"ka": k, "ga": ga_at(offset)}, device_id_type=MESH)
    for offset in range(ga):
        pl.semaphore_signal(barrier, inc=1, device_id={"ka": mate, "ga": ga_at(offset)}, device_id_type=MESH)
    for offset in range(1, ka - 1):
        other = lax.rem(lax.max(k, mate) + offset, ka)
        pl.semaphore_signal(barrier, inc=1, device_id={"ka": other, "ga": g}, device_id_type=MESH)
    pl.semaphore_wait(barrier, 2 * ga + ka - 3)

    phase("load")
    own_load.wait()

    phase("lhs")
    for at in range(0, half, 384):
        width = min(384, half - at)
        re = own[at:at + width, :].T
        im = own[half + at:half + at + width, :].T
        lhs[0:nb, at:at + width] = re
        lhs[0:nb, half + at:half + at + width] = im
        lhs[nb:2 * nb, at:at + width] = im
        lhs[nb:2 * nb, half + at:half + at + width] = -re

    plane = ka // 2
    turn_back = lax.rem(k, plane) == 0
    turn_on = lax.rem(k, plane) == plane - 1
    ranges = tuple(
        (part_at + first, last - first) for first, last in ((0, least), (least, kept), (kept, half)) for part_at in (0, half))

    def nb_copy(b, r):
        at = pl.ds(*ranges[r])
        return remote(lhs.at[pl.ds(b * BANDS, BANDS), at], nbt.at[b, :, at], nb_send, nb_recv.at[b],
                      ka_at(ka - 1), g)

    def by_class(turned, act):
        @pl.when(turned)
        def _():
            act(least)

        @pl.when(jnp.logical_and(odd == (0 if turned is turn_back else 1), jnp.logical_not(turned)))
        def _():
            act(kept)

        @pl.when(odd == (1 if turned is turn_back else 0))
        def _():
            act(half)

    for b in range(blocks):
        for r in (0, 1):
            nb_copy(b, r).start()

        @pl.when(jnp.logical_not(turn_back))
        def _():
            for r in (2, 3):
                nb_copy(b, r).start()

        @pl.when(odd == 1)
        def _():
            for r in (4, 5):
                nb_copy(b, r).start()

    phase("permute")

    @pl.when(k == ka - 1)
    def _():
        wanted = jnp.concatenate([shift[r:r + 1, :] for r in range(half // 128)], axis=1) - g * half

        def permute(b, carry):
            at = pl.multiple_of(b * 384, 384)
            index = lax.broadcasted_iota(jnp.int32, (384, half), 0) + at
            chosen = jnp.where(wanted == index, 1.0, 0.0).astype(BF16)
            moved[pl.ds(at, 384), :] = dot(chosen, own[0:half, :]).astype(BF16)
            moved[pl.ds(half + at, 384), :] = dot(chosen, own[half:2 * half, :]).astype(BF16)
            return carry

        lax.fori_loop(0, half // 384, permute, 0)
        own[...] = moved[...]

    def c_copy(r):
        first, count = ranges[2 + r]
        part_at = half * (r % 2)
        return remote(own.at[pl.ds(first, count)], cnat.at[r % 2, pl.ds(first - part_at - least, count)],
                      c_send, c_recv, ka_at(1), g)

    @pl.when(odd == 1)
    def _():
        for r in (2, 3):
            c_copy(r).start()

        @pl.when(turn_on)
        def _():
            for r in (0, 1):
                c_copy(r).start()

    def c_all(sem, short):
        @pl.when(short)
        def _():
            all_of(cnat, sem)

        @pl.when(jnp.logical_not(short))
        def _():
            all_of(cnat.at[:, pl.ds(kept - least, SHARED)], sem)

    def piece_to(i):
        across = (i // 4) * (1 - lax.rem(i, 2))
        return along_ring((1 - across) * block_of(i)[0]) + place + across * (1 - 2 * place)

    def piece_copies(i):
        return (
            remote(pieces.at[i], in_pieces.at[i], p_send.at[0], p_recv.at[lax.max(i, 3) - 3, 0], k, piece_to(i)),
            remote(scales.at[i], in_scales.at[i], p_send.at[1], p_recv.at[lax.max(i, 3) - 3, 1], k, piece_to(i)),
        )

    def coded(values):
        top = jnp.maximum(jnp.max(jnp.abs(values), axis=0, keepdims=True), 1e-30)
        code = jnp.round(values * (32767.0 / top)).astype(jnp.int32).astype(I16)
        return code, top * (1.0 / 32767.0)

    def decoded(code, scale):
        return code.astype(jnp.int32).astype(F32) * scale

    hurry = k < HURRY

    def combine():
        for copy in piece_copies(4):
            copy.wait_recv()
        code, scale = coded(part[5] + decoded(in_pieces[4], in_scales[4]))
        pieces[5] = code
        scales[5] = scale

    def send(first, last):
        for i in range(first, last):
            for copy in piece_copies(i):
                copy.start()

    def project(i, carry):
        for copy in rhs_loads(i):
            copy.wait()

        @pl.when(i + 2 < ga)
        def _():
            for copy in rhs_loads(i + 2):
                copy.start()

        part[i] = dot(lhs[...], rhs[lax.rem(i, 3)].reshape(2 * half, 2 * cols))

        @pl.when(i < ga - 3)
        def _():
            code, scale = coded(part[i])
            pieces[i] = code
            scales[i] = scale

        @pl.when(i < EARLY)
        def _():
            for copy in piece_copies(i):
                copy.start()

        return carry

    def m_copy(b, i):
        target = ga_at(1 + i)
        at = pl.ds(pl.multiple_of(target * brows, brows), brows)
        return remote(mpart.at[b, :, at, :], mrows.at[b, i], m_send.at[b], m_recv.at[b], k, target)

    def intersect(b):
        phase(f"nb_wait{b}")

        def over(count):
            re, im = nbt[b, :, 0:count], nbt[b, :, half:half + count]
            by_re = dot(jnp.concatenate([re, im], axis=0), own[0:count, :])
            by_im = dot(jnp.concatenate([im, -re], axis=0), own[half:half + count, :])
            mpart[b] = (by_re + by_im).reshape(2, BANDS, nb)

        def here(count):
            all_of(nbt.at[b, :, pl.ds(0, 2 * count)], nb_recv.at[b])
            over(count)

        by_class(turn_on, here)
        phase(f"m_dot{b}")
        for step in FAR_FIRST:
            m_copy(b, step - 1).start()

    def a_copy(i):
        at = pl.ds(pl.multiple_of(ga_at(1 + i) * brows, brows), brows)
        return remote(taken.at[:, :, at, :], taken_rows.at[i], a_send, a_recv, k, ga_at(1 + i))

    s_copy = remote(taken_sum, taken_in, s_send, s_recv, ka_at(ka - 1), g)

    def take():
        c_all(c_recv, turn_back)

        def from_wave(first):
            out = dot(lhs[:, first:half], cnat[0, first - least:])
            out = out + dot(lhs[:, half + first:2 * half], cnat[1, first - least:])
            taken[...] = out.reshape(2, blocks, BANDS, nb)

        @pl.when(turn_back)
        def _():
            from_wave(least)

        @pl.when(jnp.logical_not(turn_back))
        def _():
            from_wave(kept)

        for step in FAR_FIRST:
            a_copy(step - 1).start()

    def give_back():
        out = taken[:, :, pl.ds(pl.multiple_of(g * brows, brows), brows), :]
        all_of(taken_rows, a_recv)
        for i in range(ga - 1):
            out = out + taken_rows[i]
        taken_sum[...] = out
        s_copy.start()

    even = jnp.logical_and(odd == 0, k > 0)

    spans = ((0, blocks - 1), (blocks - 1, blocks))

    def span_rows(span):
        return pl.ds(2 * brows * spans[span][0], 2 * brows * (spans[span][1] - spans[span][0]))

    def e_copies(span, i):
        to = ga_at(1 + i)
        return (
            remote(ecode.at[span_rows(span)], ecodes.at[g, span_rows(span)], e_send.at[span, 0], e_recv.at[span, 0], k, to),
            remote(escale.at[span], escales.at[span, g], e_send.at[span, 1], e_recv.at[span, 1], k, to),
        )

    def spread(span):
        first, last = spans[span]
        code, scale = coded(erow[first:last].reshape(2 * brows * (last - first), nb))
        ecode[span_rows(span), :] = code
        escale[span] = scale
        for step in FAR_FIRST:
            for copy in e_copies(span, step - 1):
                copy.start()
        ecodes[g, span_rows(span), :] = code
        escales[span, g] = scale

    def settle(b):
        phase(f"m_rs{b}")
        total = mpart[b, :, pl.ds(pl.multiple_of(g * brows, brows), brows), :]
        all_of(mrows.at[b], m_recv.at[b])
        for i in range(ga - 1):
            total = total + mrows[b, i]
        erow[b] = total

        @pl.when(odd == 1)
        def _():
            if b == 0:
                s_copy.wait_recv()
            erow[b] = total + taken_in[:, b]

        total = erow[b]
        first = b * BANDS + g * brows
        row_at = lax.broadcasted_iota(jnp.int32, (brows, nb), 0) + first
        col_at = lax.broadcasted_iota(jnp.int32, (brows, nb), 1)
        erow[b, 0] = jnp.where(row_at == col_at, 1.0, 0.0) - total[0]
        erow[b, 1] = -total[1]

    phase("project0")
    lax.fori_loop(0, 4, project, 0)

    intersect(0)
    phase("project1")
    lax.fori_loop(4, 6, project, 0)
    intersect(1)
    phase("take")

    @pl.when(even)
    def _():
        take()


    @pl.when(k >= FIRST)
    def _():
        send(EARLY, 4)

    phase("project2")
    lax.fori_loop(6, ga, project, 0)
    intersect(2)
    intersect(3)
    phase("give_back")

    @pl.when(even)
    def _():
        give_back()

    @pl.when(k >= FIRST)
    def _():
        send(4, 5)

    settle(0)
    settle(1)
    settle(2)
    spread(0)
    settle(3)
    spread(1)
    phase("combine")

    @pl.when(k >= FIRST)
    def _():
        combine()

    @pl.when(jnp.logical_not(hurry))
    def _():
        send(5, 6)

    phase("take_last")

    @pl.when(k == 0)
    def _():
        take()

    phase("e_ag")
    def e_all(sem):
        for span in range(2):
            all_of(ecodes.at[pl.ds(0, ga - 1), span_rows(span)], sem.at[span, 0])
            all_of(escales.at[span, pl.ds(0, ga - 1)], sem.at[span, 1])

    e_all(e_recv)
    for i in range(ga):
        for b in range(blocks):
            span = b // (blocks - 1)
            code = ecodes[i, 2 * brows * b:2 * brows * (b + 1), :]
            efull[:, b * BANDS + i * brows:b * BANDS + (i + 1) * brows, :] = decoded(code, escales[span, i]).reshape(
                2, brows, nb)

    @pl.when(hurry)
    def _():
        pl.semaphore_signal(ready_sem, inc=1, device_id={"ka": mate, "ga": g}, device_id_type=MESH)

    phase("newton")
    e_re, e_im = efull[0], efull[1]
    both = efull[...].reshape(2 * nb, nb)
    sq_re, sq_im = cmul(both, e_re, e_im)
    eye = jnp.where(
        lax.broadcasted_iota(jnp.int32, (nb, nb), 0) == lax.broadcasted_iota(jnp.int32, (nb, nb), 1), 1.0, 0.0)
    cu_re, cu_im = cmul(both, sq_re, sq_im)
    xfull[0] = (eye + (e_re + (sq_re + cu_re))).T
    xfull[1] = (e_im + (sq_im + cu_im)).T

    phase("chain")
    mine = pl.ds(pl.multiple_of(g * rows, rows), rows)
    x_copy = remote(xfull, xmate, x_send, x_recv, mate, g)
    few = rows // 2

    def onward(h):
        return remote(trow.at[1, h], tin.at[h], t_send.at[h], t_recv.at[h], ka_at(2), g)

    def first(h):
        at = pl.ds(pl.multiple_of(g * rows + h * few, few), few)
        return remote(xfull.at[:, at, :], tin.at[h], t_send.at[h], t_recv.at[h], 1, g)

    def same_copy(i):
        return (
            remote(tcode.at[1], tcodes.at[g], g_send.at[0], g_recv.at[0], k, ga_at(i)),
            remote(tscale.at[1], tscales.at[g], g_send.at[1], g_recv.at[1], k, ga_at(i)),
        )

    def mate_copy(i):
        return (
            remote(tcode.at[0], tcodes.at[g], h_send.at[0], g_recv.at[0], mate, ga_at(i)),
            remote(tscale.at[0], tscales.at[g], h_send.at[1], g_recv.at[1], mate, ga_at(i)),
        )

    def encode(which):
        code, scale = coded(trow[which].reshape(2 * rows, nb))
        tcode[which] = code
        tscale[which] = scale

    @pl.when(k == 0)
    def _():
        first(0).start()
        first(1).start()
        give_back()

    @pl.when(jnp.logical_and(odd == 0, k > 0))
    def _():
        x_copy.start()

    phase("token")
    @pl.when(hurry)
    def _():
        pl.semaphore_wait(ready_sem, 1)

        @pl.when(k < FIRST)
        def _():
            send(EARLY, 5)

        @pl.when(k >= FIRST)
        def _():
            send(5, 6)

    z_copies = (
        remote(z_piece, z_in, z_send.at[0], z_recv.at[0], k, ring_at * 2 + 1 - place),
        remote(z_scale, z_in_scale, z_send.at[1], z_recv.at[1], k, ring_at * 2 + 1 - place),
    )

    def sum_ring():
        phase("p_combine")

        @pl.when(k < FIRST)
        def _():
            combine()
            send(5, 6)

        phase("p_wait")
        all_of(in_pieces.at[pl.ds(0, 4)], p_recv.at[0, 0])
        all_of(in_scales.at[pl.ds(0, 4)], p_recv.at[0, 1])
        for copy in piece_copies(5):
            copy.wait_recv()
        phase("p_sum")
        out = part[ga - 2]
        for i in (0, 1):
            out = out + decoded(in_pieces[i], in_scales[i])
        code, scale = coded(out)
        z_piece[...] = code
        z_scale[...] = scale
        for copy in z_copies:
            copy.start()
        out = part[ga - 1]
        for i in (2, 3, 5):
            out = out + decoded(in_pieces[i], in_scales[i])
        part[ga - 1] = out

    late = jnp.logical_or(odd == 0, k > LATE)

    @pl.when(late)
    def _():
        sum_ring()

    phase("chain")

    @pl.when(odd == 1)
    def _():
        def keep(re, im):
            high, low = split(re)
            qhigh[:, 0:nb] = high
            qlow[:, 0:nb] = low
            high, low = split(im)
            qhigh[:, nb:2 * nb] = high
            qlow[:, nb:2 * nb] = low

        def step(left, high, low):
            out = dot3(left, high, low)
            return join(out[:, 0:nb], out[:, nb:2 * nb])

        phase("q")

        @pl.when(k == 1)
        def _():
            keep(xfull[0], xfull[1])

        @pl.when(k > 1)
        def _():
            x_copy.wait_recv()
            keep(*cmul(xmate[...].reshape(2 * nb, nb), xfull[0], xfull[1]))

        for h in range(2):
            phase("t_in")
            onward(h).wait_recv()
            phase("t_step")
            re, im = step(tin[h].reshape(rows, nb), qhigh[...], qlow[...])
            trow[1, h, 0] = re
            trow[1, h, 1] = im

            @pl.when(k < ka - 1)
            def _():
                onward(h).start()

        encode(1)
        for i in FAR_FIRST:
            for copy in same_copy(i):
                copy.start()
        tcodes[g] = tcode[1]
        tscales[g] = tscale[1]

        phase("t_mate")

        @pl.when(k == 1)
        def _():
            trow[0] = tin[...]

        @pl.when(k > 1)
        def _():
            left = jnp.concatenate([tin[0, 0], tin[1, 0], tin[0, 1], tin[1, 1]], axis=0)
            re, im = cmul(left, xmate[0], xmate[1])
            for h in range(2):
                trow[0, h, 0] = re[h * few:(h + 1) * few]
                trow[0, h, 1] = im[h * few:(h + 1) * few]

        encode(0)
        for i in FAR_FIRST + (0,):
            for copy in mate_copy(i):
                copy.start()

    @pl.when(jnp.logical_not(late))
    def _():
        sum_ring()

    phase("z_wait")
    for copy in z_copies:
        copy.wait_recv()
    phase("z_sum")
    whole = part[ga - 1] + decoded(z_in[...], z_in_scale[...])
    b_both = jnp.concatenate([whole[0:nb, 0:cols].T, whole[nb:2 * nb, 0:cols].T], axis=0)
    d_re = whole[0:nb, cols:2 * cols].T
    d_im = whole[nb:2 * nb, cols:2 * cols].T
    atom_column = jnp.broadcast_to(atoms[pl.ds(g, 1), :].astype(F32), (cols, 128)).T

    phase("t_ag")
    def t_all(sem, count):
        all_of(tcodes.at[pl.ds(0, count)], sem.at[0])
        all_of(tscales.at[pl.ds(0, count)], sem.at[1])

    @pl.when(odd == 1)
    def _():
        t_all(g_recv, ga - 1)

    @pl.when(odd == 0)
    def _():
        t_all(g_recv, ga)

    for i in range(ga):
        lines = decoded(tcodes[i], tscales[i]).reshape(2, 2, few, nb)
        for h in range(2):
            tfull[:, i * rows + h * few:i * rows + (h + 1) * few, :] = lines[h]

    phase("w")
    w_re, w_im = cmul(b_both, tfull[0], tfull[1])
    per_proj = jnp.sum(d_re * w_im - d_im * w_re, axis=1, keepdims=True) * (1.0 / ka)
    atom_ids = lax.broadcasted_iota(jnp.int32, (cols, 128), 1).astype(F32)
    force = jnp.sum(jnp.where(atom_column == atom_ids, per_proj, 0.0), axis=0, keepdims=True)
    fka[k] = force

    def along_ka(i):
        return remote(fka.at[k], fka.at[k], f_send, f_recv, ka_at(1 + i), g)

    def along_ga(i):
        return remote(fga.at[g], fga.at[g], l_send, l_recv, k, ga_at(1 + i))

    phase("f_ka")
    for i in range(ka - 1):
        along_ka(i).start()
    all_of(fka.at[pl.ds(0, ka - 1)], f_recv)
    phase("f_ga")
    fga[g] = jnp.sum(fka[...], axis=0)
    for step in FAR_FIRST:
        along_ga(step - 1).start()
    all_of(fga.at[pl.ds(0, ga - 1)], l_recv)
    forces[...] = jnp.sum(fga[...], axis=0)

    phase("drain")
    by_class(turn_back, lambda count: all_of(nbt.at[:, :, pl.ds(0, 2 * count)], nb_send))
    for b in range(blocks):
        all_of(mrows.at[b], m_send.at[b])
    e_all(e_send)
    all_of(in_pieces, p_send.at[0])
    all_of(in_scales, p_send.at[1])
    for copy in z_copies:
        copy.wait_send()
    all_of(fga.at[pl.ds(0, ga - 1)], l_send)
    all_of(fka.at[pl.ds(0, ka - 1)], f_send)

    @pl.when(odd == 0)
    def _():
        all_of(taken_rows, a_send)
        s_copy.wait_send()

    @pl.when(k == 0)
    def _():
        first(0).wait_send()
        first(1).wait_send()

    @pl.when(jnp.logical_and(odd == 0, k > 0))
    def _():
        x_copy.wait_send()

    @pl.when(odd == 1)
    def _():
        c_all(c_send, turn_on)
        t_all(g_send, ga - 1)
        t_all(h_send, ga)

        @pl.when(k < ka - 1)
        def _():
            onward(0).wait_send()
            onward(1).wait_send()

    phase(None)


def local(ka, ga, coeffs, projectors, proj_deriv, shift_map, atom_of):
    _, _, half, nb = coeffs.shape
    np_ = projectors.shape[2]
    cols = np_ // ga
    rows = nb // ga
    blocks = nb // BANDS
    brows = BANDS // ga
    anywhere = pl.BlockSpec(memory_space=pl.ANY)
    vmem = pl.BlockSpec(memory_space=pltpu.VMEM)
    dma = pltpu.SemaphoreType.DMA
    transport, forces = pl.pallas_call(
        functools.partial(kernel, ka, ga),
        out_shape=(jax.ShapeDtypeStruct((2, nb, nb), F32), jax.ShapeDtypeStruct((1, 128), F32)),
        in_specs=[anywhere, anywhere, anywhere, vmem, vmem],
        out_specs=(vmem, vmem),
        scratch_shapes=[
            pltpu.VMEM((2 * half, nb), BF16),
            pltpu.VMEM((2 * half, nb), BF16),
            pltpu.VMEM((2 * nb, 2 * half), BF16),
            pltpu.VMEM((blocks, BANDS, 2 * half), BF16),
            pltpu.VMEM((2, TURNED, nb), BF16),
            pltpu.VMEM((2, blocks, BANDS, nb), F32),
            pltpu.VMEM((ga - 1, 2, blocks, brows, nb), F32),
            pltpu.VMEM((2, blocks, brows, nb), F32),
            pltpu.VMEM((2, blocks, brows, nb), F32),
            pltpu.VMEM((3, 2, half, 2 * cols), BF16),
            pltpu.VMEM((ga, 2 * nb, 2 * cols), F32),
            pltpu.VMEM((ga - 2, 2 * nb, 2 * cols), I16),
            pltpu.VMEM((ga - 2, 1, 2 * cols), F32),
            pltpu.VMEM((ga - 2, 2 * nb, 2 * cols), I16),
            pltpu.VMEM((ga - 2, 1, 2 * cols), F32),
            pltpu.VMEM((2 * nb, 2 * cols), I16),
            pltpu.VMEM((1, 2 * cols), F32),
            pltpu.VMEM((2 * nb, 2 * cols), I16),
            pltpu.VMEM((1, 2 * cols), F32),
            pltpu.VMEM((blocks, 2, BANDS, nb), F32),
            pltpu.VMEM((blocks, ga - 1, 2, brows, nb), F32),
            pltpu.VMEM((blocks, 2, brows, nb), F32),
            pltpu.VMEM((2 * blocks * brows, nb), I16),
            pltpu.VMEM((2, 1, nb), F32),
            pltpu.VMEM((ga, 2 * blocks * brows, nb), I16),
            pltpu.VMEM((2, ga, 1, nb), F32),
            pltpu.VMEM((2, nb, nb), F32),
            pltpu.VMEM((2, nb, nb), F32),
            pltpu.VMEM((2, nb, nb), F32),
            pltpu.VMEM((nb, 2 * nb), BF16),
            pltpu.VMEM((nb, 2 * nb), BF16),
            pltpu.VMEM((2, 2, rows // 2, nb), F32),
            pltpu.VMEM((2, 2, 2, rows // 2, nb), F32),
            pltpu.VMEM((2, 2 * rows, nb), I16),
            pltpu.VMEM((2, 1, nb), F32),
            pltpu.VMEM((ga, 2 * rows, nb), I16),
            pltpu.VMEM((ga, 1, nb), F32),
            pltpu.VMEM((ka, 1, 128), F32),
            pltpu.VMEM((ga, 1, 128), F32),
            dma, dma((3, 2)), dma, dma((blocks,)), dma((2,)), dma((2,)), dma, dma, dma, dma, dma, dma,
            dma((2,)), dma((3, 2)), dma((blocks,)), dma((blocks,)), dma((2, 2)), dma((2, 2)),
            dma, dma, dma((2,)), dma((2,)), dma((2,)), dma((2,)), dma((2,)), dma, dma, dma, dma,
            pltpu.SemaphoreType.REGULAR,
        ],
        compiler_params=pltpu.CompilerParams(
            collective_id=0, has_side_effects=True, vmem_limit_bytes=53 * 1024 * 1024),
        name="string",
    )(
        coeffs.reshape(2 * half, nb), projectors, proj_deriv,
        shift_map.reshape(half // 128, 128), atom_of.reshape(ga, cols),
    )
    return transport[None], forces.reshape(128)


def solution(mesh):
    in_specs = (P("ka", None, "ga", None), P(None, "ga", None), P(None, "ga", None), P("ga"), P())
    out_specs = (P("ka", None, None, None), P())
    body = functools.partial(local, mesh.shape["ka"], mesh.shape["ga"])
    return jax.shard_map(body, mesh=mesh, in_specs=in_specs, out_specs=out_specs, check_vma=False)
```

```python
import functools

import jax
import jax.numpy as jnp
from jax import lax
from jax.experimental import pallas as pl
from jax.experimental.pallas import tpu as pltpu
from jax.sharding import PartitionSpec as P

MESH = pl.DeviceIdType.MESH
F32 = jnp.float32
BF16 = jnp.bfloat16
I16 = jnp.int16
BANDS = 64
SHARED = 768
TURNED = 896
EARLY = 2
FIRST = 4
FAR_FIRST = (3, 5, 4, 7, 1, 2, 6)
HURRY = 12
LATE = 10


def split(value):
    high = value.astype(BF16)
    low = (value - high.astype(F32)).astype(BF16)
    return high, low


def dot(left, right):
    return jnp.dot(left, right, preferred_element_type=F32)


def dot3(left, right_high, right_low):
    left_high, left_low = split(left)
    return dot(left_high, right_high) + (dot(left_high, right_low) + dot(left_low, right_high))


def join(by_re, by_im):
    rows = by_re.shape[0] // 2
    return by_re[:rows] - by_im[rows:], by_im[:rows] + by_re[rows:]


def cmul(left, right_re, right_im):
    return join(dot3(left, *split(right_re)), dot3(left, *split(right_im)))


def kernel(
    ka, ga, coeffs, proj, deriv, shift, atoms, tfull, forces,
    own, moved, lhs, nbt, cnat, taken, taken_rows, taken_sum, taken_in, rhs, part, pieces, scales, in_pieces, in_scales, z_piece, z_scale, z_in, z_in_scale, mpart, mrows, erow, ecode, escale, ecodes, escales, efull,
    xfull, xmate, qhigh, qlow, tin, trow, tcode, tscale, tcodes, tscales, fka, fga,
    load_sem, rhs_sem, nb_send, nb_recv, z_send, z_recv, c_send, c_recv, a_send, a_recv, s_send, s_recv, p_send, p_recv, m_send, m_recv, e_send, e_recv,
    x_send, x_recv, t_send, t_recv, g_send, g_recv, h_send, f_send, f_recv, l_send, l_recv, ready_sem,
):
    phases = []

    def phase(name):
        if phases:
            phases.pop().__exit__(None, None, None)
        if name:
            phases.append(jax.named_scope(name))
            phases[-1].__enter__()

    phase("start")
    nb = own.shape[1]
    half = own.shape[0] // 2
    cols = part.shape[2] // 2
    rows = nb // ga
    blocks = nb // BANDS
    brows = BANDS // ga
    kept = half - SHARED
    least = half - TURNED
    k = lax.axis_index("ka")
    g = lax.axis_index("ga")
    odd = lax.rem(k, 2)
    mate = k + 1 - 2 * odd
    ring = ga // 2
    ring_at, place = g // 2, lax.rem(g, 2)

    def ga_at(offset):
        return lax.rem(g + offset, ga)

    def ka_at(offset):
        return lax.rem(k + offset, ka)

    def remote(source, target, send, recv, to_k, to_g):
        return pltpu.make_async_remote_copy(
            src_ref=source, dst_ref=target, send_sem=send, recv_sem=recv,
            device_id={"ka": to_k, "ga": to_g}, device_id_type=MESH)

    def all_of(ref, sem):
        pltpu.make_async_copy(ref, ref, sem).wait()

    own_load = pltpu.make_async_copy(coeffs, own, load_sem)
    own_load.start()

    def along_ring(step):
        return lax.rem(ring_at + step, ring) * 2

    def block_of(i):
        last = i // 4
        step = (1 - last) * (1 + 2 * lax.rem(i, 2)) + last * (6 - 2 * (i // 2))
        other = (1 - last) * (1 - i // 2) + last * (1 - lax.rem(i, 2))
        return step, other

    def rhs_loads(i):
        step, other = block_of(i)
        target = along_ring(step) + place + other - 2 * place * other
        slot = lax.rem(i, 3)
        at = pl.ds(pl.multiple_of(target * cols, cols), cols)
        return (
            pltpu.make_async_copy(proj.at[:, :, at], rhs.at[slot, :, :, pl.ds(0, cols)], rhs_sem.at[slot, 0]),
            pltpu.make_async_copy(deriv.at[:, :, at], rhs.at[slot, :, :, pl.ds(cols, cols)], rhs_sem.at[slot, 1]),
        )

    for i in range(2):
        for copy in rhs_loads(i):
            copy.start()

    phase("barrier")
    barrier = pltpu.get_barrier_semaphore()
    for offset in range(1, ga):
        pl.semaphore_signal(barrier, inc=1, device_id={"ka": k, "ga": ga_at(offset)}, device_id_type=MESH)
    for offset in range(ga):
        pl.semaphore_signal(barrier, inc=1, device_id={"ka": mate, "ga": ga_at(offset)}, device_id_type=MESH)
    for offset in range(1, ka - 1):
        other = lax.rem(lax.max(k, mate) + offset, ka)
        pl.semaphore_signal(barrier, inc=1, device_id={"ka": other, "ga": g}, device_id_type=MESH)
    pl.semaphore_wait(barrier, 2 * ga + ka - 3)

    phase("load")
    own_load.wait()

    phase("lhs")
    for at in range(0, half, 384):
        width = min(384, half - at)
        re = own[at:at + width, :].T
        im = own[half + at:half + at + width, :].T
        lhs[0:nb, at:at + width] = re
        lhs[0:nb, half + at:half + at + width] = im
        lhs[nb:2 * nb, at:at + width] = im
        lhs[nb:2 * nb, half + at:half + at + width] = -re

    plane = ka // 2
    turn_back = lax.rem(k, plane) == 0
    turn_on = lax.rem(k, plane) == plane - 1
    ranges = tuple(
        (part_at + first, last - first) for first, last in ((0, least), (least, kept), (kept, half)) for part_at in (0, half))

    def nb_copy(b, r):
        at = pl.ds(*ranges[r])
        return remote(lhs.at[pl.ds(b * BANDS, BANDS), at], nbt.at[b, :, at], nb_send, nb_recv.at[b],
                      ka_at(ka - 1), g)

    def by_class(turned, act):
        @pl.when(turned)
        def _():
            act(least)

        @pl.when(jnp.logical_and(odd == (0 if turned is turn_back else 1), jnp.logical_not(turned)))
        def _():
            act(kept)

        @pl.when(odd == (1 if turned is turn_back else 0))
        def _():
            act(half)

    for b in range(blocks):
        for r in (0, 1):
            nb_copy(b, r).start()

        @pl.when(jnp.logical_not(turn_back))
        def _():
            for r in (2, 3):
                nb_copy(b, r).start()

        @pl.when(odd == 1)
        def _():
            for r in (4, 5):
                nb_copy(b, r).start()

    phase("permute")

    @pl.when(k == ka - 1)
    def _():
        wanted = jnp.concatenate([shift[r:r + 1, :] for r in range(half // 128)], axis=1) - g * half

        def permute(b, carry):
            at = pl.multiple_of(b * 384, 384)
            index = lax.broadcasted_iota(jnp.int32, (384, half), 0) + at
            chosen = jnp.where(wanted == index, 1.0, 0.0).astype(BF16)
            moved[pl.ds(at, 384), :] = dot(chosen, own[0:half, :]).astype(BF16)
            moved[pl.ds(half + at, 384), :] = dot(chosen, own[half:2 * half, :]).astype(BF16)
            return carry

        lax.fori_loop(0, half // 384, permute, 0)
        own[...] = moved[...]

    def c_copy(r):
        first, count = ranges[2 + r]
        part_at = half * (r % 2)
        return remote(own.at[pl.ds(first, count)], cnat.at[r % 2, pl.ds(first - part_at - least, count)],
                      c_send, c_recv, ka_at(1), g)

    @pl.when(odd == 1)
    def _():
        for r in (2, 3):
            c_copy(r).start()

        @pl.when(turn_on)
        def _():
            for r in (0, 1):
                c_copy(r).start()

    def c_all(sem, short):
        @pl.when(short)
        def _():
            all_of(cnat, sem)

        @pl.when(jnp.logical_not(short))
        def _():
            all_of(cnat.at[:, pl.ds(kept - least, SHARED)], sem)

    def piece_to(i):
        across = (i // 4) * (1 - lax.rem(i, 2))
        return along_ring((1 - across) * block_of(i)[0]) + place + across * (1 - 2 * place)

    def piece_copies(i):
        return (
            remote(pieces.at[i], in_pieces.at[i], p_send.at[0], p_recv.at[lax.max(i, 3) - 3, 0], k, piece_to(i)),
            remote(scales.at[i], in_scales.at[i], p_send.at[1], p_recv.at[lax.max(i, 3) - 3, 1], k, piece_to(i)),
        )

    def coded(values):
        top = jnp.maximum(jnp.max(jnp.abs(values), axis=0, keepdims=True), 1e-30)
        code = jnp.round(values * (32767.0 / top)).astype(jnp.int32).astype(I16)
        return code, top * (1.0 / 32767.0)

    def decoded(code, scale):
        return code.astype(jnp.int32).astype(F32) * scale

    hurry = k < HURRY

    def combine():
        for copy in piece_copies(4):
            copy.wait_recv()
        code, scale = coded(part[5] + decoded(in_pieces[4], in_scales[4]))
        pieces[5] = code
        scales[5] = scale

    def send(first, last):
        for i in range(first, last):
            for copy in piece_copies(i):
                copy.start()

    def project(i, carry):
        for copy in rhs_loads(i):
            copy.wait()

        @pl.when(i + 2 < ga)
        def _():
            for copy in rhs_loads(i + 2):
                copy.start()

        part[i] = dot(lhs[...], rhs[lax.rem(i, 3)].reshape(2 * half, 2 * cols))

        @pl.when(i < ga - 3)
        def _():
            code, scale = coded(part[i])
            pieces[i] = code
            scales[i] = scale

        @pl.when(i < EARLY)
        def _():
            for copy in piece_copies(i):
                copy.start()

        return carry

    def m_copy(b, i):
        target = ga_at(1 + i)
        at = pl.ds(pl.multiple_of(target * brows, brows), brows)
        return remote(mpart.at[b, :, at, :], mrows.at[b, i], m_send.at[b], m_recv.at[b], k, target)

    def intersect(b):
        phase(f"nb_wait{b}")

        def over(count):
            re, im = nbt[b, :, 0:count], nbt[b, :, half:half + count]
            by_re = dot(jnp.concatenate([re, im], axis=0), own[0:count, :])
            by_im = dot(jnp.concatenate([im, -re], axis=0), own[half:half + count, :])
            mpart[b] = (by_re + by_im).reshape(2, BANDS, nb)

        def here(count):
            all_of(nbt.at[b, :, pl.ds(0, 2 * count)], nb_recv.at[b])
            over(count)

        by_class(turn_on, here)
        phase(f"m_dot{b}")
        for step in FAR_FIRST:
            m_copy(b, step - 1).start()

    def a_copy(i):
        at = pl.ds(pl.multiple_of(ga_at(1 + i) * brows, brows), brows)
        return remote(taken.at[:, :, at, :], taken_rows.at[i], a_send, a_recv, k, ga_at(1 + i))

    s_copy = remote(taken_sum, taken_in, s_send, s_recv, ka_at(ka - 1), g)

    def take():
        c_all(c_recv, turn_back)

        def from_wave(first):
            out = dot(lhs[:, first:half], cnat[0, first - least:])
            out = out + dot(lhs[:, half + first:2 * half], cnat[1, first - least:])
            taken[...] = out.reshape(2, blocks, BANDS, nb)

        @pl.when(turn_back)
        def _():
            from_wave(least)

        @pl.when(jnp.logical_not(turn_back))
        def _():
            from_wave(kept)

        for step in FAR_FIRST:
            a_copy(step - 1).start()

    def give_back():
        out = taken[:, :, pl.ds(pl.multiple_of(g * brows, brows), brows), :]
        all_of(taken_rows, a_recv)
        for i in range(ga - 1):
            out = out + taken_rows[i]
        taken_sum[...] = out
        s_copy.start()

    even = jnp.logical_and(odd == 0, k > 0)

    spans = ((0, blocks - 1), (blocks - 1, blocks))

    def span_rows(span):
        return pl.ds(2 * brows * spans[span][0], 2 * brows * (spans[span][1] - spans[span][0]))

    def e_copies(span, i):
        to = ga_at(1 + i)
        return (
            remote(ecode.at[span_rows(span)], ecodes.at[g, span_rows(span)], e_send.at[span, 0], e_recv.at[span, 0], k, to),
            remote(escale.at[span], escales.at[span, g], e_send.at[span, 1], e_recv.at[span, 1], k, to),
        )

    def spread(span):
        first, last = spans[span]
        code, scale = coded(erow[first:last].reshape(2 * brows * (last - first), nb))
        ecode[span_rows(span), :] = code
        escale[span] = scale
        for step in FAR_FIRST:
            for copy in e_copies(span, step - 1):
                copy.start()
        ecodes[g, span_rows(span), :] = code
        escales[span, g] = scale

    def settle(b):
        phase(f"m_rs{b}")
        total = mpart[b, :, pl.ds(pl.multiple_of(g * brows, brows), brows), :]
        all_of(mrows.at[b], m_recv.at[b])
        for i in range(ga - 1):
            total = total + mrows[b, i]
        erow[b] = total

        @pl.when(odd == 1)
        def _():
            if b == 0:
                s_copy.wait_recv()
            erow[b] = total + taken_in[:, b]

        total = erow[b]
        first = b * BANDS + g * brows
        row_at = lax.broadcasted_iota(jnp.int32, (brows, nb), 0) + first
        col_at = lax.broadcasted_iota(jnp.int32, (brows, nb), 1)
        erow[b, 0] = jnp.where(row_at == col_at, 1.0, 0.0) - total[0]
        erow[b, 1] = -total[1]

    phase("project0")
    lax.fori_loop(0, 4, project, 0)

    intersect(0)
    phase("project1")
    lax.fori_loop(4, 6, project, 0)
    intersect(1)
    phase("take")

    @pl.when(even)
    def _():
        take()


    @pl.when(k >= FIRST)
    def _():
        send(EARLY, 4)

    phase("project2")
    lax.fori_loop(6, ga, project, 0)
    intersect(2)
    intersect(3)
    phase("give_back")

    @pl.when(even)
    def _():
        give_back()

    @pl.when(k >= FIRST)
    def _():
        send(4, 5)

    settle(0)
    settle(1)
    settle(2)
    spread(0)
    settle(3)
    spread(1)
    phase("combine")

    @pl.when(k >= FIRST)
    def _():
        combine()

    @pl.when(jnp.logical_not(hurry))
    def _():
        send(5, 6)

    phase("take_last")

    @pl.when(k == 0)
    def _():
        take()

    phase("e_ag")
    def e_all(sem):
        for span in range(2):
            all_of(ecodes.at[pl.ds(0, ga - 1), span_rows(span)], sem.at[span, 0])
            all_of(escales.at[span, pl.ds(0, ga - 1)], sem.at[span, 1])

    e_all(e_recv)
    for i in range(ga):
        for b in range(blocks):
            span = b // (blocks - 1)
            code = ecodes[i, 2 * brows * b:2 * brows * (b + 1), :]
            efull[:, b * BANDS + i * brows:b * BANDS + (i + 1) * brows, :] = decoded(code, escales[span, i]).reshape(
                2, brows, nb)

    @pl.when(hurry)
    def _():
        pl.semaphore_signal(ready_sem, inc=1, device_id={"ka": mate, "ga": g}, device_id_type=MESH)

    phase("newton")
    e_re, e_im = efull[0], efull[1]
    both = efull[...].reshape(2 * nb, nb)
    sq_re, sq_im = cmul(both, e_re, e_im)
    eye = jnp.where(
        lax.broadcasted_iota(jnp.int32, (nb, nb), 0) == lax.broadcasted_iota(jnp.int32, (nb, nb), 1), 1.0, 0.0)
    cu_re, cu_im = cmul(both, sq_re, sq_im)
    xfull[0] = (eye + (e_re + (sq_re + cu_re))).T
    xfull[1] = (e_im + (sq_im + cu_im)).T

    phase("chain")
    mine = pl.ds(pl.multiple_of(g * rows, rows), rows)
    x_copy = remote(xfull, xmate, x_send, x_recv, mate, g)
    few = rows // 2

    def onward(h):
        return remote(trow.at[1, h], tin.at[h], t_send.at[h], t_recv.at[h], ka_at(2), g)

    def first(h):
        at = pl.ds(pl.multiple_of(g * rows + h * few, few), few)
        return remote(xfull.at[:, at, :], tin.at[h], t_send.at[h], t_recv.at[h], 1, g)

    def same_copy(i):
        return (
            remote(tcode.at[1], tcodes.at[g], g_send.at[0], g_recv.at[0], k, ga_at(i)),
            remote(tscale.at[1], tscales.at[g], g_send.at[1], g_recv.at[1], k, ga_at(i)),
        )

    def mate_copy(i):
        return (
            remote(tcode.at[0], tcodes.at[g], h_send.at[0], g_recv.at[0], mate, ga_at(i)),
            remote(tscale.at[0], tscales.at[g], h_send.at[1], g_recv.at[1], mate, ga_at(i)),
        )

    def encode(which):
        code, scale = coded(trow[which].reshape(2 * rows, nb))
        tcode[which] = code
        tscale[which] = scale

    @pl.when(k == 0)
    def _():
        first(0).start()
        first(1).start()
        give_back()

    @pl.when(jnp.logical_and(odd == 0, k > 0))
    def _():
        x_copy.start()

    phase("token")
    @pl.when(hurry)
    def _():
        pl.semaphore_wait(ready_sem, 1)

        @pl.when(k < FIRST)
        def _():
            send(EARLY, 5)

        @pl.when(k >= FIRST)
        def _():
            send(5, 6)

    z_copies = (
        remote(z_piece, z_in, z_send.at[0], z_recv.at[0], k, ring_at * 2 + 1 - place),
        remote(z_scale, z_in_scale, z_send.at[1], z_recv.at[1], k, ring_at * 2 + 1 - place),
    )

    def sum_ring():
        phase("p_combine")

        @pl.when(k < FIRST)
        def _():
            combine()
            send(5, 6)

        phase("p_wait")
        all_of(in_pieces.at[pl.ds(0, 4)], p_recv.at[0, 0])
        all_of(in_scales.at[pl.ds(0, 4)], p_recv.at[0, 1])
        for copy in piece_copies(5):
            copy.wait_recv()
        phase("p_sum")
        out = part[ga - 2]
        for i in (0, 1):
            out = out + decoded(in_pieces[i], in_scales[i])
        code, scale = coded(out)
        z_piece[...] = code
        z_scale[...] = scale
        for copy in z_copies:
            copy.start()
        out = part[ga - 1]
        for i in (2, 3, 5):
            out = out + decoded(in_pieces[i], in_scales[i])
        part[ga - 1] = out

    late = jnp.logical_or(odd == 0, k > LATE)

    @pl.when(late)
    def _():
        sum_ring()

    phase("chain")

    @pl.when(odd == 1)
    def _():
        def keep(re, im):
            high, low = split(re)
            qhigh[:, 0:nb] = high
            qlow[:, 0:nb] = low
            high, low = split(im)
            qhigh[:, nb:2 * nb] = high
            qlow[:, nb:2 * nb] = low

        def step(left, high, low):
            out = dot3(left, high, low)
            return join(out[:, 0:nb], out[:, nb:2 * nb])

        phase("q")

        @pl.when(k == 1)
        def _():
            keep(xfull[0], xfull[1])

        @pl.when(k > 1)
        def _():
            x_copy.wait_recv()
            keep(*cmul(xmate[...].reshape(2 * nb, nb), xfull[0], xfull[1]))

        for h in range(2):
            phase("t_in")
            onward(h).wait_recv()
            phase("t_step")
            re, im = step(tin[h].reshape(rows, nb), qhigh[...], qlow[...])
            trow[1, h, 0] = re
            trow[1, h, 1] = im

            @pl.when(k < ka - 1)
            def _():
                onward(h).start()

        encode(1)
        for i in FAR_FIRST:
            for copy in same_copy(i):
                copy.start()
        tcodes[g] = tcode[1]
        tscales[g] = tscale[1]

        phase("t_mate")

        @pl.when(k == 1)
        def _():
            trow[0] = tin[...]

        @pl.when(k > 1)
        def _():
            left = jnp.concatenate([tin[0, 0], tin[1, 0], tin[0, 1], tin[1, 1]], axis=0)
            re, im = cmul(left, xmate[0], xmate[1])
            for h in range(2):
                trow[0, h, 0] = re[h * few:(h + 1) * few]
                trow[0, h, 1] = im[h * few:(h + 1) * few]

        encode(0)
        for i in FAR_FIRST + (0,):
            for copy in mate_copy(i):
                copy.start()

    @pl.when(jnp.logical_not(late))
    def _():
        sum_ring()

    phase("z_wait")
    for copy in z_copies:
        copy.wait_recv()
    phase("z_sum")
    whole = part[ga - 1] + decoded(z_in[...], z_in_scale[...])
    b_both = jnp.concatenate([whole[0:nb, 0:cols].T, whole[nb:2 * nb, 0:cols].T], axis=0)
    d_re = whole[0:nb, cols:2 * cols].T
    d_im = whole[nb:2 * nb, cols:2 * cols].T
    atom_column = jnp.broadcast_to(atoms[pl.ds(g, 1), :].astype(F32), (cols, 128)).T

    phase("t_ag")
    def t_all(sem, count):
        all_of(tcodes.at[pl.ds(0, count)], sem.at[0])
        all_of(tscales.at[pl.ds(0, count)], sem.at[1])

    @pl.when(odd == 1)
    def _():
        t_all(g_recv, ga - 1)

    @pl.when(odd == 0)
    def _():
        t_all(g_recv, ga)

    for i in range(ga):
        lines = decoded(tcodes[i], tscales[i]).reshape(2, 2, few, nb)
        for h in range(2):
            tfull[:, i * rows + h * few:i * rows + (h + 1) * few, :] = lines[h]

    phase("w")
    w_re, w_im = cmul(b_both, tfull[0], tfull[1])
    per_proj = jnp.sum(d_re * w_im - d_im * w_re, axis=1, keepdims=True) * (1.0 / ka)
    atom_ids = lax.broadcasted_iota(jnp.int32, (cols, 128), 1).astype(F32)
    force = jnp.sum(jnp.where(atom_column == atom_ids, per_proj, 0.0), axis=0, keepdims=True)
    fka[k] = force

    def along_ka(i):
        return remote(fka.at[k], fka.at[k], f_send, f_recv, ka_at(1 + i), g)

    def along_ga(i):
        return remote(fga.at[g], fga.at[g], l_send, l_recv, k, ga_at(1 + i))

    phase("f_ka")
    for step in sorted(range(1, ka), key=lambda step: abs(step % (ka // 2) - ka // 4)):
        along_ka(step - 1).start()
    all_of(fka.at[pl.ds(0, ka - 1)], f_recv)
    phase("f_ga")
    fga[g] = jnp.sum(fka[...], axis=0)
    for step in FAR_FIRST:
        along_ga(step - 1).start()
    all_of(fga.at[pl.ds(0, ga - 1)], l_recv)
    forces[...] = jnp.sum(fga[...], axis=0)

    phase("drain")
    by_class(turn_back, lambda count: all_of(nbt.at[:, :, pl.ds(0, 2 * count)], nb_send))
    for b in range(blocks):
        all_of(mrows.at[b], m_send.at[b])
    e_all(e_send)
    all_of(in_pieces, p_send.at[0])
    all_of(in_scales, p_send.at[1])
    for copy in z_copies:
        copy.wait_send()
    all_of(fga.at[pl.ds(0, ga - 1)], l_send)
    all_of(fka.at[pl.ds(0, ka - 1)], f_send)

    @pl.when(odd == 0)
    def _():
        all_of(taken_rows, a_send)
        s_copy.wait_send()

    @pl.when(k == 0)
    def _():
        first(0).wait_send()
        first(1).wait_send()

    @pl.when(jnp.logical_and(odd == 0, k > 0))
    def _():
        x_copy.wait_send()

    @pl.when(odd == 1)
    def _():
        c_all(c_send, turn_on)
        t_all(g_send, ga - 1)
        t_all(h_send, ga)

        @pl.when(k < ka - 1)
        def _():
            onward(0).wait_send()
            onward(1).wait_send()

    phase(None)


def local(ka, ga, coeffs, projectors, proj_deriv, shift_map, atom_of):
    _, _, half, nb = coeffs.shape
    np_ = projectors.shape[2]
    cols = np_ // ga
    rows = nb // ga
    blocks = nb // BANDS
    brows = BANDS // ga
    anywhere = pl.BlockSpec(memory_space=pl.ANY)
    vmem = pl.BlockSpec(memory_space=pltpu.VMEM)
    dma = pltpu.SemaphoreType.DMA
    transport, forces = pl.pallas_call(
        functools.partial(kernel, ka, ga),
        out_shape=(jax.ShapeDtypeStruct((2, nb, nb), F32), jax.ShapeDtypeStruct((1, 128), F32)),
        in_specs=[anywhere, anywhere, anywhere, vmem, vmem],
        out_specs=(vmem, vmem),
        scratch_shapes=[
            pltpu.VMEM((2 * half, nb), BF16),
            pltpu.VMEM((2 * half, nb), BF16),
            pltpu.VMEM((2 * nb, 2 * half), BF16),
            pltpu.VMEM((blocks, BANDS, 2 * half), BF16),
            pltpu.VMEM((2, TURNED, nb), BF16),
            pltpu.VMEM((2, blocks, BANDS, nb), F32),
            pltpu.VMEM((ga - 1, 2, blocks, brows, nb), F32),
            pltpu.VMEM((2, blocks, brows, nb), F32),
            pltpu.VMEM((2, blocks, brows, nb), F32),
            pltpu.VMEM((3, 2, half, 2 * cols), BF16),
            pltpu.VMEM((ga, 2 * nb, 2 * cols), F32),
            pltpu.VMEM((ga - 2, 2 * nb, 2 * cols), I16),
            pltpu.VMEM((ga - 2, 1, 2 * cols), F32),
            pltpu.VMEM((ga - 2, 2 * nb, 2 * cols), I16),
            pltpu.VMEM((ga - 2, 1, 2 * cols), F32),
            pltpu.VMEM((2 * nb, 2 * cols), I16),
            pltpu.VMEM((1, 2 * cols), F32),
            pltpu.VMEM((2 * nb, 2 * cols), I16),
            pltpu.VMEM((1, 2 * cols), F32),
            pltpu.VMEM((blocks, 2, BANDS, nb), F32),
            pltpu.VMEM((blocks, ga - 1, 2, brows, nb), F32),
            pltpu.VMEM((blocks, 2, brows, nb), F32),
            pltpu.VMEM((2 * blocks * brows, nb), I16),
            pltpu.VMEM((2, 1, nb), F32),
            pltpu.VMEM((ga, 2 * blocks * brows, nb), I16),
            pltpu.VMEM((2, ga, 1, nb), F32),
            pltpu.VMEM((2, nb, nb), F32),
            pltpu.VMEM((2, nb, nb), F32),
            pltpu.VMEM((2, nb, nb), F32),
            pltpu.VMEM((nb, 2 * nb), BF16),
            pltpu.VMEM((nb, 2 * nb), BF16),
            pltpu.VMEM((2, 2, rows // 2, nb), F32),
            pltpu.VMEM((2, 2, 2, rows // 2, nb), F32),
            pltpu.VMEM((2, 2 * rows, nb), I16),
            pltpu.VMEM((2, 1, nb), F32),
            pltpu.VMEM((ga, 2 * rows, nb), I16),
            pltpu.VMEM((ga, 1, nb), F32),
            pltpu.VMEM((ka, 1, 128), F32),
            pltpu.VMEM((ga, 1, 128), F32),
            dma, dma((3, 2)), dma, dma((blocks,)), dma((2,)), dma((2,)), dma, dma, dma, dma, dma, dma,
            dma((2,)), dma((3, 2)), dma((blocks,)), dma((blocks,)), dma((2, 2)), dma((2, 2)),
            dma, dma, dma((2,)), dma((2,)), dma((2,)), dma((2,)), dma((2,)), dma, dma, dma, dma,
            pltpu.SemaphoreType.REGULAR,
        ],
        compiler_params=pltpu.CompilerParams(
            collective_id=0, has_side_effects=True, vmem_limit_bytes=53 * 1024 * 1024),
        name="string",
    )(
        coeffs.reshape(2 * half, nb), projectors, proj_deriv,
        shift_map.reshape(half // 128, 128), atom_of.reshape(ga, cols),
    )
    return transport[None], forces.reshape(128)


def solution(mesh):
    in_specs = (P("ka", None, "ga", None), P(None, "ga", None), P(None, "ga", None), P("ga"), P())
    out_specs = (P("ka", None, None, None), P())
    body = functools.partial(local, mesh.shape["ka"], mesh.shape["ga"])
    return jax.shard_map(body, mesh=mesh, in_specs=in_specs, out_specs=out_specs, check_vma=False)
```
